32 devices in a mesh: fsdp: 32 (over z, y, x, core).
Axes of the slice: x: 2, y: 2, z: 4, core: 2. Of those that a mesh axis runs over, the one named last changes fastest.
Arguments:
- patches: bfloat16 [512, 196, 768], P('fsdp')
- keep: int32 [512, 49], P('fsdp')
- w_patch: float32 [768, 1024], P(None, 'fsdp')
- b_patch: float32 [1024], P('fsdp')
- pos_table: float32 [197, 1024], P(None, 'fsdp')
- cls_tok: float32 [1024], P('fsdp')
- lnp_g: float32 [1024], P('fsdp')
- lnp_b: float32 [1024], P('fsdp')
- ln1_g: float32 [1024], P('fsdp')
- ln1_b: float32 [1024], P('fsdp')
- w_qkv: float32 [1024, 3, 16, 64], P('fsdp')
- b_qkv: float32 [3072], P('fsdp')
- w_out: float32 [1024, 1024], P('fsdp')
- b_out: float32 [1024], P('fsdp')
- ln2_g: float32 [1024], P('fsdp')
- ln2_b: float32 [1024], P('fsdp')
- w_fc: float32 [1024, 4096], P('fsdp')
- b_fc: float32 [4096], P('fsdp')
- w_proj: float32 [4096, 1024], P('fsdp')
- b_proj: float32 [1024], P('fsdp')
- grad_h1: bfloat16 [512, 50, 1024], P('fsdp')
Outputs:
- output 1: bfloat16 [512, 50, 1024], P('fsdp')
- output 2: float32 [768, 1024], P(None, 'fsdp')
- output 3: float32 [1024], P('fsdp')
- output 4: float32 [197, 1024], P(None, 'fsdp')
- output 5: float32 [1024], P('fsdp')
- output 6: float32 [1024], P('fsdp')
- output 7: float32 [1024], P('fsdp')
- output 8: float32 [1024], P('fsdp')
- output 9: float32 [1024], P('fsdp')
- output 10: float32 [1024, 3, 16, 64], P('fsdp')
- output 11: float32 [3072], P('fsdp')
- output 12: float32 [1024, 1024], P('fsdp')
- output 13: float32 [1024], P('fsdp')
- output 14: float32 [1024], P('fsdp')
- output 15: float32 [1024], P('fsdp')
- output 16: float32 [1024, 4096], P('fsdp')
- output 17: float32 [4096], P('fsdp')
- output 18: float32 [4096, 1024], P('fsdp')
- output 19: float32 [1024], P('fsdp')
All inputs are finite; a program needn't handle non-finite values.
Results may differ from the reference program's by a relative error of at most 0.02.
Values are sent between devices in bfloat16 or wider.
A program may use at most 1 GiB of HBM per device.

```python
import jax
import jax.numpy as jnp
from jax import lax

MODEL_WIDTH = 1024
NUM_HEADS = 16
MLP_WIDTH = 4096
NUM_PATCHES = 196
PATCH_PIXELS = 768
NUM_KEEP = 49
BATCH_SIZE = 512
BLOCK_IMAGES = 16
TOKENS = NUM_KEEP + 1
HEAD_DIM = MODEL_WIDTH // NUM_HEADS
LN_EPS = 1e-5
INV_SQRT2 = 0.7071067811865476
INV_SQRT_2PI = 0.3989422804014327
PARAM_NAMES = ('w_patch', 'b_patch', 'pos_table', 'cls_tok', 'lnp_g', 'lnp_b', 'ln1_g', 'ln1_b', 'w_qkv', 'b_qkv', 'w_out', 'b_out', 'ln2_g', 'ln2_b', 'w_fc', 'b_fc', 'w_proj', 'b_proj')
VECTOR_NAMES = ('b_patch', 'cls_tok', 'lnp_g', 'lnp_b', 'ln1_g', 'ln1_b', 'b_qkv', 'b_out', 'ln2_g', 'ln2_b', 'b_fc', 'b_proj')


def setup_inputs(seed: int = 0) -> dict:
    key_list = jax.random.split(jax.random.key(seed), 21)
    d_model = MODEL_WIDTH
    mlp_width = MLP_WIDTH

    def draw_normal(index, shape, scale):
        return jax.random.normal(key_list[index], shape, jnp.float32) * scale

    def gain_vec(index):
        return 1.0 + draw_normal(index, (d_model,), 0.2)

    row_keys = jax.random.split(key_list[1], BATCH_SIZE)
    perm_rows = jax.vmap(lambda row_key: jax.random.permutation(row_key, NUM_PATCHES))(row_keys)
    return {
        'patches': draw_normal(0, (BATCH_SIZE, NUM_PATCHES, PATCH_PIXELS), 1.0).astype(jnp.bfloat16),
        'keep': perm_rows[:, :NUM_KEEP].astype(jnp.int32),
        'w_patch': draw_normal(2, (PATCH_PIXELS, d_model), PATCH_PIXELS ** -0.5),
        'b_patch': draw_normal(3, (d_model,), 0.3),
        'pos_table': draw_normal(4, (NUM_PATCHES + 1, d_model), 0.5),
        'cls_tok': draw_normal(5, (d_model,), 1.0),
        'lnp_g': gain_vec(6),
        'lnp_b': draw_normal(7, (d_model,), 0.2),
        'ln1_g': gain_vec(8),
        'ln1_b': draw_normal(9, (d_model,), 0.2),
        'w_qkv': draw_normal(10, (d_model, 3, NUM_HEADS, HEAD_DIM), d_model ** -0.5),
        'b_qkv': draw_normal(11, (3 * d_model,), 0.3),
        'w_out': draw_normal(12, (d_model, d_model), d_model ** -0.5),
        'b_out': draw_normal(13, (d_model,), 0.3),
        'ln2_g': gain_vec(14),
        'ln2_b': draw_normal(15, (d_model,), 0.2),
        'w_fc': draw_normal(16, (d_model, mlp_width), d_model ** -0.5),
        'b_fc': draw_normal(17, (mlp_width,), 0.3),
        'w_proj': draw_normal(18, (mlp_width, d_model), mlp_width ** -0.5),
        'b_proj': draw_normal(19, (d_model,), 0.3),
        'grad_h1': draw_normal(20, (BATCH_SIZE, TOKENS, d_model), (BATCH_SIZE * TOKENS) ** -0.5).astype(jnp.bfloat16),
    }


def product(einsum_form, left_op, right_op):
    return jnp.einsum(einsum_form, left_op.astype(jnp.float32), right_op.astype(jnp.float32))


def norm_forward(x_in, gain_f, shift_f):
    centered = x_in - jnp.mean(x_in, axis=-1, keepdims=True)
    inv_std = lax.rsqrt(jnp.mean(centered * centered, axis=-1, keepdims=True) + LN_EPS)
    x_hat = centered * inv_std
    return x_hat * gain_f + shift_f, x_hat, inv_std


def norm_backward(d_norm, x_hat, inv_std, gain_f):
    d_hat = d_norm * gain_f
    d_in = inv_std * (d_hat - jnp.mean(d_hat, axis=-1, keepdims=True) - x_hat * jnp.mean(d_hat * x_hat, axis=-1, keepdims=True))
    return d_in, jnp.sum(d_norm * x_hat, axis=(0, 1)), jnp.sum(d_norm, axis=(0, 1))


def gelu_slope(pre_act):
    return 0.5 * (1.0 + lax.erf(pre_act * INV_SQRT2)) + pre_act * jnp.exp(-0.5 * pre_act * pre_act) * INV_SQRT_2PI


def forward(full_w, patches, keep):
    n_img = patches.shape[0]
    d_model = full_w['w_out'].shape[0]
    n_heads, head_dim = full_w['w_qkv'].shape[2], full_w['w_qkv'].shape[3]
    logit_scale = head_dim ** -0.5
    as_f32 = {name: full_w[name].astype(jnp.float32) for name in VECTOR_NAMES}
    kept_rows = jnp.take_along_axis(patches, keep[:, :, None], axis=1)
    embed_rows = product('bkq,qw->bkw', kept_rows, full_w['w_patch']) + as_f32['b_patch'] + full_w['pos_table'][1 + keep].astype(jnp.float32)
    head_row = as_f32['cls_tok'] + full_w['pos_table'][0].astype(jnp.float32)
    x_zero = jnp.concatenate([jnp.broadcast_to(head_row, (n_img, 1, d_model)), embed_rows], axis=1)
    h_zero, hat_p, inv_p = norm_forward(x_zero, as_f32['lnp_g'], as_f32['lnp_b'])
    y_one, hat_1, inv_1 = norm_forward(h_zero, as_f32['ln1_g'], as_f32['ln1_b'])
    a_in = y_one.astype(jnp.bfloat16)
    qkv_all = (product('btw,wchd->btchd', a_in, full_w['w_qkv']) + as_f32['b_qkv'].reshape(3, n_heads, head_dim)).astype(jnp.bfloat16)
    q_heads, k_heads, v_heads = qkv_all[:, :, 0], qkv_all[:, :, 1], qkv_all[:, :, 2]
    attn_prob = jax.nn.softmax(product('bqhd,bkhd->bhqk', q_heads, k_heads) * logit_scale, axis=-1)
    prob_b = attn_prob.astype(jnp.bfloat16)
    context = product('bhqk,bkhd->bqhd', prob_b, v_heads).astype(jnp.bfloat16)
    h_mid = h_zero + product('bqhd,hdw->bqw', context, full_w['w_out'].reshape(n_heads, head_dim, d_model)) + as_f32['b_out']
    y_two, hat_2, inv_2 = norm_forward(h_mid, as_f32['ln2_g'], as_f32['ln2_b'])
    c_in = y_two.astype(jnp.bfloat16)
    pre_act = product('btw,wf->btf', c_in, full_w['w_fc']) + as_f32['b_fc']
    gelu_out = jax.nn.gelu(pre_act, approximate=False).astype(jnp.bfloat16)
    h_one = (h_mid + product('btf,fw->btw', gelu_out, full_w['w_proj']) + as_f32['b_proj']).astype(jnp.bfloat16)
    saved = dict(keep=keep, kept_rows=kept_rows, hat_p=hat_p, inv_p=inv_p, hat_1=hat_1, inv_1=inv_1, a_in=a_in, q_heads=q_heads, k_heads=k_heads, v_heads=v_heads, attn_prob=attn_prob, prob_b=prob_b, context=context, hat_2=hat_2, inv_2=inv_2, c_in=c_in, pre_act=pre_act, gelu_out=gelu_out)
    return h_one, saved


def backward(weights, saved, grad_h1):
    d_model = weights['w_out'].shape[0]
    n_heads, head_dim = weights['w_qkv'].shape[2], weights['w_qkv'].shape[3]
    logit_scale = head_dim ** -0.5
    w_out3 = weights['w_out'].reshape(n_heads, head_dim, d_model)
    d_h = grad_h1.astype(jnp.float32)
    g_w_proj = product('btf,btw->fw', saved['gelu_out'], grad_h1)
    d_pre = product('btw,fw->btf', grad_h1, weights['w_proj']) * gelu_slope(saved['pre_act'])
    d_pre_b = d_pre.astype(jnp.bfloat16)
    g_w_fc = product('btw,btf->wf', saved['c_in'], d_pre_b)
    d_c = product('btf,wf->btw', d_pre_b, weights['w_fc'])
    d_norm2, g_ln2_g, g_ln2_b = norm_backward(d_c, saved['hat_2'], saved['inv_2'], weights['ln2_g'].astype(jnp.float32))
    d_mid = d_norm2 + d_h
    d_mid_b = d_mid.astype(jnp.bfloat16)
    g_w_out = product('bqhd,bqw->hdw', saved['context'], d_mid_b).reshape(d_model, d_model)
    d_ctx = product('bqw,hdw->bqhd', d_mid_b, w_out3).astype(jnp.bfloat16)
    g_v = product('bhqk,bqhd->bkhd', saved['prob_b'], d_ctx)
    d_prob = product('bqhd,bkhd->bhqk', d_ctx, saved['v_heads'])
    attn_prob = saved['attn_prob']
    d_logit = (attn_prob * (d_prob - jnp.sum(attn_prob * d_prob, axis=-1, keepdims=True)) * logit_scale).astype(jnp.bfloat16)
    g_q = product('bhqk,bkhd->bqhd', d_logit, saved['k_heads'])
    g_k = product('bhqk,bqhd->bkhd', d_logit, saved['q_heads'])
    d_qkv = jnp.stack([g_q, g_k, g_v], axis=2)
    d_qkv_b = d_qkv.astype(jnp.bfloat16)
    g_w_qkv = product('btw,btchd->wchd', saved['a_in'], d_qkv_b)
    d_a = product('btchd,wchd->btw', d_qkv_b, weights['w_qkv'])
    d_norm1, g_ln1_g, g_ln1_b = norm_backward(d_a, saved['hat_1'], saved['inv_1'], weights['ln1_g'].astype(jnp.float32))
    d_zero = d_norm1 + d_mid
    d_x, g_lnp_g, g_lnp_b = norm_backward(d_zero, saved['hat_p'], saved['inv_p'], weights['lnp_g'].astype(jnp.float32))
    d_head = jnp.sum(d_x[:, 0], axis=0)
    d_emb = d_x[:, 1:]
    d_emb_b = d_emb.astype(jnp.bfloat16)
    pos_rest = jax.ops.segment_sum(d_emb_b.astype(jnp.float32).reshape(-1, d_model), saved['keep'].reshape(-1), num_segments=NUM_PATCHES)
    g_pos = jnp.concatenate([d_head[None], pos_rest], axis=0)
    return dict(w_patch=product('bkq,bkw->qw', saved['kept_rows'], d_emb_b), b_patch=jnp.sum(d_emb, axis=(0, 1)), pos_table=g_pos, cls_tok=d_head, lnp_g=g_lnp_g, lnp_b=g_lnp_b, ln1_g=g_ln1_g, ln1_b=g_ln1_b, w_qkv=g_w_qkv, b_qkv=jnp.sum(d_qkv, axis=(0, 1)).reshape(-1), w_out=g_w_out, b_out=jnp.sum(d_mid, axis=(0, 1)), ln2_g=g_ln2_g, ln2_b=g_ln2_b, w_fc=g_w_fc, b_fc=jnp.sum(d_pre, axis=(0, 1)), w_proj=g_w_proj, b_proj=jnp.sum(d_h, axis=(0, 1)))


def reference(patches, keep, w_patch, b_patch, pos_table, cls_tok, lnp_g, lnp_b, ln1_g, ln1_b, w_qkv, b_qkv, w_out, b_out, ln2_g, ln2_b, w_fc, b_fc, w_proj, b_proj, grad_h1):
    masters = (w_patch, b_patch, pos_table, cls_tok, lnp_g, lnp_b, ln1_g, ln1_b, w_qkv, b_qkv, w_out, b_out, ln2_g, ln2_b, w_fc, b_fc, w_proj, b_proj)
    full_w = {name: value.astype(jnp.bfloat16) for name, value in zip(PARAM_NAMES, masters)}
    n_blocks = BATCH_SIZE // BLOCK_IMAGES

    def split_blocks(array_in):
        return array_in.reshape((n_blocks, BLOCK_IMAGES) + array_in.shape[1:])

    def scan_step(running, block_in):
        h_one, saved = forward(full_w, block_in[0], block_in[1])
        grad_map = backward(full_w, saved, block_in[2])
        return {name: running[name] + grad_map[name] for name in PARAM_NAMES}, h_one

    zero_grads = {name: jnp.zeros(value.shape, jnp.float32) for name, value in zip(PARAM_NAMES, masters)}
    totals, h_blocks = lax.scan(scan_step, zero_grads, (split_blocks(patches), split_blocks(keep), split_blocks(grad_h1)))
    h_out = h_blocks.reshape(BATCH_SIZE, TOKENS, MODEL_WIDTH)
    return (h_out, totals['w_patch'], totals['b_patch'], totals['pos_table'], totals['cls_tok'], totals['lnp_g'], totals['lnp_b'], totals['ln1_g'], totals['ln1_b'], totals['w_qkv'], totals['b_qkv'], totals['w_out'], totals['b_out'], totals['ln2_g'], totals['ln2_b'], totals['w_fc'], totals['b_fc'], totals['w_proj'], totals['b_proj'])
```

```python
import jax
import jax.numpy as jnp
from jax import lax
from jax.experimental import pallas as pl
from jax.experimental.pallas import tpu as pltpu
from jax.sharding import PartitionSpec as P

MESH_AXIS = 'fsdp'
LN_EPS = 1e-5
INV_SQRT2 = 0.7071067811865476
INV_SQRT_2PI = 0.3989422804014327
PARAM_NAMES = ('w_patch', 'b_patch', 'pos_table', 'cls_tok', 'lnp_g', 'lnp_b', 'ln1_g', 'ln1_b', 'w_qkv', 'b_qkv', 'w_out', 'b_out', 'ln2_g', 'ln2_b', 'w_fc', 'b_fc', 'w_proj', 'b_proj')
VECTOR_NAMES = ('b_patch', 'cls_tok', 'lnp_g', 'lnp_b', 'ln1_g', 'ln1_b', 'b_qkv', 'b_out', 'ln2_g', 'ln2_b', 'b_fc', 'b_proj')
LAST_SPLIT = ('w_patch', 'pos_table')


def product(einsum_form, left_op, right_op):
    return jnp.einsum(einsum_form, left_op, right_op, preferred_element_type=jnp.float32)


def norm_forward(x_in, gain_f, shift_f):
    centered = x_in - jnp.mean(x_in, axis=-1, keepdims=True)
    inv_std = lax.rsqrt(jnp.mean(centered * centered, axis=-1, keepdims=True) + LN_EPS)
    x_hat = centered * inv_std
    return x_hat * gain_f + shift_f, x_hat, inv_std


def norm_backward(d_norm, x_hat, inv_std, gain_f):
    d_hat = d_norm * gain_f
    d_in = inv_std * (d_hat - jnp.mean(d_hat, axis=-1, keepdims=True) - x_hat * jnp.mean(d_hat * x_hat, axis=-1, keepdims=True))
    return d_in, jnp.sum(d_norm * x_hat, axis=(0, 1)), jnp.sum(d_norm, axis=(0, 1))


def gelu_slope(pre_act):
    return 0.5 * (1.0 + lax.erf(pre_act * INV_SQRT2)) + pre_act * jnp.exp(-0.5 * pre_act * pre_act) * INV_SQRT_2PI


def forward(full_w, patches, keep):
    n_img, n_patch = patches.shape[0], patches.shape[1]
    d_model = full_w['w_out'].shape[0]
    n_heads, head_dim = full_w['w_qkv'].shape[2], full_w['w_qkv'].shape[3]
    logit_scale = head_dim ** -0.5
    as_f32 = {name: full_w[name].astype(jnp.float32) for name in VECTOR_NAMES}
    onehot_keep = (keep[:, :, None] == lax.broadcasted_iota(jnp.int32, (1, 1, n_patch), 2)).astype(jnp.bfloat16)
    kept_rows = product('bkp,bpq->bkq', onehot_keep, patches).astype(jnp.bfloat16)
    embed_rows = (product('bkq,qw->bkw', kept_rows, full_w['w_patch']) + as_f32['b_patch']
                  + product('bkp,pw->bkw', onehot_keep, full_w['pos_table'][1:]))
    head_row = as_f32['cls_tok'] + full_w['pos_table'][0].astype(jnp.float32)
    x_zero = jnp.concatenate([jnp.broadcast_to(head_row, (n_img, 1, d_model)), embed_rows], axis=1)
    h_zero, hat_p, inv_p = norm_forward(x_zero, as_f32['lnp_g'], as_f32['lnp_b'])
    y_one, hat_1, inv_1 = norm_forward(h_zero, as_f32['ln1_g'], as_f32['ln1_b'])
    a_in = y_one.astype(jnp.bfloat16)
    qkv_all = (product('btw,wchd->btchd', a_in, full_w['w_qkv']) + as_f32['b_qkv'].reshape(3, n_heads, head_dim)).astype(jnp.bfloat16)
    q_heads, k_heads, v_heads = qkv_all[:, :, 0], qkv_all[:, :, 1], qkv_all[:, :, 2]
    attn_prob = jax.nn.softmax(product('bqhd,bkhd->bhqk', q_heads, k_heads) * logit_scale, axis=-1)
    prob_b = attn_prob.astype(jnp.bfloat16)
    context = product('bhqk,bkhd->bqhd', prob_b, v_heads).astype(jnp.bfloat16)
    h_mid = h_zero + product('bqhd,hdw->bqw', context, full_w['w_out'].reshape(n_heads, head_dim, d_model)) + as_f32['b_out']
    y_two, hat_2, inv_2 = norm_forward(h_mid, as_f32['ln2_g'], as_f32['ln2_b'])
    c_in = y_two.astype(jnp.bfloat16)
    pre_act = product('btw,wf->btf', c_in, full_w['w_fc']) + as_f32['b_fc']
    gelu_out = jax.nn.gelu(pre_act, approximate=False).astype(jnp.bfloat16)
    h_one = (h_mid + product('btf,fw->btw', gelu_out, full_w['w_proj']) + as_f32['b_proj']).astype(jnp.bfloat16)
    saved = dict(onehot_keep=onehot_keep, kept_rows=kept_rows, hat_p=hat_p, inv_p=inv_p, hat_1=hat_1, inv_1=inv_1, a_in=a_in, q_heads=q_heads, k_heads=k_heads, v_heads=v_heads, attn_prob=attn_prob, prob_b=prob_b, context=context, hat_2=hat_2, inv_2=inv_2, c_in=c_in, pre_act=pre_act, gelu_out=gelu_out)
    return h_one, saved


def backward(weights, saved, grad_h1):
    d_model = weights['w_out'].shape[0]
    n_heads, head_dim = weights['w_qkv'].shape[2], weights['w_qkv'].shape[3]
    logit_scale = head_dim ** -0.5
    w_out3 = weights['w_out'].reshape(n_heads, head_dim, d_model)
    d_h = grad_h1.astype(jnp.float32)
    g_w_proj = product('btf,btw->fw', saved['gelu_out'], grad_h1)
    d_pre = product('btw,fw->btf', grad_h1, weights['w_proj']) * gelu_slope(saved['pre_act'])
    d_pre_b = d_pre.astype(jnp.bfloat16)
    g_w_fc = product('btw,btf->wf', saved['c_in'], d_pre_b)
    d_c = product('btf,wf->btw', d_pre_b, weights['w_fc'])
    d_norm2, g_ln2_g, g_ln2_b = norm_backward(d_c, saved['hat_2'], saved['inv_2'], weights['ln2_g'].astype(jnp.float32))
    d_mid = d_norm2 + d_h
    d_mid_b = d_mid.astype(jnp.bfloat16)
    g_w_out = product('bqhd,bqw->hdw', saved['context'], d_mid_b).reshape(d_model, d_model)
    d_ctx = product('bqw,hdw->bqhd', d_mid_b, w_out3).astype(jnp.bfloat16)
    g_v = product('bhqk,bqhd->bkhd', saved['prob_b'], d_ctx)
    d_prob = product('bqhd,bkhd->bhqk', d_ctx, saved['v_heads'])
    attn_prob = saved['attn_prob']
    d_logit = (attn_prob * (d_prob - jnp.sum(attn_prob * d_prob, axis=-1, keepdims=True)) * logit_scale).astype(jnp.bfloat16)
    g_q = product('bhqk,bkhd->bqhd', d_logit, saved['k_heads'])
    g_k = product('bhqk,bqhd->bkhd', d_logit, saved['q_heads'])
    d_qkv = jnp.stack([g_q, g_k, g_v], axis=2)
    d_qkv_b = d_qkv.astype(jnp.bfloat16)
    g_w_qkv = product('btw,btchd->wchd', saved['a_in'], d_qkv_b)
    d_a = product('btchd,wchd->btw', d_qkv_b, weights['w_qkv'])
    d_norm1, g_ln1_g, g_ln1_b = norm_backward(d_a, saved['hat_1'], saved['inv_1'], weights['ln1_g'].astype(jnp.float32))
    d_zero = d_norm1 + d_mid
    d_x, g_lnp_g, g_lnp_b = norm_backward(d_zero, saved['hat_p'], saved['inv_p'], weights['lnp_g'].astype(jnp.float32))
    d_head = jnp.sum(d_x[:, 0], axis=0)
    d_emb = d_x[:, 1:]
    d_emb_b = d_emb.astype(jnp.bfloat16)
    g_pos = jnp.concatenate([d_head[None], product('bkp,bkw->pw', saved['onehot_keep'], d_emb_b)], axis=0)
    return dict(w_patch=product('bkq,bkw->qw', saved['kept_rows'], d_emb_b), b_patch=jnp.sum(d_emb, axis=(0, 1)), pos_table=g_pos, cls_tok=d_head, lnp_g=g_lnp_g, lnp_b=g_lnp_b, ln1_g=g_ln1_g, ln1_b=g_ln1_b, w_qkv=g_w_qkv, b_qkv=jnp.sum(d_qkv, axis=(0, 1)).reshape(-1), w_out=g_w_out, b_out=jnp.sum(d_mid, axis=(0, 1)), ln2_g=g_ln2_g, ln2_b=g_ln2_b, w_fc=g_w_fc, b_fc=jnp.sum(d_pre, axis=(0, 1)), w_proj=g_w_proj, b_proj=jnp.sum(d_h, axis=(0, 1)))


RINGS = (
    (0, 4, 8, 10, 11, 15, 14, 12, 13, 9, 5, 7, 6, 2, 3, 1),
    (0, 2, 3, 7, 11, 9, 8, 12, 13, 15, 14, 10, 6, 4, 5, 1),
    (0, 1, 3, 7, 5, 4, 8, 9, 11, 15, 13, 12, 14, 10, 6, 2),
    (0, 1, 5, 7, 3, 2, 6, 10, 14, 15, 11, 9, 13, 12, 8, 4),
    (0, 4, 6, 7, 11, 10, 8, 12, 14, 15, 13, 9, 5, 1, 3, 2),
    (0, 2, 6, 7, 3, 1, 5, 9, 13, 15, 11, 10, 14, 12, 8, 4),
)
N_CHIP = 16
MESH_ID = pl.DeviceIdType.MESH
ARRAYS = ((32, 4096), (128, 1024), (32, 3072), (32, 1024), (32, 1024))
FC, PROJ, QKV, OUT, MISC = range(5)
GATHER_STREAMS = (
    (MISC, 0, 32, 0, 256, 0), (MISC, 0, 32, 256, 256, 1), (MISC, 0, 32, 512, 256, 2), (MISC, 0, 32, 768, 256, 3),
    (QKV, 0, 32, 0, 2048, 4), (QKV, 0, 32, 2048, 1024, 5), (OUT, 0, 32, 0, 1024, 5),
    (FC, 0, 32, 0, 2048, 0), (FC, 0, 32, 2048, 2048, 1), (PROJ, 0, 64, 0, 1024, 2), (PROJ, 64, 64, 0, 1024, 3),
)
REDUCE_STREAMS = (
    (FC, 0, 64, 0, 1024, 0), (FC, 0, 64, 1024, 1024, 1), (PROJ, 0, 128, 0, 512, 2), (PROJ, 128, 128, 0, 512, 3),
    (QKV, 0, 64, 0, 1024, 4), (QKV, 0, 64, 1024, 512, 5), (OUT, 0, 64, 0, 512, 5),
    (MISC, 0, 64, 0, 128, 0), (MISC, 0, 64, 128, 128, 1), (MISC, 0, 64, 256, 128, 2), (MISC, 0, 64, 384, 128, 3),
)


def pick(table, index):
    value = jnp.int32(table[0])
    for place in range(1, len(table)):
        value = jnp.where(index == place, jnp.int32(table[place]), value)
    return value


class Place:
    def __init__(self):
        me = lax.axis_index(MESH_AXIS)
        self.core = lax.rem(me, 2)
        self.chip = lax.div(me, 2)
        self.sibling = me + 1 - 2 * self.core
        where_in = [[ring.index(chip) for chip in range(N_CHIP)] for ring in RINGS]
        self.spot = [pick(table, self.chip) for table in where_in]
        self.after = [2 * pick([ring[(table[chip] + 1) % N_CHIP] for chip in range(N_CHIP)], self.chip) + self.core
                      for ring, table in zip(RINGS, where_in)]
        self.before = [2 * pick([ring[(table[chip] - 1) % N_CHIP] for chip in range(N_CHIP)], self.chip) + self.core
                       for ring, table in zip(RINGS, where_in)]

    def chips_back(self, steps):
        return [pick(ring, lax.rem(self.spot[k] + 2 * N_CHIP - steps, N_CHIP)) for k, ring in enumerate(RINGS)]

    def meet(self):
        barrier = pltpu.get_barrier_semaphore()
        for other in self.after + self.before + [self.sibling]:
            pl.semaphore_signal(barrier, inc=1, device_id=(other,), device_id_type=MESH_ID)
        pl.semaphore_wait(barrier, 2 * len(RINGS) + 1)


def gather_kernel(*refs):
    shards, wholes = refs[:5], refs[5:10]
    own_sem, send_sem, recv_sem, twin_send, twin_recv = refs[10:]
    place = Place()

    def block(i, chip, core):
        arr, row, rows, col, cols, _ = GATHER_STREAMS[i]
        first = (2 * chip + core) * ARRAYS[arr][0] + row
        return wholes[arr].at[pl.ds(pl.multiple_of(first, 32), rows), pl.ds(col, cols)]

    def remote(src, dst, sems, i, step, device):
        return pltpu.make_async_remote_copy(src_ref=src, dst_ref=dst, send_sem=sems[0].at[i, step], recv_sem=sems[1].at[i, step],
                                            device_id=(device,), device_id_type=MESH_ID)

    place.meet()
    n_streams = len(GATHER_STREAMS)
    for i in range(n_streams):
        arr, row, rows, col, cols, k = GATHER_STREAMS[i]
        mine = shards[arr].at[pl.ds(row, rows), pl.ds(col, cols)]
        here = block(i, place.chip, place.core)
        remote(mine, here, (send_sem, recv_sem), i, 0, place.after[k]).start()
        remote(mine, here, (twin_send, twin_recv), i, 0, place.sibling).start()
    for arr in range(5):
        rows = ARRAYS[arr][0]
        first = pl.multiple_of((2 * place.chip + place.core) * rows, 32)
        pltpu.make_async_copy(shards[arr], wholes[arr].at[pl.ds(first, rows), :], own_sem.at[arr]).start()

    def ring_step(step, carry):
        chips = place.chips_back(step)
        for i in range(n_streams):
            k = GATHER_STREAMS[i][5]
            here = block(i, chips[k], place.core)
            remote(here, here, (send_sem, recv_sem), i, step - 1, place.after[k]).wait_recv()

            @pl.when(step < N_CHIP - 1)
            def _():
                remote(here, here, (send_sem, recv_sem), i, step, place.after[k]).start()

            remote(here, here, (twin_send, twin_recv), i, step, place.sibling).start()
        return carry

    lax.fori_loop(1, N_CHIP, ring_step, 0)

    def drain(step, carry):
        chips = place.chips_back(step)
        for i in range(n_streams):
            k = GATHER_STREAMS[i][5]
            here = block(i, chips[k], place.core)
            there = block(i, chips[k], 1 - place.core)

            @pl.when(step < N_CHIP - 1)
            def _():
                remote(here, here, (send_sem, recv_sem), i, step, place.after[k]).wait_send()

            remote(here, here, (twin_send, twin_recv), i, step, place.sibling).wait_send()
            remote(there, there, (twin_send, twin_recv), i, step, place.sibling).wait_recv()
        return carry

    lax.fori_loop(0, N_CHIP, drain, 0)
    for arr in range(5):
        rows = ARRAYS[arr][0]
        first = pl.multiple_of((2 * place.chip + place.core) * rows, 32)
        pltpu.make_async_copy(shards[arr], wholes[arr].at[pl.ds(first, rows), :], own_sem.at[arr]).wait()


def gather_all(shards):
    n_streams = len(GATHER_STREAMS)
    ring_sems, twin_sems = pltpu.SemaphoreType.DMA((n_streams, N_CHIP - 1)), pltpu.SemaphoreType.DMA((n_streams, N_CHIP))
    return pl.pallas_call(
        gather_kernel,
        out_shape=[jax.ShapeDtypeStruct((2 * N_CHIP * rows, cols), jnp.bfloat16) for rows, cols in ARRAYS],
        in_specs=[pl.BlockSpec(memory_space=pltpu.VMEM)] * 5,
        out_specs=[pl.BlockSpec(memory_space=pl.ANY)] * 5,
        scratch_shapes=[pltpu.SemaphoreType.DMA((5,)), ring_sems, ring_sems, twin_sems, twin_sems],
        compiler_params=pltpu.CompilerParams(collective_id=0, has_side_effects=True),
        name='gather_all',
    )(*shards)


def reduce_kernel(*refs):
    grads, outs = refs[:5], refs[5:10]
    accs, owns, twins = refs[10:15], refs[15:20], refs[20:25]
    own_sem, twin_send, twin_recv, send_sem, recv_sem, ring_free, twin_free, end_own, end_send, end_recv = refs[25:]
    place = Place()
    n_streams = len(REDUCE_STREAMS)

    def part(i, ref, slot):
        _, row, rows, col, cols, _ = REDUCE_STREAMS[i]
        return ref.at[slot, pl.ds(row, rows), pl.ds(col, cols)]

    def source(i, chip, core):
        arr, row, rows, col, cols, _ = REDUCE_STREAMS[i]
        half = ARRAYS[arr][1] // 2
        first = pl.multiple_of(2 * chip * ARRAYS[arr][0] + row, 64)
        return grads[arr].at[pl.ds(first, rows), pl.ds(pl.multiple_of(core * half + col, 128), cols)]

    def load(i, chip, slot):
        return pltpu.make_async_copy(source(i, chip, place.core), part(i, owns[REDUCE_STREAMS[i][0]], slot), own_sem.at[i, slot])

    def push(i, chip, slot):
        return pltpu.make_async_remote_copy(src_ref=source(i, chip, 1 - place.core), dst_ref=part(i, twins[REDUCE_STREAMS[i][0]], slot),
                                            send_sem=twin_send.at[i, slot], recv_sem=twin_recv.at[i, slot],
                                            device_id=(place.sibling,), device_id_type=MESH_ID)

    def pass_on(i, slot, slot_next):
        arr, k = REDUCE_STREAMS[i][0], REDUCE_STREAMS[i][5]
        return pltpu.make_async_remote_copy(src_ref=part(i, accs[arr], slot), dst_ref=part(i, accs[arr], slot_next),
                                            send_sem=send_sem.at[i, slot], recv_sem=recv_sem.at[i, slot_next],
                                            device_id=(place.after[k],), device_id_type=MESH_ID)

    place.meet()
    for step in range(2):
        chips = place.chips_back(step + 1)
        for i in range(n_streams):
            load(i, chips[REDUCE_STREAMS[i][5]], step).start()
            push(i, chips[REDUCE_STREAMS[i][5]], step).start()

    def ring_step(step, carry):
        slot, pair = lax.rem(step, 3), lax.rem(step, 2)
        slot_next, slot_last = lax.rem(step + 1, 3), lax.rem(step + 2, 3)
        chips = place.chips_back(step + 3)
        for i in range(n_streams):
            arr, row, rows, col, cols, k = REDUCE_STREAMS[i]
            load(i, chips[k], pair).wait()
            push(i, chips[k], pair).wait_recv()

            @pl.when(step == 0)
            def _():
                def add_two(r, c):
                    at = pl.ds(pl.multiple_of(row + 8 * r, 8), 8)
                    lanes = pl.ds(col, cols)
                    accs[arr][slot, at, lanes] = owns[arr][pair, at, lanes] + twins[arr][pair, at, lanes]
                    return c
                lax.fori_loop(0, rows // 8, add_two, 0)

            @pl.when(step > 0)
            def _():
                pass_on(i, slot, slot).wait_recv()

                def add_three(r, c):
                    at = pl.ds(pl.multiple_of(row + 8 * r, 8), 8)
                    lanes = pl.ds(col, cols)
                    accs[arr][slot, at, lanes] = accs[arr][slot, at, lanes] + (owns[arr][pair, at, lanes] + twins[arr][pair, at, lanes])
                    return c
                lax.fori_loop(0, rows // 8, add_three, 0)

            @pl.when(jnp.logical_and(step >= 2, step < N_CHIP - 1))
            def _():
                pl.semaphore_wait(ring_free.at[i], 1)

            @pl.when(step < N_CHIP - 1)
            def _():
                pass_on(i, slot, slot_next).start()

            @pl.when(step < N_CHIP - 2)
            def _():
                pl.semaphore_signal(twin_free.at[i], inc=1, device_id=(place.sibling,), device_id_type=MESH_ID)
                load(i, chips[k], pair).start()

        for i in range(n_streams):
            k = REDUCE_STREAMS[i][5]
            push(i, chips[k], pair).wait_send()

            @pl.when(step < N_CHIP - 2)
            def _():
                pl.semaphore_wait(twin_free.at[i], 1)
                push(i, chips[k], pair).start()

            @pl.when(step >= 1)
            def _():
                pass_on(i, slot_last, slot).wait_send()

            @pl.when(jnp.logical_and(step >= 1, step < N_CHIP - 2))
            def _():
                pl.semaphore_signal(ring_free.at[i], inc=1, device_id=(place.before[k],), device_id_type=MESH_ID)
        return carry

    lax.fori_loop(0, N_CHIP, ring_step, 0)
    last = (N_CHIP - 1) % 3

    def end_copies(arr):
        rows, half = ARRAYS[arr][0], ARRAYS[arr][1] // 2
        target = outs[arr].at[:, pl.ds(pl.multiple_of(place.core * half, 128), half)]
        keep_rows = accs[arr].at[last, pl.ds(pl.multiple_of(place.core * rows, 32), rows), :]
        give_rows = accs[arr].at[last, pl.ds(pl.multiple_of((1 - place.core) * rows, 32), rows), :]
        return (pltpu.make_async_copy(keep_rows, target, end_own.at[arr]),
                pltpu.make_async_remote_copy(src_ref=give_rows, dst_ref=target, send_sem=end_send.at[arr], recv_sem=end_recv.at[arr],
                                             device_id=(place.sibling,), device_id_type=MESH_ID))

    for arr in range(5):
        local, cross = end_copies(arr)
        local.start()
        cross.start()
    for arr in range(5):
        local, cross = end_copies(arr)
        local.wait()
        cross.wait()


def reduce_all(grads):
    n_streams = len(REDUCE_STREAMS)
    slots = lambda n: [pltpu.VMEM((n, 2 * rows, cols // 2), jnp.float32) for rows, cols in ARRAYS]
    sems = lambda n: pltpu.SemaphoreType.DMA((n_streams, n))
    return pl.pallas_call(
        reduce_kernel,
        out_shape=[jax.ShapeDtypeStruct((rows, cols), jnp.float32) for rows, cols in ARRAYS],
        in_specs=[pl.BlockSpec(memory_space=pl.ANY)] * 5,
        out_specs=[pl.BlockSpec(memory_space=pl.ANY)] * 5,
        scratch_shapes=slots(3) + slots(2) + slots(2) + [
            sems(2), sems(2), sems(2), sems(3), sems(3),
            pltpu.SemaphoreType.REGULAR((n_streams,)), pltpu.SemaphoreType.REGULAR((n_streams,)),
            pltpu.SemaphoreType.DMA((5,)), pltpu.SemaphoreType.DMA((5,)), pltpu.SemaphoreType.DMA((5,)),
        ],
        compiler_params=pltpu.CompilerParams(collective_id=1, has_side_effects=True),
        name='reduce_all',
    )(*grads)


ROW_VECTORS = ('b_patch', 'cls_tok', 'lnp_g', 'lnp_b', 'ln1_g', 'ln1_b', 'b_out', 'ln2_g', 'ln2_b', 'b_proj')
N_PIXEL, N_POS = 768, 197
MISC_USED = N_PIXEL + N_POS + len(ROW_VECTORS) + 3 + 4


def solution(mesh):
    def spec_of(name):
        return P(None, MESH_AXIS) if name in LAST_SPLIT else P(MESH_AXIS)

    def pack_misc(part):
        rows = part['w_patch'].shape[1]
        columns = [part['w_patch'].T, part['pos_table'].T] + [part[name][:, None] for name in ROW_VECTORS]
        columns += [part['b_qkv'].reshape(rows, 3), part['b_fc'].reshape(rows, 4)]
        return jnp.pad(jnp.concatenate(columns, axis=1), ((0, 0), (0, 1024 - MISC_USED)))

    def unpack_misc(misc):
        part = {'w_patch': misc[:, :N_PIXEL].T, 'pos_table': misc[:, N_PIXEL:N_PIXEL + N_POS].T}
        first = N_PIXEL + N_POS
        for name in ROW_VECTORS:
            part[name] = misc[:, first]
            first += 1
        part['b_qkv'] = misc[:, first:first + 3].reshape(-1)
        part['b_fc'] = misc[:, first + 3:first + 7].reshape(-1)
        return part

    def local_step(patches, keep, *rest):
        shards = dict(zip(PARAM_NAMES, rest[:-1]))
        grad_h1 = rest[-1]
        n_rows, _, n_heads, head_dim = shards['w_qkv'].shape
        casts = {name: shards[name].astype(jnp.bfloat16) for name in PARAM_NAMES}
        w_fc, w_proj, w_qkv, w_out, misc = gather_all((casts['w_fc'], casts['w_proj'], casts['w_qkv'].reshape(n_rows, -1), casts['w_out'], pack_misc(casts)))
        full_w = unpack_misc(misc)
        full_w.update(w_fc=w_fc, w_proj=w_proj, w_qkv=w_qkv.reshape(-1, 3, n_heads, head_dim), w_out=w_out)
        h_one, saved = forward(full_w, patches, keep)
        grad_map = backward(full_w, saved, grad_h1)
        d_model = w_out.shape[0]
        sums = reduce_all((grad_map['w_fc'], grad_map['w_proj'], grad_map['w_qkv'].reshape(d_model, -1), grad_map['w_out'], pack_misc(grad_map)))
        own = unpack_misc(sums[MISC])
        own.update(w_fc=sums[FC], w_proj=sums[PROJ], w_qkv=sums[QKV].reshape(n_rows, 3, n_heads, head_dim), w_out=sums[OUT])
        return (h_one,) + tuple(own[name] for name in PARAM_NAMES)

    batch_spec = P(MESH_AXIS)
    param_specs = tuple(spec_of(name) for name in PARAM_NAMES)
    return jax.shard_map(local_step, mesh=mesh, in_specs=(batch_spec, batch_spec) + param_specs + (batch_spec,), out_specs=(batch_spec,) + param_specs, check_vma=False)
```

```python
import jax
import jax.numpy as jnp
from jax import lax
from jax.experimental import pallas as pl
from jax.experimental.pallas import tpu as pltpu
from jax.sharding import PartitionSpec as P

MESH_AXIS = 'fsdp'
LN_EPS = 1e-5
INV_SQRT2 = 0.7071067811865476
INV_SQRT_2PI = 0.3989422804014327
PARAM_NAMES = ('w_patch', 'b_patch', 'pos_table', 'cls_tok', 'lnp_g', 'lnp_b', 'ln1_g', 'ln1_b', 'w_qkv', 'b_qkv', 'w_out', 'b_out', 'ln2_g', 'ln2_b', 'w_fc', 'b_fc', 'w_proj', 'b_proj')
LAST_SPLIT = ('w_patch', 'pos_table')


RINGS = (
    (0, 4, 8, 10, 11, 15, 14, 12, 13, 9, 5, 7, 6, 2, 3, 1),
    (0, 2, 3, 7, 11, 9, 8, 12, 13, 15, 14, 10, 6, 4, 5, 1),
    (0, 1, 3, 7, 5, 4, 8, 9, 11, 15, 13, 12, 14, 10, 6, 2),
    (0, 1, 5, 7, 3, 2, 6, 10, 14, 15, 11, 9, 13, 12, 8, 4),
    (0, 4, 6, 7, 11, 10, 8, 12, 14, 15, 13, 9, 5, 1, 3, 2),
    (0, 2, 6, 7, 3, 1, 5, 9, 13, 15, 11, 10, 14, 12, 8, 4),
)
N_CHIP = 16
MESH_ID = pl.DeviceIdType.MESH
ARRAYS = ((32, 4096), (128, 1024), (32, 3072), (32, 1024), (32, 1024))
FC, PROJ, QKV, OUT, MISC = range(5)
GATHER_STREAMS = (
    (MISC, 0, 32, 0, 256, 0), (MISC, 0, 32, 256, 256, 1), (MISC, 0, 32, 512, 256, 2), (MISC, 0, 32, 768, 256, 3),
    (QKV, 0, 32, 0, 2048, 4), (QKV, 0, 32, 2048, 1024, 5), (OUT, 0, 32, 0, 1024, 5),
    (FC, 0, 32, 0, 2048, 0), (FC, 0, 32, 2048, 2048, 1), (PROJ, 0, 64, 0, 1024, 2), (PROJ, 64, 64, 0, 1024, 3),
)
REDUCE_STREAMS = (
    (FC, 0, 64, 0, 1024, 0), (FC, 0, 64, 1024, 1024, 1), (PROJ, 0, 128, 0, 512, 2), (PROJ, 128, 128, 0, 512, 3),
    (QKV, 0, 64, 0, 1024, 4), (QKV, 0, 64, 1024, 512, 5), (OUT, 0, 64, 0, 512, 5),
    (MISC, 0, 64, 0, 128, 0), (MISC, 0, 64, 128, 128, 1), (MISC, 0, 64, 256, 128, 2), (MISC, 0, 64, 384, 128, 3),
)


def pick(table, index):
    value = jnp.int32(table[0])
    for place in range(1, len(table)):
        value = jnp.where(index == place, jnp.int32(table[place]), value)
    return value


class Place:
    def __init__(self):
        me = lax.axis_index(MESH_AXIS)
        self.core = lax.rem(me, 2)
        self.chip = lax.div(me, 2)
        self.sibling = me + 1 - 2 * self.core
        where_in = [[ring.index(chip) for chip in range(N_CHIP)] for ring in RINGS]
        self.spot = [pick(table, self.chip) for table in where_in]
        self.after = [2 * pick([ring[(table[chip] + 1) % N_CHIP] for chip in range(N_CHIP)], self.chip) + self.core
                      for ring, table in zip(RINGS, where_in)]
        self.before = [2 * pick([ring[(table[chip] - 1) % N_CHIP] for chip in range(N_CHIP)], self.chip) + self.core
                       for ring, table in zip(RINGS, where_in)]

    def chips_back(self, steps):
        return [pick(ring, lax.rem(self.spot[k] + 2 * N_CHIP - steps, N_CHIP)) for k, ring in enumerate(RINGS)]

    def meet(self):
        barrier = pltpu.get_barrier_semaphore()
        for other in self.after + self.before + [self.sibling]:
            pl.semaphore_signal(barrier, inc=1, device_id=(other,), device_id_type=MESH_ID)
        pl.semaphore_wait(barrier, 2 * len(RINGS) + 1)


def gather_kernel(*refs):
    shards, wholes = refs[:5], refs[5:10]
    own_sem, send_sem, recv_sem, twin_send, twin_recv = refs[10:]
    place = Place()

    def block(i, chip, core):
        arr, row, rows, col, cols, _ = GATHER_STREAMS[i]
        first = (2 * chip + core) * ARRAYS[arr][0] + row
        return wholes[arr].at[pl.ds(pl.multiple_of(first, 32), rows), pl.ds(col, cols)]

    def remote(src, dst, sems, i, step, device):
        return pltpu.make_async_remote_copy(src_ref=src, dst_ref=dst, send_sem=sems[0].at[i, step], recv_sem=sems[1].at[i, step],
                                            device_id=(device,), device_id_type=MESH_ID)

    place.meet()
    n_streams = len(GATHER_STREAMS)
    for i in range(n_streams):
        arr, row, rows, col, cols, k = GATHER_STREAMS[i]
        mine = shards[arr].at[pl.ds(row, rows), pl.ds(col, cols)]
        here = block(i, place.chip, place.core)
        remote(mine, here, (send_sem, recv_sem), i, 0, place.after[k]).start()
        remote(mine, here, (twin_send, twin_recv), i, 0, place.sibling).start()
    for arr in range(5):
        rows = ARRAYS[arr][0]
        first = pl.multiple_of((2 * place.chip + place.core) * rows, 32)
        pltpu.make_async_copy(shards[arr], wholes[arr].at[pl.ds(first, rows), :], own_sem.at[arr]).start()

    def ring_step(step, carry):
        chips = place.chips_back(step)
        for i in range(n_streams):
            k = GATHER_STREAMS[i][5]
            here = block(i, chips[k], place.core)
            remote(here, here, (send_sem, recv_sem), i, step - 1, place.after[k]).wait_recv()

            @pl.when(step < N_CHIP - 1)
            def _():
                remote(here, here, (send_sem, recv_sem), i, step, place.after[k]).start()

            remote(here, here, (twin_send, twin_recv), i, step, place.sibling).start()
        return carry

    lax.fori_loop(1, N_CHIP, ring_step, 0)

    def drain(step, carry):
        chips = place.chips_back(step)
        for i in range(n_streams):
            k = GATHER_STREAMS[i][5]
            here = block(i, chips[k], place.core)
            there = block(i, chips[k], 1 - place.core)

            @pl.when(step < N_CHIP - 1)
            def _():
                remote(here, here, (send_sem, recv_sem), i, step, place.after[k]).wait_send()

            remote(here, here, (twin_send, twin_recv), i, step, place.sibling).wait_send()
            remote(there, there, (twin_send, twin_recv), i, step, place.sibling).wait_recv()
        return carry

    lax.fori_loop(0, N_CHIP, drain, 0)
    for arr in range(5):
        rows = ARRAYS[arr][0]
        first = pl.multiple_of((2 * place.chip + place.core) * rows, 32)
        pltpu.make_async_copy(shards[arr], wholes[arr].at[pl.ds(first, rows), :], own_sem.at[arr]).wait()


def gather_all(shards):
    n_streams = len(GATHER_STREAMS)
    ring_sems, twin_sems = pltpu.SemaphoreType.DMA((n_streams, N_CHIP - 1)), pltpu.SemaphoreType.DMA((n_streams, N_CHIP))
    return pl.pallas_call(
        gather_kernel,
        out_shape=[jax.ShapeDtypeStruct((2 * N_CHIP * rows, cols), jnp.bfloat16) for rows, cols in ARRAYS],
        in_specs=[pl.BlockSpec(memory_space=pltpu.VMEM)] * 5,
        out_specs=[pl.BlockSpec(memory_space=pl.ANY)] * 5,
        scratch_shapes=[pltpu.SemaphoreType.DMA((5,)), ring_sems, ring_sems, twin_sems, twin_sems],
        compiler_params=pltpu.CompilerParams(collective_id=0, has_side_effects=True),
        name='gather_all',
    )(*shards)


def reduce_kernel(*refs):
    grads, outs = refs[:5], refs[5:10]
    accs, owns, twins = refs[10:15], refs[15:20], refs[20:25]
    own_sem, twin_send, twin_recv, send_sem, recv_sem, ring_free, twin_free, end_own, end_send, end_recv = refs[25:]
    place = Place()
    n_streams = len(REDUCE_STREAMS)

    def part(i, ref, slot):
        _, row, rows, col, cols, _ = REDUCE_STREAMS[i]
        return ref.at[slot, pl.ds(row, rows), pl.ds(col, cols)]

    def source(i, chip, core):
        arr, row, rows, col, cols, _ = REDUCE_STREAMS[i]
        half = ARRAYS[arr][1] // 2
        first = pl.multiple_of(2 * chip * ARRAYS[arr][0] + row, 64)
        return grads[arr].at[pl.ds(first, rows), pl.ds(pl.multiple_of(core * half + col, 128), cols)]

    def load(i, chip, slot):
        return pltpu.make_async_copy(source(i, chip, place.core), part(i, owns[REDUCE_STREAMS[i][0]], slot), own_sem.at[i, slot])

    def push(i, chip, slot):
        return pltpu.make_async_remote_copy(src_ref=source(i, chip, 1 - place.core), dst_ref=part(i, twins[REDUCE_STREAMS[i][0]], slot),
                                            send_sem=twin_send.at[i, slot], recv_sem=twin_recv.at[i, slot],
                                            device_id=(place.sibling,), device_id_type=MESH_ID)

    def pass_on(i, slot, slot_next):
        arr, k = REDUCE_STREAMS[i][0], REDUCE_STREAMS[i][5]
        return pltpu.make_async_remote_copy(src_ref=part(i, accs[arr], slot), dst_ref=part(i, accs[arr], slot_next),
                                            send_sem=send_sem.at[i, slot], recv_sem=recv_sem.at[i, slot_next],
                                            device_id=(place.after[k],), device_id_type=MESH_ID)

    place.meet()
    for step in range(2):
        chips = place.chips_back(step + 1)
        for i in range(n_streams):
            load(i, chips[REDUCE_STREAMS[i][5]], step).start()
            push(i, chips[REDUCE_STREAMS[i][5]], step).start()

    def ring_step(step, carry):
        slot, pair = lax.rem(step, 3), lax.rem(step, 2)
        slot_next, slot_last = lax.rem(step + 1, 3), lax.rem(step + 2, 3)
        chips = place.chips_back(step + 3)
        for i in range(n_streams):
            arr, row, rows, col, cols, k = REDUCE_STREAMS[i]
            load(i, chips[k], pair).wait()
            push(i, chips[k], pair).wait_recv()

            @pl.when(step == 0)
            def _():
                def add_two(r, c):
                    at = pl.ds(pl.multiple_of(row + 8 * r, 8), 8)
                    lanes = pl.ds(col, cols)
                    accs[arr][slot, at, lanes] = owns[arr][pair, at, lanes] + twins[arr][pair, at, lanes]
                    return c
                lax.fori_loop(0, rows // 8, add_two, 0)

            @pl.when(step > 0)
            def _():
                pass_on(i, slot, slot).wait_recv()

                def add_three(r, c):
                    at = pl.ds(pl.multiple_of(row + 8 * r, 8), 8)
                    lanes = pl.ds(col, cols)
                    accs[arr][slot, at, lanes] = accs[arr][slot, at, lanes] + (owns[arr][pair, at, lanes] + twins[arr][pair, at, lanes])
                    return c
                lax.fori_loop(0, rows // 8, add_three, 0)

            @pl.when(jnp.logical_and(step >= 2, step < N_CHIP - 1))
            def _():
                pl.semaphore_wait(ring_free.at[i], 1)

            @pl.when(step < N_CHIP - 1)
            def _():
                pass_on(i, slot, slot_next).start()

            @pl.when(step < N_CHIP - 2)
            def _():
                pl.semaphore_signal(twin_free.at[i], inc=1, device_id=(place.sibling,), device_id_type=MESH_ID)
                load(i, chips[k], pair).start()

        for i in range(n_streams):
            k = REDUCE_STREAMS[i][5]
            push(i, chips[k], pair).wait_send()

            @pl.when(step < N_CHIP - 2)
            def _():
                pl.semaphore_wait(twin_free.at[i], 1)
                push(i, chips[k], pair).start()

            @pl.when(step >= 1)
            def _():
                pass_on(i, slot_last, slot).wait_send()

            @pl.when(jnp.logical_and(step >= 1, step < N_CHIP - 2))
            def _():
                pl.semaphore_signal(ring_free.at[i], inc=1, device_id=(place.before[k],), device_id_type=MESH_ID)
        return carry

    lax.fori_loop(0, N_CHIP, ring_step, 0)
    last = (N_CHIP - 1) % 3

    def end_copies(arr):
        rows, half = ARRAYS[arr][0], ARRAYS[arr][1] // 2
        target = outs[arr].at[:, pl.ds(pl.multiple_of(place.core * half, 128), half)]
        keep_rows = accs[arr].at[last, pl.ds(pl.multiple_of(place.core * rows, 32), rows), :]
        give_rows = accs[arr].at[last, pl.ds(pl.multiple_of((1 - place.core) * rows, 32), rows), :]
        return (pltpu.make_async_copy(keep_rows, target, end_own.at[arr]),
                pltpu.make_async_remote_copy(src_ref=give_rows, dst_ref=target, send_sem=end_send.at[arr], recv_sem=end_recv.at[arr],
                                             device_id=(place.sibling,), device_id_type=MESH_ID))

    for arr in range(5):
        local, cross = end_copies(arr)
        local.start()
        cross.start()
    for arr in range(5):
        local, cross = end_copies(arr)
        local.wait()
        cross.wait()


def reduce_all(grads):
    n_streams = len(REDUCE_STREAMS)
    slots = lambda n: [pltpu.VMEM((n, 2 * rows, cols // 2), jnp.float32) for rows, cols in ARRAYS]
    sems = lambda n: pltpu.SemaphoreType.DMA((n_streams, n))
    return pl.pallas_call(
        reduce_kernel,
        out_shape=[jax.ShapeDtypeStruct((rows, cols), jnp.float32) for rows, cols in ARRAYS],
        in_specs=[pl.BlockSpec(memory_space=pl.ANY)] * 5,
        out_specs=[pl.BlockSpec(memory_space=pl.ANY)] * 5,
        scratch_shapes=slots(3) + slots(2) + slots(2) + [
            sems(2), sems(2), sems(2), sems(3), sems(3),
            pltpu.SemaphoreType.REGULAR((n_streams,)), pltpu.SemaphoreType.REGULAR((n_streams,)),
            pltpu.SemaphoreType.DMA((5,)), pltpu.SemaphoreType.DMA((5,)), pltpu.SemaphoreType.DMA((5,)),
        ],
        compiler_params=pltpu.CompilerParams(collective_id=1, has_side_effects=True),
        name='reduce_all',
    )(*grads)

HEAD_GROUP, HEAD_DIM, SEQ, N_TOKEN = 256, 64, 64, 50
ROWS = 256
LOGIT_SCALE = HEAD_DIM ** -0.5
VEC_NAMES = ('b_patch', 'cls_tok', 'lnp_g', 'lnp_b', 'ln1_g', 'ln1_b', 'b_out', 'ln2_g', 'ln2_b', 'b_proj')
VEC_AT = {name: place for place, name in enumerate(VEC_NAMES)}
VEC_QKV, VEC_FC, VEC_ROWS = 10, 13, 24


def dot_nn(left, right):
    return lax.dot_general(left, right, (((1,), (0,)), ((), ())), preferred_element_type=jnp.float32)


def dot_nt(left, right):
    return lax.dot_general(left, right, (((1,), (1,)), ((), ())), preferred_element_type=jnp.float32)


def dot_tn(left, right):
    return lax.dot_general(left, right, (((0,), (0,)), ((), ())), preferred_element_type=jnp.float32)


def normalize(x_in):
    centered = x_in - jnp.mean(x_in, axis=-1, keepdims=True)
    inv_std = lax.rsqrt(jnp.mean(centered * centered, axis=-1, keepdims=True) + LN_EPS)
    return centered * inv_std, inv_std


def normalize_back(d_norm, x_hat, inv_std, gain):
    d_hat = d_norm * gain
    return inv_std * (d_hat - jnp.mean(d_hat, axis=-1, keepdims=True) - x_hat * jnp.mean(d_hat * x_hat, axis=-1, keepdims=True))


def lane_ids(shape):
    return lax.broadcasted_iota(jnp.int32, shape, 1)


def stack_heads(block):
    head = lane_ids((1, HEAD_GROUP)) // HEAD_DIM
    return jnp.concatenate([block * (head == h).astype(jnp.bfloat16) for h in range(4)], axis=0)


def unstack_heads(stacked):
    head = lane_ids((1, HEAD_GROUP)) // HEAD_DIM
    total = jnp.where(head == 0, stacked[:SEQ], 0.0)
    for h in range(1, 4):
        total = jnp.where(head == h, stacked[h * SEQ:(h + 1) * SEQ], total)
    return total


def per_head(block, reducer, neutral):
    halves = []
    for j in range(2):
        half = block[:, 128 * j:128 * (j + 1)]
        low = lane_ids(half.shape) < HEAD_DIM
        first = reducer(jnp.where(low, half, neutral), axis=1, keepdims=True)
        second = reducer(jnp.where(low, neutral, half), axis=1, keepdims=True)
        halves.append(jnp.where(low, first, second))
    return jnp.concatenate(halves, axis=1)


def probabilities(q_block, k_stack):
    logits = dot_nt(q_block, k_stack) * LOGIT_SCALE
    logits = jnp.where(lane_ids(logits.shape) % HEAD_DIM < N_TOKEN, logits, -jnp.inf)
    powers = jnp.exp(logits - per_head(logits, jnp.max, -jnp.inf))
    return powers / per_head(powers, jnp.sum, 0.0)


def row_of(vecs, name):
    place = VEC_AT[name]
    return vecs[place:place + 1, :]


def is_cls():
    return lax.broadcasted_iota(jnp.int32, (ROWS, 1), 0) % SEQ == 0


def stage_one(x_in, misc, w_qkv, w_out, vecs, x_zero, a_out, qkv, ctx, h_mid, c_out):
    start = jnp.where(is_cls(), row_of(vecs, 'cls_tok'), row_of(vecs, 'b_patch'))
    x_sum = dot_nt(x_in[...], misc[...]) + start
    x_zero[...] = x_sum
    h_zero = normalize(x_sum)[0] * row_of(vecs, 'lnp_g') + row_of(vecs, 'lnp_b')
    a_in = (normalize(h_zero)[0] * row_of(vecs, 'ln1_g') + row_of(vecs, 'ln1_b')).astype(jnp.bfloat16)
    a_out[...] = a_in
    for s in range(3):
        cols = pl.ds(1024 * s, 1024)
        qkv[:, cols] = (dot_nn(a_in, w_qkv[:, cols]) + vecs[VEC_QKV + s:VEC_QKV + s + 1, :]).astype(jnp.bfloat16)

    def image(b, carry):
        rows = pl.ds(pl.multiple_of(b * SEQ, SEQ), SEQ)
        for g in range(4):
            q_block, k_block, v_block = [qkv[rows, pl.ds(1024 * s + HEAD_GROUP * g, HEAD_GROUP)] for s in range(3)]
            prob = probabilities(q_block, stack_heads(k_block)).astype(jnp.bfloat16)
            ctx[rows, pl.ds(HEAD_GROUP * g, HEAD_GROUP)] = dot_nn(prob, stack_heads(v_block)).astype(jnp.bfloat16)
        return carry

    lax.fori_loop(0, ROWS // SEQ, image, 0)
    mid = h_zero + dot_nn(ctx[...], w_out[...]) + row_of(vecs, 'b_out')
    h_mid[...] = mid
    c_out[...] = (normalize(mid)[0] * row_of(vecs, 'ln2_g') + row_of(vecs, 'ln2_b')).astype(jnp.bfloat16)


def add_row(sums, place, value):
    sums[place:place + 1, :] += jnp.sum(value, axis=0, keepdims=True)


def clear_first(sums):
    @pl.when(pl.program_id(0) == 0)
    def _():
        sums[...] = jnp.zeros_like(sums)


def stage_two(c_in, h_mid, grad_h1, w_fc, w_proj, vecs, gelu_out, d_pre_out, h_one, d_mid, d_mid_b, sums, h_acc, d_c_acc):
    clear_first(sums)
    c_block, g_block = c_in[...], grad_h1[...]
    tile = 1024
    for f in range(4096 // tile):
        cols = pl.ds(tile * f, tile)
        pre_act = dot_nn(c_block, w_fc[:, cols]) + vecs[VEC_FC + f:VEC_FC + f + 1, :]
        normal_cdf = 0.5 * (1.0 + lax.erf(pre_act * INV_SQRT2))
        gelu = (pre_act * normal_cdf).astype(jnp.bfloat16)
        gelu_out[:, cols] = gelu
        slope = normal_cdf + pre_act * jnp.exp(-0.5 * pre_act * pre_act) * INV_SQRT_2PI
        d_pre = dot_nt(g_block, w_proj[cols, :]) * slope
        add_row(sums, VEC_FC + f, d_pre)
        d_pre_b = d_pre.astype(jnp.bfloat16)
        d_pre_out[:, cols] = d_pre_b
        h_part = dot_nn(gelu, w_proj[cols, :])
        d_part = dot_nt(d_pre_b, w_fc[:, cols])
        if f == 0:
            h_acc[...] = h_part
            d_c_acc[...] = d_part
        else:
            h_acc[...] += h_part
            d_c_acc[...] += d_part
    mid = h_mid[...]
    h_one[...] = (mid + h_acc[...] + row_of(vecs, 'b_proj')).astype(jnp.bfloat16)
    d_c = d_c_acc[...]
    x_hat, inv_std = normalize(mid)
    d_h = g_block.astype(jnp.float32)
    d_sum = normalize_back(d_c, x_hat, inv_std, row_of(vecs, 'ln2_g')) + d_h
    d_mid[...] = d_sum
    d_mid_b[...] = d_sum.astype(jnp.bfloat16)
    add_row(sums, VEC_AT['ln2_g'], d_c * x_hat)
    add_row(sums, VEC_AT['ln2_b'], d_c)
    add_row(sums, VEC_AT['b_proj'], d_h)
    add_row(sums, VEC_AT['b_out'], d_sum)


def stage_three(x_zero, d_mid, d_mid_b, qkv, w_qkv, w_out, vecs, d_qkv_out, d_emb_out, sums, d_ctx, d_part):
    clear_first(sums)
    d_ctx[...] = dot_nt(d_mid_b[...], w_out[...]).astype(jnp.bfloat16)
    d_part[...] = jnp.zeros_like(d_part)

    def image(b, carry):
        rows = pl.ds(pl.multiple_of(b * SEQ, SEQ), SEQ)
        for g in range(4):
            places = [pl.ds(1024 * s + HEAD_GROUP * g, HEAD_GROUP) for s in range(3)]
            q_block, k_block, v_block = [qkv[rows, place] for place in places]
            d_block = d_ctx[rows, pl.ds(HEAD_GROUP * g, HEAD_GROUP)]
            k_stack = stack_heads(k_block)
            prob = probabilities(q_block, k_stack)
            d_prob = dot_nt(d_block, stack_heads(v_block))
            d_logit = (prob * (d_prob - per_head(prob * d_prob, jnp.sum, 0.0)) * LOGIT_SCALE).astype(jnp.bfloat16)
            g_q = dot_nn(d_logit, k_stack)
            g_k = unstack_heads(dot_tn(d_logit, q_block))
            g_v = unstack_heads(dot_tn(prob.astype(jnp.bfloat16), d_block))
            for place, grad in zip(places, (g_q, g_k, g_v)):
                d_qkv_out[rows, place] = grad.astype(jnp.bfloat16)
                d_part[:, place] += jnp.sum(grad.reshape(SEQ // 8, 8, HEAD_GROUP), axis=0)
        return carry

    lax.fori_loop(0, ROWS // SEQ, image, 0)
    for s in range(3):
        add_row(sums, VEC_QKV + s, d_part[:, pl.ds(1024 * s, 1024)])
    d_a = dot_nt(d_qkv_out[...], w_qkv[...])
    hat_p, inv_p = normalize(x_zero[...])
    h_zero = hat_p * row_of(vecs, 'lnp_g') + row_of(vecs, 'lnp_b')
    hat_1, inv_1 = normalize(h_zero)
    add_row(sums, VEC_AT['ln1_g'], d_a * hat_1)
    add_row(sums, VEC_AT['ln1_b'], d_a)
    d_zero = normalize_back(d_a, hat_1, inv_1, row_of(vecs, 'ln1_g')) + d_mid[...]
    add_row(sums, VEC_AT['lnp_g'], d_zero * hat_p)
    add_row(sums, VEC_AT['lnp_b'], d_zero)
    d_x = normalize_back(d_zero, hat_p, inv_p, row_of(vecs, 'lnp_g'))
    d_emb = jnp.where(is_cls(), 0.0, d_x)
    add_row(sums, VEC_AT['cls_tok'], jnp.where(is_cls(), d_x, 0.0))
    add_row(sums, VEC_AT['b_patch'], d_emb)
    d_emb_out[...] = d_emb.astype(jnp.bfloat16)


def whole(shape):
    return pl.BlockSpec(shape, lambda i: (0, 0), pipeline_mode=pl.Buffered(1))


def rows_of(width):
    return pl.BlockSpec((ROWS, width), lambda i: (i, 0))


def stage_call(body, name, n_rows, ins, outs, scratch=()):
    in_specs = [rows_of(a.shape[1]) if a.shape[0] == n_rows and not held else whole(a.shape) for a, held in ins]
    out_specs = [pl.BlockSpec((VEC_ROWS, 1024), lambda i: (0, 0)) if dtype is None else rows_of(width) for width, dtype in outs]
    out_shape = [jax.ShapeDtypeStruct((VEC_ROWS, 1024), jnp.float32) if dtype is None else jax.ShapeDtypeStruct((n_rows, width), dtype) for width, dtype in outs]
    return pl.pallas_call(body, grid=(n_rows // ROWS,), in_specs=in_specs, out_specs=out_specs, out_shape=out_shape, scratch_shapes=list(scratch),
                          compiler_params=pltpu.CompilerParams(vmem_limit_bytes=62 * 1024 * 1024, dimension_semantics=('arbitrary',)), name=name)(*[a for a, _ in ins])

N_PIXEL, N_POS = 768, 197
MISC_USED = N_PIXEL + N_POS + len(VEC_NAMES) + 3 + 4


def solution(mesh):
    def spec_of(name):
        return P(None, MESH_AXIS) if name in LAST_SPLIT else P(MESH_AXIS)

    def vector_columns(part, rows):
        columns = [part[name].reshape(rows, 1) for name in VEC_NAMES] + [part['b_qkv'].reshape(rows, 3), part['b_fc'].reshape(rows, 4)]
        return jnp.pad(jnp.concatenate(columns, axis=1), ((0, 0), (0, 1024 - MISC_USED)))

    def pack_misc(part):
        rows = part['w_patch'].shape[1]
        return jnp.concatenate([part['w_patch'].T, part['pos_table'].T, vector_columns(part, rows)], axis=1)

    def unpack_misc(misc):
        part = {'w_patch': misc[:, :N_PIXEL].T, 'pos_table': misc[:, N_PIXEL:N_PIXEL + N_POS].T}
        first = N_PIXEL + N_POS
        for place, name in enumerate(VEC_NAMES):
            part[name] = misc[:, first + place]
        first += len(VEC_NAMES)
        part['b_qkv'] = misc[:, first:first + 3].reshape(-1)
        part['b_fc'] = misc[:, first + 3:first + 7].reshape(-1)
        return part

    def local_step(patches, keep, *rest):
        shards = dict(zip(PARAM_NAMES, rest[:-1]))
        grad_h1 = rest[-1]
        n_img, n_patch, _ = patches.shape
        n_token, d_model = grad_h1.shape[1:]
        n_shard, _, n_heads, head_dim = shards['w_qkv'].shape
        n_rows = n_img * SEQ
        casts = {name: shards[name].astype(jnp.bfloat16) for name in PARAM_NAMES}
        w_fc, w_proj, w_qkv, w_out, misc = gather_all((casts['w_fc'], casts['w_proj'], casts['w_qkv'].reshape(n_shard, -1), casts['w_out'], pack_misc(casts)))
        position = jnp.pad(keep + 1, ((0, 0), (1, 0)))
        position = jnp.pad(position, ((0, 0), (0, SEQ - n_token)), constant_values=-1)[:, :, None]
        onehot_patch = (position == 1 + lax.broadcasted_iota(jnp.int32, (1, 1, n_patch), 2)).astype(jnp.bfloat16)
        onehot_pos = (position == lax.broadcasted_iota(jnp.int32, (1, 1, 1024 - N_PIXEL), 2)).astype(jnp.bfloat16)
        kept_rows = jnp.einsum('bkp,bpq->bkq', onehot_patch, patches, preferred_element_type=jnp.float32).astype(jnp.bfloat16)
        x_in = jnp.concatenate([kept_rows, onehot_pos], axis=2).reshape(n_rows, 1024)
        grad_rows = jnp.pad(grad_h1, ((0, 0), (0, SEQ - n_token), (0, 0))).reshape(n_rows, d_model)

        vec_part = misc[:, N_PIXEL + N_POS:MISC_USED].astype(jnp.float32)
        n_vec = len(VEC_NAMES)
        vecs = jnp.concatenate([vec_part[:, :n_vec].T, vec_part[:, n_vec:n_vec + 3].reshape(3, 1024), vec_part[:, n_vec + 3:].reshape(4, 1024)], axis=0)
        vecs = jnp.pad(vecs, ((0, VEC_ROWS - vecs.shape[0]), (0, 0)))

        bf, f32 = jnp.bfloat16, jnp.float32
        x_zero, a_in, qkv, ctx, h_mid, c_in = stage_call(
            stage_one, 'stage_one', n_rows, [(x_in, False), (misc, True), (w_qkv, True), (w_out, True), (vecs, True)],
            [(1024, f32), (1024, bf), (3072, bf), (1024, bf), (1024, f32), (1024, bf)])
        gelu, d_pre, h_one, d_mid, d_mid_b, sums_two = stage_call(
            stage_two, 'stage_two', n_rows, [(c_in, False), (h_mid, False), (grad_rows, False), (w_fc, True), (w_proj, True), (vecs, True)],
            [(4096, bf), (4096, bf), (1024, bf), (1024, f32), (1024, bf), (0, None)],
            [pltpu.VMEM((ROWS, 1024), f32), pltpu.VMEM((ROWS, 1024), f32)])
        d_qkv, d_emb, sums_three = stage_call(
            stage_three, 'stage_three', n_rows, [(x_zero, False), (d_mid, False), (d_mid_b, False), (qkv, False), (w_qkv, True), (w_out, True), (vecs, True)],
            [(3072, bf), (1024, bf), (0, None)],
            [pltpu.VMEM((ROWS, 1024), bf), pltpu.VMEM((8, 3072), f32)])
        h_one = h_one.reshape(n_img, SEQ, d_model)[:, :n_token]
        outer = lambda left, right: lax.dot_general(left, right, (((0,), (0,)), ((), ())), preferred_element_type=f32)
        sums = sums_two + sums_three
        totals = {name: sums[place] for name, place in VEC_AT.items()}
        totals.update(b_qkv=sums[VEC_QKV:VEC_QKV + 3], b_fc=sums[VEC_FC:VEC_FC + 4])
        g_vec = jnp.concatenate([totals['cls_tok'].reshape(1024, 1), jnp.zeros((1024, N_POS - 1), f32), vector_columns(totals, 1024)], axis=1)
        g_misc = outer(d_emb, x_in) + jnp.pad(g_vec, ((0, 0), (N_PIXEL, 0)))
        reduced = reduce_all((outer(c_in, d_pre), outer(gelu, grad_rows), outer(a_in, d_qkv), outer(ctx, d_mid_b), g_misc))
        own = unpack_misc(reduced[MISC])
        own.update(w_fc=reduced[FC], w_proj=reduced[PROJ], w_qkv=reduced[QKV].reshape(n_shard, 3, n_heads, head_dim), w_out=reduced[OUT])
        return (h_one,) + tuple(own[name] for name in PARAM_NAMES)

    batch_spec = P(MESH_AXIS)
    param_specs = tuple(spec_of(name) for name in PARAM_NAMES)
    return jax.shard_map(local_step, mesh=mesh, in_specs=(batch_spec, batch_spec) + param_specs + (batch_spec,), out_specs=(batch_spec,) + param_specs, check_vma=False)
```

```python
import jax
import jax.numpy as jnp
from jax import lax
from jax.experimental import pallas as pl
from jax.experimental.pallas import tpu as pltpu
from jax.sharding import PartitionSpec as P

MESH_AXIS = 'fsdp'
LN_EPS = 1e-5
INV_SQRT2 = 0.7071067811865476
INV_SQRT_2PI = 0.3989422804014327
PARAM_NAMES = ('w_patch', 'b_patch', 'pos_table', 'cls_tok', 'lnp_g', 'lnp_b', 'ln1_g', 'ln1_b', 'w_qkv', 'b_qkv', 'w_out', 'b_out', 'ln2_g', 'ln2_b', 'w_fc', 'b_fc', 'w_proj', 'b_proj')
LAST_SPLIT = ('w_patch', 'pos_table')


RINGS = (
    (0, 4, 8, 10, 11, 15, 14, 12, 13, 9, 5, 7, 6, 2, 3, 1),
    (0, 2, 3, 7, 11, 9, 8, 12, 13, 15, 14, 10, 6, 4, 5, 1),
    (0, 1, 3, 7, 5, 4, 8, 9, 11, 15, 13, 12, 14, 10, 6, 2),
    (0, 1, 5, 7, 3, 2, 6, 10, 14, 15, 11, 9, 13, 12, 8, 4),
    (0, 4, 6, 7, 11, 10, 8, 12, 14, 15, 13, 9, 5, 1, 3, 2),
    (0, 2, 6, 7, 3, 1, 5, 9, 13, 15, 11, 10, 14, 12, 8, 4),
)
N_CHIP = 16
MESH_ID = pl.DeviceIdType.MESH
ARRAYS = ((32, 4096), (128, 1024), (32, 3072), (32, 1024), (32, 1024))
FC, PROJ, QKV, OUT, MISC = range(5)
GATHER_STREAMS = (
    (MISC, 0, 32, 0, 256, 0), (MISC, 0, 32, 256, 256, 1), (MISC, 0, 32, 512, 256, 2), (MISC, 0, 32, 768, 256, 3),
    (QKV, 0, 32, 0, 2048, 4), (QKV, 0, 32, 2048, 1024, 5), (OUT, 0, 32, 0, 1024, 5),
    (FC, 0, 32, 0, 2048, 0), (FC, 0, 32, 2048, 2048, 1), (PROJ, 0, 64, 0, 1024, 2), (PROJ, 64, 64, 0, 1024, 3),
)
MLP_STREAMS = tuple((FC, 0, 64, 384 * k, 384, k) for k in range(4)) + ((FC, 0, 64, 1536, 256, 4), (FC, 0, 64, 1792, 256, 5)) + tuple(
    (PROJ, 128 * (place % 2), 128, 128 * (place // 2), 128, ring) for place, ring in enumerate((0, 1, 2, 3, 4, 5, 4, 5)))
REST_STREAMS = tuple((QKV, 0, 64, 256 * k, 256, k) for k in range(6)) + tuple((OUT, 0, 64, 128 * k, 128, k) for k in range(4)) + (
    (MISC, 0, 64, 0, 128, 4), (MISC, 0, 64, 128, 128, 5), (MISC, 0, 32, 256, 128, 0), (MISC, 32, 32, 256, 128, 1),
    (MISC, 0, 32, 384, 128, 2), (MISC, 32, 32, 384, 128, 3))


def pick(table, index):
    value = jnp.int32(table[0])
    for place in range(1, len(table)):
        value = jnp.where(index == place, jnp.int32(table[place]), value)
    return value


class Place:
    def __init__(self):
        me = lax.axis_index(MESH_AXIS)
        self.core = lax.rem(me, 2)
        self.chip = lax.div(me, 2)
        self.sibling = me + 1 - 2 * self.core
        where_in = [[ring.index(chip) for chip in range(N_CHIP)] for ring in RINGS]
        self.spot = [pick(table, self.chip) for table in where_in]
        self.after = [2 * pick([ring[(table[chip] + 1) % N_CHIP] for chip in range(N_CHIP)], self.chip) + self.core
                      for ring, table in zip(RINGS, where_in)]
        self.before = [2 * pick([ring[(table[chip] - 1) % N_CHIP] for chip in range(N_CHIP)], self.chip) + self.core
                       for ring, table in zip(RINGS, where_in)]

    def chips_back(self, steps):
        return [pick(ring, lax.rem(self.spot[k] + 2 * N_CHIP - steps, N_CHIP)) for k, ring in enumerate(RINGS)]

    def meet(self):
        barrier = pltpu.get_barrier_semaphore()
        for other in self.after + self.before + [self.sibling]:
            pl.semaphore_signal(barrier, inc=1, device_id=(other,), device_id_type=MESH_ID)
        pl.semaphore_wait(barrier, 2 * len(RINGS) + 1)


def gather_kernel(*refs):
    shards, wholes = refs[:5], refs[5:10]
    own_sem, send_sem, recv_sem, twin_send, twin_recv = refs[10:]
    place = Place()

    def block(i, chip, core):
        arr, row, rows, col, cols, _ = GATHER_STREAMS[i]
        first = (2 * chip + core) * ARRAYS[arr][0] + row
        return wholes[arr].at[pl.ds(pl.multiple_of(first, 32), rows), pl.ds(col, cols)]

    def remote(src, dst, sems, i, step, device):
        return pltpu.make_async_remote_copy(src_ref=src, dst_ref=dst, send_sem=sems[0].at[i, step], recv_sem=sems[1].at[i, step],
                                            device_id=(device,), device_id_type=MESH_ID)

    place.meet()
    n_streams = len(GATHER_STREAMS)
    for i in range(n_streams):
        arr, row, rows, col, cols, k = GATHER_STREAMS[i]
        mine = shards[arr].at[pl.ds(row, rows), pl.ds(col, cols)]
        here = block(i, place.chip, place.core)
        remote(mine, here, (send_sem, recv_sem), i, 0, place.after[k]).start()
        remote(mine, here, (twin_send, twin_recv), i, 0, place.sibling).start()
    for arr in range(5):
        rows = ARRAYS[arr][0]
        first = pl.multiple_of((2 * place.chip + place.core) * rows, 32)
        pltpu.make_async_copy(shards[arr], wholes[arr].at[pl.ds(first, rows), :], own_sem.at[arr]).start()

    def ring_step(step, carry):
        chips = place.chips_back(step)
        for i in range(n_streams):
            k = GATHER_STREAMS[i][5]
            here = block(i, chips[k], place.core)
            remote(here, here, (send_sem, recv_sem), i, step - 1, place.after[k]).wait_recv()

            @pl.when(step < N_CHIP - 1)
            def _():
                remote(here, here, (send_sem, recv_sem), i, step, place.after[k]).start()

            remote(here, here, (twin_send, twin_recv), i, step, place.sibling).start()
        return carry

    lax.fori_loop(1, N_CHIP, ring_step, 0)

    def drain(step, carry):
        chips = place.chips_back(step)
        for i in range(n_streams):
            k = GATHER_STREAMS[i][5]
            here = block(i, chips[k], place.core)
            there = block(i, chips[k], 1 - place.core)

            @pl.when(step < N_CHIP - 1)
            def _():
                remote(here, here, (send_sem, recv_sem), i, step, place.after[k]).wait_send()

            remote(here, here, (twin_send, twin_recv), i, step, place.sibling).wait_send()
            remote(there, there, (twin_send, twin_recv), i, step, place.sibling).wait_recv()
        return carry

    lax.fori_loop(0, N_CHIP, drain, 0)
    for arr in range(5):
        rows = ARRAYS[arr][0]
        first = pl.multiple_of((2 * place.chip + place.core) * rows, 32)
        pltpu.make_async_copy(shards[arr], wholes[arr].at[pl.ds(first, rows), :], own_sem.at[arr]).wait()


def gather_all(shards):
    n_streams = len(GATHER_STREAMS)
    ring_sems, twin_sems = pltpu.SemaphoreType.DMA((n_streams, N_CHIP - 1)), pltpu.SemaphoreType.DMA((n_streams, N_CHIP))
    return pl.pallas_call(
        gather_kernel,
        out_shape=[jax.ShapeDtypeStruct((2 * N_CHIP * rows, cols), jnp.bfloat16) for rows, cols in ARRAYS],
        in_specs=[pl.BlockSpec(memory_space=pltpu.VMEM)] * 5,
        out_specs=[pl.BlockSpec(memory_space=pl.ANY)] * 5,
        scratch_shapes=[pltpu.SemaphoreType.DMA((5,)), ring_sems, ring_sems, twin_sems, twin_sems],
        compiler_params=pltpu.CompilerParams(collective_id=0, has_side_effects=True),
        name='gather_all',
    )(*shards)


class RingSum:
    def __init__(self, place, arrays, streams, accs, owns, gives, twins, sems, term):
        self.place, self.streams, self.term, self.arrays = place, streams, term, arrays
        self.accs, self.owns, self.gives, self.twins = [dict(zip(arrays, refs)) for refs in (accs, owns, gives, twins)]
        (self.twin_send, self.twin_recv, self.send_sem, self.recv_sem, self.ring_free, self.twin_free,
         self.end_own, self.end_send, self.end_recv) = sems

    def part(self, i, ref, *slot):
        _, row, rows, col, cols, _ = self.streams[i]
        return ref.at[(*slot, pl.ds(row, rows), pl.ds(col, cols))]

    def push(self, i, slot):
        arr = self.streams[i][0]
        return pltpu.make_async_remote_copy(src_ref=self.part(i, self.gives[arr]), dst_ref=self.part(i, self.twins[arr], slot),
                                            send_sem=self.twin_send.at[i], recv_sem=self.twin_recv.at[i, slot],
                                            device_id=(self.place.sibling,), device_id_type=MESH_ID)

    def pass_on(self, i, slot, slot_next):
        arr, k = self.streams[i][0], self.streams[i][5]
        return pltpu.make_async_remote_copy(src_ref=self.part(i, self.accs[arr], slot), dst_ref=self.part(i, self.accs[arr], slot_next),
                                            send_sem=self.send_sem.at[i, slot], recv_sem=self.recv_sem.at[i, slot_next],
                                            device_id=(self.place.after[k],), device_id_type=MESH_ID)

    def compute(self, group, step, first):
        chips = self.place.chips_back(step + 1)
        slot = lax.rem(jnp.int32(step), 2)
        for i in group:
            arr, k = self.streams[i][0], self.streams[i][5]
            if not first:
                self.push(i, slot).wait_send()
            self.part(i, self.gives[arr])[...] = self.term(i, chips[k], 1 - self.place.core)
            if not first:
                @pl.when(step >= 2)
                def _():
                    pl.semaphore_wait(self.twin_free.at[i], 1)
            self.push(i, slot).start()
            self.part(i, self.owns[arr])[...] = self.term(i, chips[k], self.place.core)

    def advance(self, group, step):
        slot, slot_next, slot_last, pair = lax.rem(step, 3), lax.rem(step + 1, 3), lax.rem(step + 2, 3), lax.rem(step, 2)
        for i in group:
            arr, row, rows, col, cols, k = self.streams[i]
            acc, own, twin = self.part(i, self.accs[arr], slot), self.part(i, self.owns[arr]), self.part(i, self.twins[arr], pair)
            self.push(i, pair).wait_recv()

            @pl.when(step == 0)
            def _():
                acc[...] = own[...] + twin[...]

            @pl.when(step > 0)
            def _():
                self.pass_on(i, slot, slot).wait_recv()
                acc[...] = acc[...] + (own[...] + twin[...])

            @pl.when(jnp.logical_and(step >= 2, step < N_CHIP - 1))
            def _():
                pl.semaphore_wait(self.ring_free.at[i], 1)

            @pl.when(step < N_CHIP - 1)
            def _():
                self.pass_on(i, slot, slot_next).start()

            @pl.when(step < N_CHIP - 2)
            def _():
                pl.semaphore_signal(self.twin_free.at[i], inc=1, device_id=(self.place.sibling,), device_id_type=MESH_ID)

        for i in group:
            k = self.streams[i][5]

            @pl.when(step >= 1)
            def _():
                self.pass_on(i, slot_last, slot).wait_send()

            @pl.when(jnp.logical_and(step >= 1, step < N_CHIP - 2))
            def _():
                pl.semaphore_signal(self.ring_free.at[i], inc=1, device_id=(self.place.before[k],), device_id_type=MESH_ID)

    def run(self, groups, hook):
        for group in groups:
            self.compute(group, 0, True)

        def ring_step(step, carry):
            for place, group in enumerate(groups):
                self.advance(group, step)

                @pl.when(step < N_CHIP - 1)
                def _():
                    self.compute(group, step + 1, False)

                hook(place, step)
            return carry

        lax.fori_loop(0, N_CHIP, ring_step, 0)

    def finish(self, outs):
        for i in range(len(self.streams)):
            self.push(i, (N_CHIP - 1) % 2).wait_send()
        last = (N_CHIP - 1) % 3
        ends = []
        for place, arr in enumerate(self.arrays):
            rows, half, core = ARRAYS[arr][0], ARRAYS[arr][1] // 2, self.place.core
            target = outs[place].at[:, pl.ds(pl.multiple_of(core * half, 128), half)]
            keep_rows = self.accs[arr].at[last, pl.ds(pl.multiple_of(core * rows, 32), rows), :]
            give_rows = self.accs[arr].at[last, pl.ds(pl.multiple_of((1 - core) * rows, 32), rows), :]
            ends.append(pltpu.make_async_copy(keep_rows, target, self.end_own.at[place]))
            ends.append(pltpu.make_async_remote_copy(src_ref=give_rows, dst_ref=target, send_sem=self.end_send.at[place], recv_sem=self.end_recv.at[place],
                                                     device_id=(self.place.sibling,), device_id_type=MESH_ID))
        for end in ends:
            end.start()
        for end in ends:
            end.wait()


def ring_scratch(arrays, streams):
    shapes = [(2 * ARRAYS[arr][0], ARRAYS[arr][1] // 2) for arr in arrays]
    buffers = [pltpu.VMEM((*lead, *shape), jnp.float32) for lead in ((3,), (), (), (2,)) for shape in shapes]
    dma, regular, n = pltpu.SemaphoreType.DMA, pltpu.SemaphoreType.REGULAR, len(streams)
    return buffers + [dma((n,)), dma((n, 2)), dma((n, 3)), dma((n, 3)), regular((n,)), regular((n,))] + [dma((len(arrays),))] * 3


def split_scratch(refs, n_arrays):
    buffers, sems = refs[:4 * n_arrays], refs[4 * n_arrays:4 * n_arrays + 9]
    return [buffers[n_arrays * b:n_arrays * (b + 1)] for b in range(4)], sems


def term_of(streams, lefts, rights):
    def term(i, chip, core):
        arr, row, rows, col, cols, _ = streams[i]
        half = ARRAYS[arr][1] // 2
        first = pl.multiple_of(2 * chip * ARRAYS[arr][0] + row, 16)
        return dot_nn(lefts[arr][pl.ds(first, rows), :], rights[arr][:, pl.ds(pl.multiple_of(core * half + col, 128), cols)])
    return term


HEAD_GROUP, HEAD_DIM, SEQ, N_TOKEN = 256, 64, 64, 50
ROWS = 256
LOGIT_SCALE = HEAD_DIM ** -0.5
VEC_NAMES = ('b_patch', 'cls_tok', 'lnp_g', 'lnp_b', 'ln1_g', 'ln1_b', 'b_out', 'ln2_g', 'ln2_b', 'b_proj')
VEC_AT = {name: place for place, name in enumerate(VEC_NAMES)}
VEC_QKV, VEC_FC, VEC_ROWS = 10, 13, 24


def dot_nn(left, right):
    return lax.dot_general(left, right, (((1,), (0,)), ((), ())), preferred_element_type=jnp.float32)


def dot_nt(left, right):
    return lax.dot_general(left, right, (((1,), (1,)), ((), ())), preferred_element_type=jnp.float32)


def dot_tn(left, right):
    return lax.dot_general(left, right, (((0,), (0,)), ((), ())), preferred_element_type=jnp.float32)


def normalize(x_in):
    centered = x_in - jnp.mean(x_in, axis=-1, keepdims=True)
    inv_std = lax.rsqrt(jnp.mean(centered * centered, axis=-1, keepdims=True) + LN_EPS)
    return centered * inv_std, inv_std


def normalize_back(d_norm, x_hat, inv_std, gain):
    d_hat = d_norm * gain
    return inv_std * (d_hat - jnp.mean(d_hat, axis=-1, keepdims=True) - x_hat * jnp.mean(d_hat * x_hat, axis=-1, keepdims=True))


def lane_ids(shape):
    return lax.broadcasted_iota(jnp.int32, shape, 1)


def stack_heads(block):
    head = lane_ids((1, HEAD_GROUP)) // HEAD_DIM
    return jnp.concatenate([block * (head == h).astype(jnp.bfloat16) for h in range(4)], axis=0)


def unstack_heads(stacked):
    head = lane_ids((1, HEAD_GROUP)) // HEAD_DIM
    total = jnp.where(head == 0, stacked[:SEQ], 0.0)
    for h in range(1, 4):
        total = jnp.where(head == h, stacked[h * SEQ:(h + 1) * SEQ], total)
    return total


def per_head(block, reducer, neutral):
    halves = []
    for j in range(2):
        half = block[:, 128 * j:128 * (j + 1)]
        low = lane_ids(half.shape) < HEAD_DIM
        first = reducer(jnp.where(low, half, neutral), axis=1, keepdims=True)
        second = reducer(jnp.where(low, neutral, half), axis=1, keepdims=True)
        halves.append(jnp.where(low, first, second))
    return jnp.concatenate(halves, axis=1)


def probabilities(q_block, k_stack):
    logits = dot_nt(q_block, k_stack) * LOGIT_SCALE
    logits = jnp.where(lane_ids(logits.shape) % HEAD_DIM < N_TOKEN, logits, -jnp.inf)
    powers = jnp.exp(logits - per_head(logits, jnp.max, -jnp.inf))
    return powers / per_head(powers, jnp.sum, 0.0)


def row_of(vecs, name):
    place = VEC_AT[name]
    return vecs[place:place + 1, :]


def is_cls(rows):
    return lax.broadcasted_iota(jnp.int32, (rows, 1), 0) % SEQ == 0


def stage_one(x_in, misc, w_qkv, w_out, vecs, x_zero, a_turned, qkv, ctx_turned, h_mid, c_out, c_turned, ctx):
    start = jnp.where(is_cls(ROWS), row_of(vecs, 'cls_tok'), row_of(vecs, 'b_patch'))
    x_sum = dot_nt(x_in[...], misc[...]) + start
    x_zero[...] = x_sum
    h_zero = normalize(x_sum)[0] * row_of(vecs, 'lnp_g') + row_of(vecs, 'lnp_b')
    a_in = (normalize(h_zero)[0] * row_of(vecs, 'ln1_g') + row_of(vecs, 'ln1_b')).astype(jnp.bfloat16)
    a_turned[...] = a_in.T
    for s in range(3):
        cols = pl.ds(1024 * s, 1024)
        qkv[:, cols] = (dot_nn(a_in, w_qkv[:, cols]) + vecs[VEC_QKV + s:VEC_QKV + s + 1, :]).astype(jnp.bfloat16)

    def image(b, carry):
        rows = pl.ds(pl.multiple_of(b * SEQ, SEQ), SEQ)
        for g in range(4):
            q_block, k_block, v_block = [qkv[rows, pl.ds(1024 * s + HEAD_GROUP * g, HEAD_GROUP)] for s in range(3)]
            prob = probabilities(q_block, stack_heads(k_block)).astype(jnp.bfloat16)
            ctx[rows, pl.ds(HEAD_GROUP * g, HEAD_GROUP)] = dot_nn(prob, stack_heads(v_block)).astype(jnp.bfloat16)
        return carry

    lax.fori_loop(0, ROWS // SEQ, image, 0)
    context = ctx[...]
    ctx_turned[...] = context.T
    mid = h_zero + dot_nn(context, w_out[...]) + row_of(vecs, 'b_out')
    h_mid[...] = mid
    c_in = (normalize(mid)[0] * row_of(vecs, 'ln2_g') + row_of(vecs, 'ln2_b')).astype(jnp.bfloat16)
    c_out[...] = c_in
    c_turned[...] = c_in.T


def add_row(sums, place, value):
    sums[place:place + 1, :] += jnp.sum(value, axis=0, keepdims=True)


def clear_first(sums):
    @pl.when(pl.program_id(0) == 0)
    def _():
        sums[...] = jnp.zeros_like(sums)


def stage_two(c_in, h_mid, grad_h1, w_fc, w_proj, vecs, gelu_turned, d_pre_out, h_one, d_mid, d_mid_b, sums, h_acc, d_c_acc):
    clear_first(sums)
    c_block, g_block = c_in[...], grad_h1[...]
    tile = 1024
    for f in range(4096 // tile):
        cols = pl.ds(tile * f, tile)
        pre_act = dot_nn(c_block, w_fc[:, cols]) + vecs[VEC_FC + f:VEC_FC + f + 1, :]
        normal_cdf = 0.5 * (1.0 + lax.erf(pre_act * INV_SQRT2))
        gelu = (pre_act * normal_cdf).astype(jnp.bfloat16)
        gelu_turned[cols, :] = gelu.T
        slope = normal_cdf + pre_act * jnp.exp(-0.5 * pre_act * pre_act) * INV_SQRT_2PI
        d_pre = dot_nt(g_block, w_proj[cols, :]) * slope
        add_row(sums, VEC_FC + f, d_pre)
        d_pre_b = d_pre.astype(jnp.bfloat16)
        d_pre_out[:, cols] = d_pre_b
        h_part = dot_nn(gelu, w_proj[cols, :])
        d_part = dot_nt(d_pre_b, w_fc[:, cols])
        if f == 0:
            h_acc[...] = h_part
            d_c_acc[...] = d_part
        else:
            h_acc[...] += h_part
            d_c_acc[...] += d_part
    mid = h_mid[...]
    h_one[...] = (mid + h_acc[...] + row_of(vecs, 'b_proj')).astype(jnp.bfloat16)
    d_c = d_c_acc[...]
    x_hat, inv_std = normalize(mid)
    d_h = g_block.astype(jnp.float32)
    d_sum = normalize_back(d_c, x_hat, inv_std, row_of(vecs, 'ln2_g')) + d_h
    d_mid[...] = d_sum
    d_mid_b[...] = d_sum.astype(jnp.bfloat16)
    add_row(sums, VEC_AT['ln2_g'], d_c * x_hat)
    add_row(sums, VEC_AT['ln2_b'], d_c)
    add_row(sums, VEC_AT['b_proj'], d_h)
    add_row(sums, VEC_AT['b_out'], d_sum)


def context_back(b, qkv, d_ctx, d_qkv, d_part):
    for g in range(4):
        places = [pl.ds(1024 * s + HEAD_GROUP * g, HEAD_GROUP) for s in range(3)]
        q_block, k_block, v_block = [qkv[b, :, place] for place in places]
        d_block = d_ctx[:, HEAD_GROUP * g:HEAD_GROUP * (g + 1)]
        k_stack = stack_heads(k_block)
        prob = probabilities(q_block, k_stack)
        d_prob = dot_nt(d_block, stack_heads(v_block))
        d_logit = (prob * (d_prob - per_head(prob * d_prob, jnp.sum, 0.0)) * LOGIT_SCALE).astype(jnp.bfloat16)
        g_q = dot_nn(d_logit, k_stack)
        g_k = unstack_heads(dot_tn(d_logit, q_block))
        g_v = unstack_heads(dot_tn(prob.astype(jnp.bfloat16), d_block))
        for place, grad in zip(places, (g_q, g_k, g_v)):
            d_qkv[b, :, place] = grad.astype(jnp.bfloat16)
            d_part[:, place] += jnp.sum(grad.reshape(SEQ // 8, 8, HEAD_GROUP), axis=0)


def entry_back(x_sum, d_mid, d_a, vecs, sums):
    hat_p, inv_p = normalize(x_sum)
    h_zero = hat_p * row_of(vecs, 'lnp_g') + row_of(vecs, 'lnp_b')
    hat_1, inv_1 = normalize(h_zero)
    add_row(sums, VEC_AT['ln1_g'], d_a * hat_1)
    add_row(sums, VEC_AT['ln1_b'], d_a)
    d_zero = normalize_back(d_a, hat_1, inv_1, row_of(vecs, 'ln1_g')) + d_mid
    add_row(sums, VEC_AT['lnp_g'], d_zero * hat_p)
    add_row(sums, VEC_AT['lnp_b'], d_zero)
    d_x = normalize_back(d_zero, hat_p, inv_p, row_of(vecs, 'lnp_g'))
    cls = is_cls(SEQ)
    d_emb = jnp.where(cls, 0.0, d_x)
    add_row(sums, VEC_AT['cls_tok'], jnp.where(cls, d_x, 0.0))
    add_row(sums, VEC_AT['b_patch'], d_emb)
    return d_emb.astype(jnp.bfloat16)


def mlp_sums_kernel(*refs):
    (c_hbm, pre_hbm, gelu_hbm, rows_hbm, qkv_w_hbm, out_w_hbm, vecs, x_hbm, mid_hbm, mid_b_hbm, qkv_hbm) = refs[:11]
    fc_out, proj_out, d_qkv_out, d_emb_out, sums = refs[11:16]
    (c_turned, d_pre, gelu_turned, grad_rows, w_qkv, w_out, x_zero, d_mid, d_mid_b, qkv, d_qkv, d_emb, d_part,
     load_sem, in_sem, out_sem) = refs[16:32]
    (accs, owns, gives, twins), sems = split_scratch(refs[32:], 2)
    place = Place()
    loads = [pltpu.make_async_copy(src, dst, load_sem.at[n]) for n, (src, dst) in enumerate(
        ((c_hbm, c_turned), (pre_hbm, d_pre), (gelu_hbm, gelu_turned), (rows_hbm, grad_rows), (qkv_w_hbm, w_qkv), (out_w_hbm, w_out)))]
    for load in loads:
        load.start()
    n_img = x_hbm.shape[0] // SEQ

    def image_in(b, slot):
        rows = pl.ds(pl.multiple_of(b * SEQ, SEQ), SEQ)
        return [pltpu.make_async_copy(src.at[rows, :], dst.at[slot], in_sem.at[n, slot]) for n, (src, dst) in enumerate(
            ((x_hbm, x_zero), (mid_hbm, d_mid), (mid_b_hbm, d_mid_b), (qkv_hbm, qkv)))]

    def image_out(b, slot):
        rows = pl.ds(pl.multiple_of(b * SEQ, SEQ), SEQ)
        return [pltpu.make_async_copy(src.at[slot], dst.at[rows, :], out_sem.at[n, slot]) for n, (src, dst) in enumerate(
            ((d_qkv, d_qkv_out), (d_emb, d_emb_out)))]

    for copy in image_in(0, 0):
        copy.start()
    sums[...] = jnp.zeros_like(sums)
    d_part[...] = jnp.zeros_like(d_part)
    place.meet()
    term = term_of(MLP_STREAMS, {FC: c_turned, PROJ: gelu_turned}, {FC: d_pre, PROJ: grad_rows})
    ring = RingSum(place, (FC, PROJ), MLP_STREAMS, accs, owns, gives, twins, sems, term)
    for load in loads:
        load.wait()

    def hook(half, step):
        slot = lax.rem(step, 2)
        if half == 0:
            @pl.when(step < n_img - 1)
            def _():
                for copy in image_in(step + 1, 1 - slot):
                    copy.start()

            for copy in image_in(step, slot):
                copy.wait()

            @pl.when(step >= 2)
            def _():
                for copy in image_out(step - 2, slot):
                    copy.wait()

            d_ctx = dot_nt(d_mid_b[slot], w_out[...]).astype(jnp.bfloat16)
            context_back(slot, qkv, d_ctx, d_qkv, d_part)
        else:
            d_a = dot_nt(d_qkv[slot], w_qkv[...])
            d_emb[slot] = entry_back(x_zero[slot], d_mid[slot], d_a, vecs, sums)
            for copy in image_out(step, slot):
                copy.start()

    ring.run((tuple(range(6)), tuple(range(6, len(MLP_STREAMS)))), hook)
    for step in (n_img - 2, n_img - 1):
        for copy in image_out(step, step % 2):
            copy.wait()
    for s in range(3):
        add_row(sums, VEC_QKV + s, d_part[:, pl.ds(1024 * s, 1024)])
    ring.finish((fc_out, proj_out))


def mlp_sums(c_turned, d_pre, gelu_turned, grad_rows, w_qkv, w_out, vecs, x_zero, d_mid, d_mid_b, qkv):
    bf, f32, dma = jnp.bfloat16, jnp.float32, pltpu.SemaphoreType.DMA
    n_rows = x_zero.shape[0]
    assert n_rows // SEQ == N_CHIP
    out_shape = [jax.ShapeDtypeStruct(ARRAYS[FC], f32), jax.ShapeDtypeStruct(ARRAYS[PROJ], f32), jax.ShapeDtypeStruct((n_rows, 3072), bf),
                 jax.ShapeDtypeStruct((n_rows, 1024), bf), jax.ShapeDtypeStruct((VEC_ROWS, 1024), f32)]
    anywhere, vmem = pl.BlockSpec(memory_space=pl.ANY), pl.BlockSpec(memory_space=pltpu.VMEM)
    scratch = [pltpu.VMEM(a.shape, bf) for a in (c_turned, d_pre, gelu_turned, grad_rows, w_qkv, w_out)]
    scratch += [pltpu.VMEM((2, SEQ, 1024), f32), pltpu.VMEM((2, SEQ, 1024), f32), pltpu.VMEM((2, SEQ, 1024), bf), pltpu.VMEM((2, SEQ, 3072), bf),
                pltpu.VMEM((2, SEQ, 3072), bf), pltpu.VMEM((2, SEQ, 1024), bf), pltpu.VMEM((8, 3072), f32), dma((6,)), dma((4, 2)), dma((2, 2))]
    return pl.pallas_call(
        mlp_sums_kernel, out_shape=out_shape, in_specs=[anywhere] * 6 + [vmem] + [anywhere] * 4, out_specs=[anywhere] * 4 + [vmem],
        scratch_shapes=scratch + ring_scratch((FC, PROJ), MLP_STREAMS),
        compiler_params=pltpu.CompilerParams(collective_id=1, has_side_effects=True, vmem_limit_bytes=62 * 1024 * 1024), name='mlp_sums',
    )(c_turned, d_pre, gelu_turned, grad_rows, w_qkv, w_out, vecs, x_zero, d_mid, d_mid_b, qkv)


def rest_sums_kernel(*refs):
    (a_hbm, dqkv_hbm, ctx_hbm, mid_hbm, emb_hbm, in_hbm, vec_hbm) = refs[:7]
    outs = refs[7:10]
    (a_turned, d_qkv, ctx_turned, d_mid_b, emb_turned, x_in, g_vec, load_sem) = refs[10:18]
    (accs, owns, gives, twins), sems = split_scratch(refs[18:], 3)
    place = Place()
    loads = [pltpu.make_async_copy(src, dst, load_sem.at[n]) for n, (src, dst) in enumerate(
        ((a_hbm, a_turned), (dqkv_hbm, d_qkv), (ctx_hbm, ctx_turned), (mid_hbm, d_mid_b), (emb_hbm, emb_turned), (in_hbm, x_in), (vec_hbm, g_vec)))]
    for load in loads:
        load.start()
    place.meet()
    product = term_of(REST_STREAMS, {QKV: a_turned, OUT: ctx_turned, MISC: emb_turned}, {QKV: d_qkv, OUT: d_mid_b, MISC: x_in})

    def term(i, chip, core):
        arr, row, rows, col, cols, _ = REST_STREAMS[i]
        block = product(i, chip, core)
        if arr == MISC and col >= 256:
            first = pl.multiple_of(2 * chip * ARRAYS[arr][0] + row, 16)
            block = block + jnp.where(core == 1, g_vec[pl.ds(first, rows), pl.ds(col - 256, cols)], 0.0)
        return block

    ring = RingSum(place, (QKV, OUT, MISC), REST_STREAMS, accs, owns, gives, twins, sems, term)
    for load in loads:
        load.wait()
    ring.run((tuple(range(6)), tuple(range(6, len(REST_STREAMS)))), lambda half, step: None)
    ring.finish(outs)


def rest_sums(a_turned, d_qkv, ctx_turned, d_mid_b, emb_turned, x_in, g_vec):
    arrays = (QKV, OUT, MISC)
    operands = (a_turned, d_qkv, ctx_turned, d_mid_b, emb_turned, x_in, g_vec)
    anywhere = pl.BlockSpec(memory_space=pl.ANY)
    return pl.pallas_call(
        rest_sums_kernel, out_shape=[jax.ShapeDtypeStruct(ARRAYS[arr], jnp.float32) for arr in arrays],
        in_specs=[anywhere] * 7, out_specs=[anywhere] * 3,
        scratch_shapes=[pltpu.VMEM(a.shape, a.dtype) for a in operands] + [pltpu.SemaphoreType.DMA((7,))] + ring_scratch(arrays, REST_STREAMS),
        compiler_params=pltpu.CompilerParams(collective_id=2, has_side_effects=True, vmem_limit_bytes=62 * 1024 * 1024), name='rest_sums',
    )(*operands)


def whole(shape):
    return pl.BlockSpec(shape, lambda i: (0, 0), pipeline_mode=pl.Buffered(1))


def rows_of(width):
    return pl.BlockSpec((ROWS, width), lambda i: (i, 0))


def stage_call(body, name, n_rows, ins, outs, scratch=()):
    in_specs = [rows_of(a.shape[1]) if a.shape[0] == n_rows and not held else whole(a.shape) for a, held in ins]
    out_specs, out_shape = [], []
    for width, dtype in outs:
        if dtype is None:
            out_specs.append(pl.BlockSpec((VEC_ROWS, 1024), lambda i: (0, 0)))
            out_shape.append(jax.ShapeDtypeStruct((VEC_ROWS, 1024), jnp.float32))
        elif width < 0:
            out_specs.append(pl.BlockSpec((-width, ROWS), lambda i: (0, i)))
            out_shape.append(jax.ShapeDtypeStruct((-width, n_rows), dtype))
        else:
            out_specs.append(rows_of(width))
            out_shape.append(jax.ShapeDtypeStruct((n_rows, width), dtype))
    return pl.pallas_call(body, grid=(n_rows // ROWS,), in_specs=in_specs, out_specs=out_specs, out_shape=out_shape, scratch_shapes=list(scratch),
                          compiler_params=pltpu.CompilerParams(vmem_limit_bytes=62 * 1024 * 1024, dimension_semantics=('arbitrary',)), name=name)(*[a for a, _ in ins])

N_PIXEL, N_POS = 768, 197
MISC_USED = N_PIXEL + N_POS + len(VEC_NAMES) + 3 + 4


def solution(mesh):
    def spec_of(name):
        return P(None, MESH_AXIS) if name in LAST_SPLIT else P(MESH_AXIS)

    def vector_columns(part, rows):
        columns = [part[name].reshape(rows, 1) for name in VEC_NAMES] + [part['b_qkv'].reshape(rows, 3), part['b_fc'].reshape(rows, 4)]
        return jnp.pad(jnp.concatenate(columns, axis=1), ((0, 0), (0, 1024 - MISC_USED)))

    def pack_misc(part):
        rows = part['w_patch'].shape[1]
        return jnp.concatenate([part['w_patch'].T, part['pos_table'].T, vector_columns(part, rows)], axis=1)

    def unpack_misc(misc):
        part = {'w_patch': misc[:, :N_PIXEL].T, 'pos_table': misc[:, N_PIXEL:N_PIXEL + N_POS].T}
        first = N_PIXEL + N_POS
        for place, name in enumerate(VEC_NAMES):
            part[name] = misc[:, first + place]
        first += len(VEC_NAMES)
        part['b_qkv'] = misc[:, first:first + 3].reshape(-1)
        part['b_fc'] = misc[:, first + 3:first + 7].reshape(-1)
        return part

    def local_step(patches, keep, *rest):
        shards = dict(zip(PARAM_NAMES, rest[:-1]))
        grad_h1 = rest[-1]
        n_img, n_patch, _ = patches.shape
        n_token, d_model = grad_h1.shape[1:]
        n_shard, _, n_heads, head_dim = shards['w_qkv'].shape
        n_rows = n_img * SEQ
        casts = {name: shards[name].astype(jnp.bfloat16) for name in PARAM_NAMES}
        w_fc, w_proj, w_qkv, w_out, misc = gather_all((casts['w_fc'], casts['w_proj'], casts['w_qkv'].reshape(n_shard, -1), casts['w_out'], pack_misc(casts)))
        position = jnp.pad(keep + 1, ((0, 0), (1, 0)))
        position = jnp.pad(position, ((0, 0), (0, SEQ - n_token)), constant_values=-1)[:, :, None]
        onehot_patch = (position == 1 + lax.broadcasted_iota(jnp.int32, (1, 1, n_patch), 2)).astype(jnp.bfloat16)
        onehot_pos = (position == lax.broadcasted_iota(jnp.int32, (1, 1, 1024 - N_PIXEL), 2)).astype(jnp.bfloat16)
        kept_rows = jnp.einsum('bkp,bpq->bkq', onehot_patch, patches, preferred_element_type=jnp.float32).astype(jnp.bfloat16)
        x_in = jnp.concatenate([kept_rows, onehot_pos], axis=2).reshape(n_rows, 1024)
        grad_rows = jnp.pad(grad_h1, ((0, 0), (0, SEQ - n_token), (0, 0))).reshape(n_rows, d_model)

        vec_part = misc[:, N_PIXEL + N_POS:MISC_USED].astype(jnp.float32)
        n_vec = len(VEC_NAMES)
        vecs = jnp.concatenate([vec_part[:, :n_vec].T, vec_part[:, n_vec:n_vec + 3].reshape(3, 1024), vec_part[:, n_vec + 3:].reshape(4, 1024)], axis=0)
        vecs = jnp.pad(vecs, ((0, VEC_ROWS - vecs.shape[0]), (0, 0)))

        bf, f32 = jnp.bfloat16, jnp.float32
        x_zero, a_turned, qkv, ctx_turned, h_mid, c_in, c_turned = stage_call(
            stage_one, 'stage_one', n_rows, [(x_in, False), (misc, True), (w_qkv, True), (w_out, True), (vecs, True)],
            [(1024, f32), (-1024, bf), (3072, bf), (-1024, bf), (1024, f32), (1024, bf), (-1024, bf)], [pltpu.VMEM((ROWS, 1024), bf)])
        gelu_turned, d_pre, h_one, d_mid, d_mid_b, sums_two = stage_call(
            stage_two, 'stage_two', n_rows, [(c_in, False), (h_mid, False), (grad_rows, False), (w_fc, True), (w_proj, True), (vecs, True)],
            [(-4096, bf), (4096, bf), (1024, bf), (1024, f32), (1024, bf), (0, None)],
            [pltpu.VMEM((ROWS, 1024), f32), pltpu.VMEM((ROWS, 1024), f32)])
        h_one = h_one.reshape(n_img, SEQ, d_model)[:, :n_token]
        fc_sum, proj_sum, d_qkv, d_emb, sums_three = mlp_sums(c_turned, d_pre, gelu_turned, grad_rows, w_qkv, w_out, vecs, x_zero, d_mid, d_mid_b, qkv)
        sums = sums_two + sums_three
        vec_rows = jnp.concatenate([sums[:n_vec], sums[VEC_QKV:VEC_QKV + 3].reshape(1024, 3).T, sums[VEC_FC:VEC_FC + 4].reshape(1024, 4).T], axis=0)
        g_rows = jnp.concatenate([sums[VEC_AT['cls_tok']][None], jnp.zeros((N_POS - 1, 1024), f32), vec_rows], axis=0)
        g_vec = jnp.pad(g_rows, ((0, 1024 - N_PIXEL - g_rows.shape[0]), (0, 0))).T
        qkv_sum, out_sum, misc_sum = rest_sums(a_turned, d_qkv, ctx_turned, d_mid_b, d_emb.T, x_in, g_vec)
        own = unpack_misc(misc_sum)
        own.update(w_fc=fc_sum, w_proj=proj_sum, w_qkv=qkv_sum.reshape(n_shard, 3, n_heads, head_dim), w_out=out_sum)
        return (h_one,) + tuple(own[name] for name in PARAM_NAMES)

    batch_spec = P(MESH_AXIS)
    param_specs = tuple(spec_of(name) for name in PARAM_NAMES)
    return jax.shard_map(local_step, mesh=mesh, in_specs=(batch_spec, batch_spec) + param_specs + (batch_spec,), out_specs=(batch_spec,) + param_specs, check_vma=False)
```

```python
import jax
import jax.numpy as jnp
from jax import lax
from jax.experimental import pallas as pl
from jax.experimental.pallas import tpu as pltpu
from jax.sharding import PartitionSpec as P

MESH_AXIS = 'fsdp'
LN_EPS = 1e-5
INV_SQRT2 = 0.7071067811865476
INV_SQRT_2PI = 0.3989422804014327
PARAM_NAMES = ('w_patch', 'b_patch', 'pos_table', 'cls_tok', 'lnp_g', 'lnp_b', 'ln1_g', 'ln1_b', 'w_qkv', 'b_qkv', 'w_out', 'b_out', 'ln2_g', 'ln2_b', 'w_fc', 'b_fc', 'w_proj', 'b_proj')
LAST_SPLIT = ('w_patch', 'pos_table')


RINGS = (
    (0, 4, 8, 10, 11, 15, 14, 12, 13, 9, 5, 7, 6, 2, 3, 1),
    (0, 2, 3, 7, 11, 9, 8, 12, 13, 15, 14, 10, 6, 4, 5, 1),
    (0, 1, 3, 7, 5, 4, 8, 9, 11, 15, 13, 12, 14, 10, 6, 2),
    (0, 1, 5, 7, 3, 2, 6, 10, 14, 15, 11, 9, 13, 12, 8, 4),
    (0, 4, 6, 7, 11, 10, 8, 12, 14, 15, 13, 9, 5, 1, 3, 2),
    (0, 2, 6, 7, 3, 1, 5, 9, 13, 15, 11, 10, 14, 12, 8, 4),
)
N_CHIP = 16
MESH_ID = pl.DeviceIdType.MESH
ARRAYS = ((32, 4096), (128, 1024), (32, 3072), (32, 1024), (32, 1024))
FC, PROJ, QKV, OUT, MISC = range(5)
FIRST_STREAMS = tuple((QKV, 0, 32, 512 * k, 512, k) for k in range(6)) + (
    (OUT, 0, 32, 0, 384, 0), (OUT, 0, 32, 384, 384, 1), (OUT, 0, 32, 768, 256, 4),
    (MISC, 0, 32, 0, 384, 2), (MISC, 0, 32, 384, 384, 3), (MISC, 0, 32, 768, 256, 5))
SECOND_STREAMS = (
    (FC, 0, 32, 0, 896, 0), (FC, 0, 32, 896, 896, 1), (FC, 0, 32, 1792, 384, 2), (FC, 0, 32, 2176, 384, 3),
    (FC, 0, 32, 2560, 768, 4), (FC, 0, 32, 3328, 768, 5), (PROJ, 0, 128, 0, 128, 0), (PROJ, 0, 128, 128, 128, 1),
    (PROJ, 0, 128, 256, 256, 2), (PROJ, 0, 128, 512, 256, 3), (PROJ, 0, 128, 768, 128, 4), (PROJ, 0, 128, 896, 128, 5))
MLP_STREAMS = tuple((FC, 0, 64, 384 * k, 384, k) for k in range(4)) + ((FC, 0, 64, 1536, 256, 4), (FC, 0, 64, 1792, 256, 5)) + tuple(
    (PROJ, 128 * (place % 2), 128, 128 * (place // 2), 128, ring) for place, ring in enumerate((0, 1, 2, 3, 4, 5, 4, 5)))
REST_STREAMS = tuple((QKV, 0, 64, 256 * k, 256, k) for k in range(6)) + tuple((OUT, 0, 64, 128 * k, 128, k) for k in range(4)) + (
    (MISC, 0, 64, 0, 128, 4), (MISC, 0, 64, 128, 128, 5), (MISC, 0, 32, 256, 128, 0), (MISC, 32, 32, 256, 128, 1),
    (MISC, 0, 32, 384, 128, 2), (MISC, 32, 32, 384, 128, 3))


def pick(table, index):
    value = jnp.int32(table[0])
    for place in range(1, len(table)):
        value = jnp.where(index == place, jnp.int32(table[place]), value)
    return value


class Place:
    def __init__(self):
        me = lax.axis_index(MESH_AXIS)
        self.core = lax.rem(me, 2)
        self.chip = lax.div(me, 2)
        self.sibling = me + 1 - 2 * self.core
        where_in = [[ring.index(chip) for chip in range(N_CHIP)] for ring in RINGS]
        self.spot = [pick(table, self.chip) for table in where_in]
        self.after = [2 * pick([ring[(table[chip] + 1) % N_CHIP] for chip in range(N_CHIP)], self.chip) + self.core
                      for ring, table in zip(RINGS, where_in)]
        self.before = [2 * pick([ring[(table[chip] - 1) % N_CHIP] for chip in range(N_CHIP)], self.chip) + self.core
                       for ring, table in zip(RINGS, where_in)]

    def chips_back(self, steps):
        return [pick(ring, lax.rem(self.spot[k] + 2 * N_CHIP - steps, N_CHIP)) for k, ring in enumerate(RINGS)]

    def meet(self):
        barrier = pltpu.get_barrier_semaphore()
        for other in self.after + self.before + [self.sibling]:
            pl.semaphore_signal(barrier, inc=1, device_id=(other,), device_id_type=MESH_ID)
        pl.semaphore_wait(barrier, 2 * len(RINGS) + 1)


class RingGather:
    def __init__(self, place, arrays, streams, shards, wholes, sems):
        self.place, self.arrays, self.streams = place, arrays, streams
        self.shards, self.wholes = dict(zip(arrays, shards)), dict(zip(arrays, wholes))
        self.own_sem, self.send_sem, self.recv_sem, self.twin_send, self.twin_recv = sems

    def block(self, i, chip, core):
        arr, row, rows, col, cols, _ = self.streams[i]
        first = (2 * chip + core) * ARRAYS[arr][0] + row
        return self.wholes[arr].at[pl.ds(pl.multiple_of(first, 32), rows), pl.ds(col, cols)]

    def ring_copy(self, i, src, dst, step):
        return pltpu.make_async_remote_copy(src_ref=src, dst_ref=dst, send_sem=self.send_sem.at[i, step], recv_sem=self.recv_sem.at[i, step],
                                            device_id=(self.place.after[self.streams[i][5]],), device_id_type=MESH_ID)

    def twin_copy(self, i, src, dst, step):
        return pltpu.make_async_remote_copy(src_ref=src, dst_ref=dst, send_sem=self.twin_send.at[i, step], recv_sem=self.twin_recv.at[i, step],
                                            device_id=(self.place.sibling,), device_id_type=MESH_ID)

    def own_copies(self):
        for place, arr in enumerate(self.arrays):
            rows = ARRAYS[arr][0]
            first = pl.multiple_of((2 * self.place.chip + self.place.core) * rows, 32)
            yield pltpu.make_async_copy(self.shards[arr], self.wholes[arr].at[pl.ds(first, rows), :], self.own_sem.at[place])

    def run(self, hook):
        place = self.place
        for i in range(len(self.streams)):
            arr, row, rows, col, cols, _ = self.streams[i]
            mine = self.shards[arr].at[pl.ds(row, rows), pl.ds(col, cols)]
            here = self.block(i, place.chip, place.core)
            self.ring_copy(i, mine, here, 0).start()
            self.twin_copy(i, mine, here, 0).start()
        for copy in self.own_copies():
            copy.start()
        hook(jnp.int32(0))

        def ring_step(step, carry):
            chips = place.chips_back(step)
            for i in range(len(self.streams)):
                here = self.block(i, chips[self.streams[i][5]], place.core)
                self.ring_copy(i, here, here, step - 1).wait_recv()

                @pl.when(step < N_CHIP - 1)
                def _():
                    self.ring_copy(i, here, here, step).start()

                self.twin_copy(i, here, here, step).start()
            hook(step)
            return carry

        lax.fori_loop(1, N_CHIP, ring_step, 0)

        def drain(step, carry):
            chips = place.chips_back(step)
            for i in range(len(self.streams)):
                k = self.streams[i][5]
                here, there = self.block(i, chips[k], place.core), self.block(i, chips[k], 1 - place.core)

                @pl.when(step < N_CHIP - 1)
                def _():
                    self.ring_copy(i, here, here, step).wait_send()

                self.twin_copy(i, here, here, step).wait_send()
                self.twin_copy(i, there, there, step).wait_recv()
            return carry

        lax.fori_loop(0, N_CHIP, drain, 0)
        for copy in self.own_copies():
            copy.wait()


def gather_sems(arrays, streams):
    ring, twin = pltpu.SemaphoreType.DMA((len(streams), N_CHIP - 1)), pltpu.SemaphoreType.DMA((len(streams), N_CHIP))
    return [pltpu.SemaphoreType.DMA((len(arrays),)), ring, ring, twin, twin]


def gathered_shapes(arrays):
    return [jax.ShapeDtypeStruct((2 * N_CHIP * ARRAYS[arr][0], ARRAYS[arr][1]), jnp.bfloat16) for arr in arrays]


FIRST_ARRAYS, SECOND_ARRAYS = (QKV, OUT, MISC), (FC, PROJ)


def gather_first_kernel(*refs):
    place = Place()
    place.meet()
    RingGather(place, FIRST_ARRAYS, FIRST_STREAMS, refs[:3], refs[3:6], refs[6:]).run(lambda step: None)


def gather_first(shards):
    return pl.pallas_call(
        gather_first_kernel, out_shape=gathered_shapes(FIRST_ARRAYS),
        in_specs=[pl.BlockSpec(memory_space=pltpu.VMEM)] * 3, out_specs=[pl.BlockSpec(memory_space=pl.ANY)] * 3,
        scratch_shapes=gather_sems(FIRST_ARRAYS, FIRST_STREAMS),
        compiler_params=pltpu.CompilerParams(collective_id=0, has_side_effects=True), name='gather_first',
    )(*shards)


class RingSum:
    def __init__(self, place, arrays, streams, accs, owns, gives, twins, sems, term):
        self.place, self.streams, self.term, self.arrays = place, streams, term, arrays
        self.accs, self.owns, self.gives, self.twins = [dict(zip(arrays, refs)) for refs in (accs, owns, gives, twins)]
        (self.twin_send, self.twin_recv, self.send_sem, self.recv_sem, self.ring_free, self.twin_free,
         self.end_own, self.end_send, self.end_recv) = sems

    def part(self, i, ref, *slot):
        _, row, rows, col, cols, _ = self.streams[i]
        return ref.at[(*slot, pl.ds(row, rows), pl.ds(col, cols))]

    def push(self, i, slot):
        arr = self.streams[i][0]
        return pltpu.make_async_remote_copy(src_ref=self.part(i, self.gives[arr], slot), dst_ref=self.part(i, self.twins[arr], slot),
                                            send_sem=self.twin_send.at[i, slot], recv_sem=self.twin_recv.at[i, slot],
                                            device_id=(self.place.sibling,), device_id_type=MESH_ID)

    def pass_on(self, i, slot, slot_next):
        arr, k = self.streams[i][0], self.streams[i][5]
        return pltpu.make_async_remote_copy(src_ref=self.part(i, self.accs[arr], slot), dst_ref=self.part(i, self.accs[arr], slot_next),
                                            send_sem=self.send_sem.at[i, slot], recv_sem=self.recv_sem.at[i, slot_next],
                                            device_id=(self.place.after[k],), device_id_type=MESH_ID)

    def make_own(self, group, step):
        chips = self.place.chips_back(step + 1)
        for i in group:
            arr, k = self.streams[i][0], self.streams[i][5]
            self.part(i, self.owns[arr])[...] = self.term(i, chips[k], self.place.core)

    def make_give(self, group, step):
        chips, slot = self.place.chips_back(step + 1), lax.rem(jnp.int32(step), 2)
        for i in group:
            arr, k = self.streams[i][0], self.streams[i][5]
            self.part(i, self.gives[arr], slot)[...] = self.term(i, chips[k], 1 - self.place.core)

    def push_next(self, group, step):
        slot, slot_next = lax.rem(step, 2), lax.rem(step + 1, 2)
        for i in group:
            self.push(i, slot).wait_send()

            @pl.when(step >= 1)
            def _():
                pl.semaphore_wait(self.twin_free.at[i], 1)
            self.push(i, slot_next).start()

    def advance(self, group, step):
        slot, slot_next, slot_last, pair = lax.rem(step, 3), lax.rem(step + 1, 3), lax.rem(step + 2, 3), lax.rem(step, 2)
        for i in group:
            arr, row, rows, col, cols, k = self.streams[i]
            acc, own, twin = self.part(i, self.accs[arr], slot), self.part(i, self.owns[arr]), self.part(i, self.twins[arr], pair)
            self.push(i, pair).wait_recv()

            @pl.when(step == 0)
            def _():
                acc[...] = own[...] + twin[...]

            @pl.when(step > 0)
            def _():
                self.pass_on(i, slot, slot).wait_recv()
                acc[...] = acc[...] + (own[...] + twin[...])

            @pl.when(jnp.logical_and(step >= 2, step < N_CHIP - 1))
            def _():
                pl.semaphore_wait(self.ring_free.at[i], 1)

            @pl.when(step < N_CHIP - 1)
            def _():
                self.pass_on(i, slot, slot_next).start()

            @pl.when(step < N_CHIP - 2)
            def _():
                pl.semaphore_signal(self.twin_free.at[i], inc=1, device_id=(self.place.sibling,), device_id_type=MESH_ID)

        for i in group:
            k = self.streams[i][5]

            @pl.when(step >= 1)
            def _():
                self.pass_on(i, slot_last, slot).wait_send()

            @pl.when(jnp.logical_and(step >= 1, step < N_CHIP - 2))
            def _():
                pl.semaphore_signal(self.ring_free.at[i], inc=1, device_id=(self.place.before[k],), device_id_type=MESH_ID)

    def run(self, groups, hook):
        for group in groups:
            self.make_give(group, 0)
            for i in group:
                self.push(i, 0).start()
            self.make_own(group, 0)
            self.make_give(group, 1)

        def ring_step(step, carry):
            for place, group in enumerate(groups):
                self.advance(group, step)

                @pl.when(step < N_CHIP - 1)
                def _():
                    self.push_next(group, step)
                    self.make_own(group, step + 1)

                @pl.when(step < N_CHIP - 2)
                def _():
                    self.make_give(group, step + 2)

                hook(place, step)
            return carry

        lax.fori_loop(0, N_CHIP, ring_step, 0)

    def finish(self, outs):
        for i in range(len(self.streams)):
            self.push(i, (N_CHIP - 1) % 2).wait_send()
        last = (N_CHIP - 1) % 3
        ends = []
        for place, arr in enumerate(self.arrays):
            rows, half, core = ARRAYS[arr][0], ARRAYS[arr][1] // 2, self.place.core
            target = outs[place].at[:, pl.ds(pl.multiple_of(core * half, 128), half)]
            keep_rows = self.accs[arr].at[last, pl.ds(pl.multiple_of(core * rows, 32), rows), :]
            give_rows = self.accs[arr].at[last, pl.ds(pl.multiple_of((1 - core) * rows, 32), rows), :]
            ends.append(pltpu.make_async_copy(keep_rows, target, self.end_own.at[place]))
            ends.append(pltpu.make_async_remote_copy(src_ref=give_rows, dst_ref=target, send_sem=self.end_send.at[place], recv_sem=self.end_recv.at[place],
                                                     device_id=(self.place.sibling,), device_id_type=MESH_ID))
        for end in ends:
            end.start()
        for end in ends:
            end.wait()


def ring_scratch(arrays, streams):
    shapes = [(2 * ARRAYS[arr][0], ARRAYS[arr][1] // 2) for arr in arrays]
    buffers = [pltpu.VMEM((*lead, *shape), jnp.float32) for lead in ((3,), (), (2,), (2,)) for shape in shapes]
    dma, regular, n = pltpu.SemaphoreType.DMA, pltpu.SemaphoreType.REGULAR, len(streams)
    return buffers + [dma((n, 2)), dma((n, 2)), dma((n, 3)), dma((n, 3)), regular((n,)), regular((n,))] + [dma((len(arrays),))] * 3


def split_scratch(refs, n_arrays):
    buffers, sems = refs[:4 * n_arrays], refs[4 * n_arrays:4 * n_arrays + 9]
    return [buffers[n_arrays * b:n_arrays * (b + 1)] for b in range(4)], sems


def term_of(streams, lefts, rights):
    def term(i, chip, core):
        arr, row, rows, col, cols, _ = streams[i]
        half = ARRAYS[arr][1] // 2
        first = pl.multiple_of(2 * chip * ARRAYS[arr][0] + row, 16)
        return dot_nn(lefts[arr][pl.ds(first, rows), :], rights[arr][:, pl.ds(pl.multiple_of(core * half + col, 128), cols)])
    return term


HEAD_GROUP, HEAD_DIM, SEQ, N_TOKEN = 256, 64, 64, 50
ROWS = 256
LOGIT_SCALE = HEAD_DIM ** -0.5
VEC_NAMES = ('b_patch', 'cls_tok', 'lnp_g', 'lnp_b', 'ln1_g', 'ln1_b', 'b_out', 'ln2_g', 'ln2_b', 'b_proj')
VEC_AT = {name: place for place, name in enumerate(VEC_NAMES)}
VEC_QKV, VEC_FC, VEC_ROWS = 10, 13, 24


def dot_nn(left, right):
    return lax.dot_general(left, right, (((1,), (0,)), ((), ())), preferred_element_type=jnp.float32)


def dot_nt(left, right):
    return lax.dot_general(left, right, (((1,), (1,)), ((), ())), preferred_element_type=jnp.float32)


def dot_tn(left, right):
    return lax.dot_general(left, right, (((0,), (0,)), ((), ())), preferred_element_type=jnp.float32)


def normalize(x_in):
    centered = x_in - jnp.mean(x_in, axis=-1, keepdims=True)
    inv_std = lax.rsqrt(jnp.mean(centered * centered, axis=-1, keepdims=True) + LN_EPS)
    return centered * inv_std, inv_std


def normalize_back(d_norm, x_hat, inv_std, gain):
    d_hat = d_norm * gain
    return inv_std * (d_hat - jnp.mean(d_hat, axis=-1, keepdims=True) - x_hat * jnp.mean(d_hat * x_hat, axis=-1, keepdims=True))


def lane_ids(shape):
    return lax.broadcasted_iota(jnp.int32, shape, 1)


def stack_heads(block):
    head = lane_ids((1, HEAD_GROUP)) // HEAD_DIM
    return jnp.concatenate([block * (head == h).astype(jnp.bfloat16) for h in range(4)], axis=0)


def unstack_heads(stacked):
    head = lane_ids((1, HEAD_GROUP)) // HEAD_DIM
    total = jnp.where(head == 0, stacked[:SEQ], 0.0)
    for h in range(1, 4):
        total = jnp.where(head == h, stacked[h * SEQ:(h + 1) * SEQ], total)
    return total


def per_head(block, reducer, neutral):
    halves = []
    for j in range(2):
        half = block[:, 128 * j:128 * (j + 1)]
        low = lane_ids(half.shape) < HEAD_DIM
        first = reducer(jnp.where(low, half, neutral), axis=1, keepdims=True)
        second = reducer(jnp.where(low, neutral, half), axis=1, keepdims=True)
        halves.append(jnp.where(low, first, second))
    return jnp.concatenate(halves, axis=1)


def probabilities(q_block, k_stack):
    logits = dot_nt(q_block, k_stack) * LOGIT_SCALE
    logits = jnp.where(lane_ids(logits.shape) % HEAD_DIM < N_TOKEN, logits, -jnp.inf)
    powers = jnp.exp(logits - per_head(logits, jnp.max, -jnp.inf))
    return powers / per_head(powers, jnp.sum, 0.0)


def row_of(vecs, name):
    place = VEC_AT[name]
    return vecs[place:place + 1, :]


def is_cls(rows):
    return lax.broadcasted_iota(jnp.int32, (rows, 1), 0) % SEQ == 0


PAIR = 2 * SEQ


def gather_second_kernel(*refs):
    fc_shard, proj_shard, in_hbm, misc_hbm, qkv_w_hbm, out_w_hbm, vecs = refs[:7]
    fc_whole, proj_whole = refs[7:9]
    results = refs[9:16]
    x_in, misc, w_qkv, w_out, h_zero, ctx = refs[16:22]
    buffers = refs[22:29]
    x_zero, a_turned, qkv, ctx_turned, h_mid, c_out, c_turned = buffers
    load_sem, out_sem = refs[29:31]
    place = Place()
    loads = [pltpu.make_async_copy(src, dst, load_sem.at[n]) for n, (src, dst) in enumerate(
        ((in_hbm, x_in), (misc_hbm, misc), (qkv_w_hbm, w_qkv), (out_w_hbm, w_out)))]
    for load in loads:
        load.start()
    place.meet()

    def pair_out(p, slot):
        span = pl.ds(pl.multiple_of(p * PAIR, PAIR), PAIR)
        for n, (src, dst) in enumerate(zip(buffers, results)):
            target = dst.at[:, span] if n in (1, 3, 6) else dst.at[span, :]
            yield pltpu.make_async_copy(src.at[slot], target, out_sem.at[n, slot])

    def enter(p, slot):
        rows = pl.ds(pl.multiple_of(p * PAIR, PAIR), PAIR)
        start = jnp.where(is_cls(PAIR), row_of(vecs, 'cls_tok'), row_of(vecs, 'b_patch'))
        x_sum = dot_nt(x_in[rows, :], misc[...]) + start
        x_zero[slot] = x_sum
        h_sum = normalize(x_sum)[0] * row_of(vecs, 'lnp_g') + row_of(vecs, 'lnp_b')
        h_zero[...] = h_sum
        a_in = (normalize(h_sum)[0] * row_of(vecs, 'ln1_g') + row_of(vecs, 'ln1_b')).astype(jnp.bfloat16)
        a_turned[slot] = a_in.T
        for s in range(3):
            cols = pl.ds(1024 * s, 1024)
            qkv[slot, :, cols] = (dot_nn(a_in, w_qkv[:, cols]) + vecs[VEC_QKV + s:VEC_QKV + s + 1, :]).astype(jnp.bfloat16)

    def attend(slot):
        for b in range(2):
            rows = pl.ds(b * SEQ, SEQ)
            for g in range(4):
                q_block, k_block, v_block = [qkv[slot, rows, pl.ds(1024 * s + HEAD_GROUP * g, HEAD_GROUP)] for s in range(3)]
                prob = probabilities(q_block, stack_heads(k_block)).astype(jnp.bfloat16)
                ctx[rows, pl.ds(HEAD_GROUP * g, HEAD_GROUP)] = dot_nn(prob, stack_heads(v_block)).astype(jnp.bfloat16)
        context = ctx[...]
        ctx_turned[slot] = context.T
        mid = h_zero[...] + dot_nn(context, w_out[...]) + row_of(vecs, 'b_out')
        h_mid[slot] = mid
        c_in = (normalize(mid)[0] * row_of(vecs, 'ln2_g') + row_of(vecs, 'ln2_b')).astype(jnp.bfloat16)
        c_out[slot] = c_in
        c_turned[slot] = c_in.T

    def hook(step):
        p = lax.div(step, 2)
        slot = lax.rem(p, 2)

        @pl.when(step == 0)
        def _():
            for load in loads:
                load.wait()

        @pl.when(lax.rem(step, 2) == 0)
        def _():
            @pl.when(p >= 2)
            def _():
                for copy in pair_out(p - 2, slot):
                    copy.wait()
            enter(p, slot)

        @pl.when(lax.rem(step, 2) == 1)
        def _():
            attend(slot)
            for copy in pair_out(p, slot):
                copy.start()

    RingGather(place, SECOND_ARRAYS, SECOND_STREAMS, (fc_shard, proj_shard), (fc_whole, proj_whole), refs[31:]).run(hook)
    for p in (N_CHIP // 2 - 2, N_CHIP // 2 - 1):
        for copy in pair_out(p, p % 2):
            copy.wait()


def gather_second(fc_shard, proj_shard, x_in, misc, w_qkv, w_out, vecs):
    bf, f32, dma = jnp.bfloat16, jnp.float32, pltpu.SemaphoreType.DMA
    n_rows = x_in.shape[0]
    assert n_rows // SEQ == N_CHIP
    anywhere, vmem = pl.BlockSpec(memory_space=pl.ANY), pl.BlockSpec(memory_space=pltpu.VMEM)
    kinds = ((1024, f32), (-1024, bf), (3072, bf), (-1024, bf), (1024, f32), (1024, bf), (-1024, bf))
    out_shape = gathered_shapes(SECOND_ARRAYS) + [jax.ShapeDtypeStruct((n_rows, width) if width > 0 else (-width, n_rows), dtype) for width, dtype in kinds]
    scratch = [pltpu.VMEM(a.shape, bf) for a in (x_in, misc, w_qkv, w_out)] + [pltpu.VMEM((PAIR, 1024), f32), pltpu.VMEM((PAIR, 1024), bf)]
    scratch += [pltpu.VMEM((2, PAIR, width) if width > 0 else (2, -width, PAIR), dtype) for width, dtype in kinds]
    scratch += [dma((4,)), dma((7, 2))]
    return pl.pallas_call(
        gather_second_kernel, out_shape=out_shape, in_specs=[vmem, vmem] + [anywhere] * 4 + [vmem], out_specs=[anywhere] * len(out_shape),
        scratch_shapes=scratch + gather_sems(SECOND_ARRAYS, SECOND_STREAMS),
        compiler_params=pltpu.CompilerParams(collective_id=3, has_side_effects=True, vmem_limit_bytes=62 * 1024 * 1024), name='gather_second',
    )(fc_shard, proj_shard, x_in, misc, w_qkv, w_out, vecs)


def add_row(sums, place, value):
    sums[place:place + 1, :] += jnp.sum(value, axis=0, keepdims=True)


def clear_first(sums):
    @pl.when(pl.program_id(0) == 0)
    def _():
        sums[...] = jnp.zeros_like(sums)


def stage_two(c_in, h_mid, grad_h1, w_fc, w_proj, vecs, gelu_turned, d_pre_out, h_one, d_mid, d_mid_b, sums, h_acc, d_c_acc):
    clear_first(sums)
    c_block, g_block = c_in[...], grad_h1[...]
    tile = 1024
    for f in range(4096 // tile):
        cols = pl.ds(tile * f, tile)
        pre_act = dot_nn(c_block, w_fc[:, cols]) + vecs[VEC_FC + f:VEC_FC + f + 1, :]
        normal_cdf = 0.5 * (1.0 + lax.erf(pre_act * INV_SQRT2))
        gelu = (pre_act * normal_cdf).astype(jnp.bfloat16)
        gelu_turned[cols, :] = gelu.T
        slope = normal_cdf + pre_act * jnp.exp(-0.5 * pre_act * pre_act) * INV_SQRT_2PI
        d_pre = dot_nt(g_block, w_proj[cols, :]) * slope
        add_row(sums, VEC_FC + f, d_pre)
        d_pre_b = d_pre.astype(jnp.bfloat16)
        d_pre_out[:, cols] = d_pre_b
        h_part = dot_nn(gelu, w_proj[cols, :])
        d_part = dot_nt(d_pre_b, w_fc[:, cols])
        if f == 0:
            h_acc[...] = h_part
            d_c_acc[...] = d_part
        else:
            h_acc[...] += h_part
            d_c_acc[...] += d_part
    mid = h_mid[...]
    h_one[...] = (mid + h_acc[...] + row_of(vecs, 'b_proj')).astype(jnp.bfloat16)
    d_c = d_c_acc[...]
    x_hat, inv_std = normalize(mid)
    d_h = g_block.astype(jnp.float32)
    d_sum = normalize_back(d_c, x_hat, inv_std, row_of(vecs, 'ln2_g')) + d_h
    d_mid[...] = d_sum
    d_mid_b[...] = d_sum.astype(jnp.bfloat16)
    add_row(sums, VEC_AT['ln2_g'], d_c * x_hat)
    add_row(sums, VEC_AT['ln2_b'], d_c)
    add_row(sums, VEC_AT['b_proj'], d_h)
    add_row(sums, VEC_AT['b_out'], d_sum)


def context_back(b, qkv, d_ctx, d_qkv, d_part):
    for g in range(4):
        places = [pl.ds(1024 * s + HEAD_GROUP * g, HEAD_GROUP) for s in range(3)]
        q_block, k_block, v_block = [qkv[b, :, place] for place in places]
        d_block = d_ctx[:, HEAD_GROUP * g:HEAD_GROUP * (g + 1)]
        k_stack = stack_heads(k_block)
        prob = probabilities(q_block, k_stack)
        d_prob = dot_nt(d_block, stack_heads(v_block))
        d_logit = (prob * (d_prob - per_head(prob * d_prob, jnp.sum, 0.0)) * LOGIT_SCALE).astype(jnp.bfloat16)
        g_q = dot_nn(d_logit, k_stack)
        g_k = unstack_heads(dot_tn(d_logit, q_block))
        g_v = unstack_heads(dot_tn(prob.astype(jnp.bfloat16), d_block))
        for place, grad in zip(places, (g_q, g_k, g_v)):
            d_qkv[b, :, place] = grad.astype(jnp.bfloat16)
            d_part[:, place] += jnp.sum(grad.reshape(SEQ // 8, 8, HEAD_GROUP), axis=0)


def entry_back(x_sum, d_mid, d_a, vecs, sums):
    hat_p, inv_p = normalize(x_sum)
    h_zero = hat_p * row_of(vecs, 'lnp_g') + row_of(vecs, 'lnp_b')
    hat_1, inv_1 = normalize(h_zero)
    add_row(sums, VEC_AT['ln1_g'], d_a * hat_1)
    add_row(sums, VEC_AT['ln1_b'], d_a)
    d_zero = normalize_back(d_a, hat_1, inv_1, row_of(vecs, 'ln1_g')) + d_mid
    add_row(sums, VEC_AT['lnp_g'], d_zero * hat_p)
    add_row(sums, VEC_AT['lnp_b'], d_zero)
    d_x = normalize_back(d_zero, hat_p, inv_p, row_of(vecs, 'lnp_g'))
    cls = is_cls(SEQ)
    d_emb = jnp.where(cls, 0.0, d_x)
    add_row(sums, VEC_AT['cls_tok'], jnp.where(cls, d_x, 0.0))
    add_row(sums, VEC_AT['b_patch'], d_emb)
    return d_emb.astype(jnp.bfloat16)


def mlp_sums_kernel(*refs):
    (c_hbm, pre_hbm, gelu_hbm, rows_hbm, qkv_w_hbm, out_w_hbm, vecs, x_hbm, mid_hbm, mid_b_hbm, qkv_hbm) = refs[:11]
    fc_out, proj_out, d_qkv_out, d_emb_out, sums = refs[11:16]
    (c_turned, d_pre, gelu_turned, grad_rows, w_qkv, w_out, x_zero, d_mid, d_mid_b, qkv, d_qkv, d_emb, d_part,
     load_sem, in_sem, out_sem) = refs[16:32]
    (accs, owns, gives, twins), sems = split_scratch(refs[32:], 2)
    place = Place()
    loads = [pltpu.make_async_copy(src, dst, load_sem.at[n]) for n, (src, dst) in enumerate(
        ((c_hbm, c_turned), (pre_hbm, d_pre), (gelu_hbm, gelu_turned), (rows_hbm, grad_rows), (qkv_w_hbm, w_qkv), (out_w_hbm, w_out)))]
    for load in loads:
        load.start()
    n_img = x_hbm.shape[0] // SEQ

    def image_in(b, slot):
        rows = pl.ds(pl.multiple_of(b * SEQ, SEQ), SEQ)
        return [pltpu.make_async_copy(src.at[rows, :], dst.at[slot], in_sem.at[n, slot]) for n, (src, dst) in enumerate(
            ((x_hbm, x_zero), (mid_hbm, d_mid), (mid_b_hbm, d_mid_b), (qkv_hbm, qkv)))]

    def image_out(b, slot):
        rows = pl.ds(pl.multiple_of(b * SEQ, SEQ), SEQ)
        return [pltpu.make_async_copy(src.at[slot], dst.at[rows, :], out_sem.at[n, slot]) for n, (src, dst) in enumerate(
            ((d_qkv, d_qkv_out), (d_emb, d_emb_out)))]

    for copy in image_in(0, 0):
        copy.start()
    sums[...] = jnp.zeros_like(sums)
    d_part[...] = jnp.zeros_like(d_part)
    place.meet()
    term = term_of(MLP_STREAMS, {FC: c_turned, PROJ: gelu_turned}, {FC: d_pre, PROJ: grad_rows})
    ring = RingSum(place, (FC, PROJ), MLP_STREAMS, accs, owns, gives, twins, sems, term)
    for load in loads:
        load.wait()

    def hook(half, step):
        slot = lax.rem(step, 2)
        if half == 0:
            @pl.when(step < n_img - 1)
            def _():
                for copy in image_in(step + 1, 1 - slot):
                    copy.start()

            for copy in image_in(step, slot):
                copy.wait()

            @pl.when(step >= 2)
            def _():
                for copy in image_out(step - 2, slot):
                    copy.wait()

            d_ctx = dot_nt(d_mid_b[slot], w_out[...]).astype(jnp.bfloat16)
            context_back(slot, qkv, d_ctx, d_qkv, d_part)
        else:
            d_a = dot_nt(d_qkv[slot], w_qkv[...])
            d_emb[slot] = entry_back(x_zero[slot], d_mid[slot], d_a, vecs, sums)
            for copy in image_out(step, slot):
                copy.start()

    ring.run((tuple(range(6)), tuple(range(6, len(MLP_STREAMS)))), hook)
    for step in (n_img - 2, n_img - 1):
        for copy in image_out(step, step % 2):
            copy.wait()
    for s in range(3):
        add_row(sums, VEC_QKV + s, d_part[:, pl.ds(1024 * s, 1024)])
    ring.finish((fc_out, proj_out))


def mlp_sums(c_turned, d_pre, gelu_turned, grad_rows, w_qkv, w_out, vecs, x_zero, d_mid, d_mid_b, qkv):
    bf, f32, dma = jnp.bfloat16, jnp.float32, pltpu.SemaphoreType.DMA
    n_rows = x_zero.shape[0]
    assert n_rows // SEQ == N_CHIP
    out_shape = [jax.ShapeDtypeStruct(ARRAYS[FC], f32), jax.ShapeDtypeStruct(ARRAYS[PROJ], f32), jax.ShapeDtypeStruct((n_rows, 3072), bf),
                 jax.ShapeDtypeStruct((n_rows, 1024), bf), jax.ShapeDtypeStruct((VEC_ROWS, 1024), f32)]
    anywhere, vmem = pl.BlockSpec(memory_space=pl.ANY), pl.BlockSpec(memory_space=pltpu.VMEM)
    scratch = [pltpu.VMEM(a.shape, bf) for a in (c_turned, d_pre, gelu_turned, grad_rows, w_qkv, w_out)]
    scratch += [pltpu.VMEM((2, SEQ, 1024), f32), pltpu.VMEM((2, SEQ, 1024), f32), pltpu.VMEM((2, SEQ, 1024), bf), pltpu.VMEM((2, SEQ, 3072), bf),
                pltpu.VMEM((2, SEQ, 3072), bf), pltpu.VMEM((2, SEQ, 1024), bf), pltpu.VMEM((8, 3072), f32), dma((6,)), dma((4, 2)), dma((2, 2))]
    return pl.pallas_call(
        mlp_sums_kernel, out_shape=out_shape, in_specs=[anywhere] * 6 + [vmem] + [anywhere] * 4, out_specs=[anywhere] * 4 + [vmem],
        scratch_shapes=scratch + ring_scratch((FC, PROJ), MLP_STREAMS),
        compiler_params=pltpu.CompilerParams(collective_id=1, has_side_effects=True, vmem_limit_bytes=62 * 1024 * 1024), name='mlp_sums',
    )(c_turned, d_pre, gelu_turned, grad_rows, w_qkv, w_out, vecs, x_zero, d_mid, d_mid_b, qkv)


def rest_sums_kernel(*refs):
    (a_hbm, dqkv_hbm, ctx_hbm, mid_hbm, emb_hbm, in_hbm, vec_hbm) = refs[:7]
    outs = refs[7:10]
    (a_turned, d_qkv, ctx_turned, d_mid_b, emb_turned, x_in, g_vec, load_sem) = refs[10:18]
    (accs, owns, gives, twins), sems = split_scratch(refs[18:], 3)
    place = Place()
    loads = [pltpu.make_async_copy(src, dst, load_sem.at[n]) for n, (src, dst) in enumerate(
        ((a_hbm, a_turned), (dqkv_hbm, d_qkv), (ctx_hbm, ctx_turned), (mid_hbm, d_mid_b), (emb_hbm, emb_turned), (in_hbm, x_in), (vec_hbm, g_vec)))]
    for load in loads:
        load.start()
    place.meet()
    product = term_of(REST_STREAMS, {QKV: a_turned, OUT: ctx_turned, MISC: emb_turned}, {QKV: d_qkv, OUT: d_mid_b, MISC: x_in})

    def term(i, chip, core):
        arr, row, rows, col, cols, _ = REST_STREAMS[i]
        block = product(i, chip, core)
        if arr == MISC and col >= 256:
            first = pl.multiple_of(2 * chip * ARRAYS[arr][0] + row, 16)
            block = block + jnp.where(core == 1, g_vec[pl.ds(first, rows), pl.ds(col - 256, cols)], 0.0)
        return block

    ring = RingSum(place, (QKV, OUT, MISC), REST_STREAMS, accs, owns, gives, twins, sems, term)
    for load in loads:
        load.wait()
    ring.run((tuple(range(6)), tuple(range(6, len(REST_STREAMS)))), lambda half, step: None)
    ring.finish(outs)


def rest_sums(a_turned, d_qkv, ctx_turned, d_mid_b, emb_turned, x_in, g_vec):
    arrays = (QKV, OUT, MISC)
    operands = (a_turned, d_qkv, ctx_turned, d_mid_b, emb_turned, x_in, g_vec)
    anywhere = pl.BlockSpec(memory_space=pl.ANY)
    return pl.pallas_call(
        rest_sums_kernel, out_shape=[jax.ShapeDtypeStruct(ARRAYS[arr], jnp.float32) for arr in arrays],
        in_specs=[anywhere] * 7, out_specs=[anywhere] * 3,
        scratch_shapes=[pltpu.VMEM(a.shape, a.dtype) for a in operands] + [pltpu.SemaphoreType.DMA((7,))] + ring_scratch(arrays, REST_STREAMS),
        compiler_params=pltpu.CompilerParams(collective_id=2, has_side_effects=True, vmem_limit_bytes=62 * 1024 * 1024), name='rest_sums',
    )(*operands)


def whole(shape):
    return pl.BlockSpec(shape, lambda i: (0, 0), pipeline_mode=pl.Buffered(1))


def rows_of(width):
    return pl.BlockSpec((ROWS, width), lambda i: (i, 0))


def stage_call(body, name, n_rows, ins, outs, scratch=()):
    in_specs = [rows_of(a.shape[1]) if a.shape[0] == n_rows and not held else whole(a.shape) for a, held in ins]
    out_specs, out_shape = [], []
    for width, dtype in outs:
        if dtype is None:
            out_specs.append(pl.BlockSpec((VEC_ROWS, 1024), lambda i: (0, 0)))
            out_shape.append(jax.ShapeDtypeStruct((VEC_ROWS, 1024), jnp.float32))
        elif width < 0:
            out_specs.append(pl.BlockSpec((-width, ROWS), lambda i: (0, i)))
            out_shape.append(jax.ShapeDtypeStruct((-width, n_rows), dtype))
        else:
            out_specs.append(rows_of(width))
            out_shape.append(jax.ShapeDtypeStruct((n_rows, width), dtype))
    return pl.pallas_call(body, grid=(n_rows // ROWS,), in_specs=in_specs, out_specs=out_specs, out_shape=out_shape, scratch_shapes=list(scratch),
                          compiler_params=pltpu.CompilerParams(vmem_limit_bytes=62 * 1024 * 1024, dimension_semantics=('arbitrary',)), name=name)(*[a for a, _ in ins])

N_PIXEL, N_POS = 768, 197
MISC_USED = N_PIXEL + N_POS + len(VEC_NAMES) + 3 + 4


def solution(mesh):
    def spec_of(name):
        return P(None, MESH_AXIS) if name in LAST_SPLIT else P(MESH_AXIS)

    def vector_columns(part, rows):
        columns = [part[name].reshape(rows, 1) for name in VEC_NAMES] + [part['b_qkv'].reshape(rows, 3), part['b_fc'].reshape(rows, 4)]
        return jnp.pad(jnp.concatenate(columns, axis=1), ((0, 0), (0, 1024 - MISC_USED)))

    def pack_misc(part):
        rows = part['w_patch'].shape[1]
        return jnp.concatenate([part['w_patch'].T, part['pos_table'].T, vector_columns(part, rows)], axis=1)

    def unpack_misc(misc):
        part = {'w_patch': misc[:, :N_PIXEL].T, 'pos_table': misc[:, N_PIXEL:N_PIXEL + N_POS].T}
        first = N_PIXEL + N_POS
        for place, name in enumerate(VEC_NAMES):
            part[name] = misc[:, first + place]
        first += len(VEC_NAMES)
        part['b_qkv'] = misc[:, first:first + 3].reshape(-1)
        part['b_fc'] = misc[:, first + 3:first + 7].reshape(-1)
        return part

    def local_step(patches, keep, *rest):
        shards = dict(zip(PARAM_NAMES, rest[:-1]))
        grad_h1 = rest[-1]
        n_img, n_patch, _ = patches.shape
        n_token, d_model = grad_h1.shape[1:]
        n_shard, _, n_heads, head_dim = shards['w_qkv'].shape
        n_rows = n_img * SEQ
        casts = {name: shards[name].astype(jnp.bfloat16) for name in PARAM_NAMES}
        w_qkv, w_out, misc = gather_first((casts['w_qkv'].reshape(n_shard, -1), casts['w_out'], pack_misc(casts)))
        position = jnp.pad(keep + 1, ((0, 0), (1, 0)))
        position = jnp.pad(position, ((0, 0), (0, SEQ - n_token)), constant_values=-1)[:, :, None]
        onehot_patch = (position == 1 + lax.broadcasted_iota(jnp.int32, (1, 1, n_patch), 2)).astype(jnp.bfloat16)
        onehot_pos = (position == lax.broadcasted_iota(jnp.int32, (1, 1, 1024 - N_PIXEL), 2)).astype(jnp.bfloat16)
        kept_rows = jnp.einsum('bkp,bpq->bkq', onehot_patch, patches, preferred_element_type=jnp.float32).astype(jnp.bfloat16)
        x_in = jnp.concatenate([kept_rows, onehot_pos], axis=2).reshape(n_rows, 1024)
        grad_rows = jnp.pad(grad_h1, ((0, 0), (0, SEQ - n_token), (0, 0))).reshape(n_rows, d_model)

        vec_part = misc[:, N_PIXEL + N_POS:MISC_USED].astype(jnp.float32)
        n_vec = len(VEC_NAMES)
        vecs = jnp.concatenate([vec_part[:, :n_vec].T, vec_part[:, n_vec:n_vec + 3].reshape(3, 1024), vec_part[:, n_vec + 3:].reshape(4, 1024)], axis=0)
        vecs = jnp.pad(vecs, ((0, VEC_ROWS - vecs.shape[0]), (0, 0)))

        bf, f32 = jnp.bfloat16, jnp.float32
        w_fc, w_proj, x_zero, a_turned, qkv, ctx_turned, h_mid, c_in, c_turned = gather_second(casts['w_fc'], casts['w_proj'], x_in, misc, w_qkv, w_out, vecs)
        gelu_turned, d_pre, h_one, d_mid, d_mid_b, sums_two = stage_call(
            stage_two, 'stage_two', n_rows, [(c_in, False), (h_mid, False), (grad_rows, False), (w_fc, True), (w_proj, True), (vecs, True)],
            [(-4096, bf), (4096, bf), (1024, bf), (1024, f32), (1024, bf), (0, None)],
            [pltpu.VMEM((ROWS, 1024), f32), pltpu.VMEM((ROWS, 1024), f32)])
        h_one = h_one.reshape(n_img, SEQ, d_model)[:, :n_token]
        fc_sum, proj_sum, d_qkv, d_emb, sums_three = mlp_sums(c_turned, d_pre, gelu_turned, grad_rows, w_qkv, w_out, vecs, x_zero, d_mid, d_mid_b, qkv)
        sums = sums_two + sums_three
        vec_rows = jnp.concatenate([sums[:n_vec], sums[VEC_QKV:VEC_QKV + 3].reshape(1024, 3).T, sums[VEC_FC:VEC_FC + 4].reshape(1024, 4).T], axis=0)
        g_rows = jnp.concatenate([sums[VEC_AT['cls_tok']][None], jnp.zeros((N_POS - 1, 1024), f32), vec_rows], axis=0)
        g_vec = jnp.pad(g_rows, ((0, 1024 - N_PIXEL - g_rows.shape[0]), (0, 0))).T
        qkv_sum, out_sum, misc_sum = rest_sums(a_turned, d_qkv, ctx_turned, d_mid_b, d_emb.T, x_in, g_vec)
        own = unpack_misc(misc_sum)
        own.update(w_fc=fc_sum, w_proj=proj_sum, w_qkv=qkv_sum.reshape(n_shard, 3, n_heads, head_dim), w_out=out_sum)
        return (h_one,) + tuple(own[name] for name in PARAM_NAMES)

    batch_spec = P(MESH_AXIS)
    param_specs = tuple(spec_of(name) for name in PARAM_NAMES)
    return jax.shard_map(local_step, mesh=mesh, in_specs=(batch_spec, batch_spec) + param_specs + (batch_spec,), out_specs=(batch_spec,) + param_specs, check_vma=False)
```

```python
import jax
import jax.numpy as jnp
from jax import lax
from jax.experimental import pallas as pl
from jax.experimental.pallas import tpu as pltpu
from jax.sharding import PartitionSpec as P

MESH_AXIS = 'fsdp'
LN_EPS = 1e-5
INV_SQRT2 = 0.7071067811865476
INV_SQRT_2PI = 0.3989422804014327
PARAM_NAMES = ('w_patch', 'b_patch', 'pos_table', 'cls_tok', 'lnp_g', 'lnp_b', 'ln1_g', 'ln1_b', 'w_qkv', 'b_qkv', 'w_out', 'b_out', 'ln2_g', 'ln2_b', 'w_fc', 'b_fc', 'w_proj', 'b_proj')
LAST_SPLIT = ('w_patch', 'pos_table')


RINGS = (
    (0, 4, 8, 10, 11, 15, 14, 12, 13, 9, 5, 7, 6, 2, 3, 1),
    (0, 2, 3, 7, 11, 9, 8, 12, 13, 15, 14, 10, 6, 4, 5, 1),
    (0, 1, 3, 7, 5, 4, 8, 9, 11, 15, 13, 12, 14, 10, 6, 2),
    (0, 1, 5, 7, 3, 2, 6, 10, 14, 15, 11, 9, 13, 12, 8, 4),
    (0, 4, 6, 7, 11, 10, 8, 12, 14, 15, 13, 9, 5, 1, 3, 2),
    (0, 2, 6, 7, 3, 1, 5, 9, 13, 15, 11, 10, 14, 12, 8, 4),
)
N_CHIP = 16
MESH_ID = pl.DeviceIdType.MESH
ARRAYS = ((32, 4096), (128, 1024), (32, 3072), (32, 1024), (32, 1024))
FC, PROJ, QKV, OUT, MISC = range(5)
FIRST_STREAMS = tuple((QKV, 0, 32, 512 * k, 512, k) for k in range(6)) + (
    (OUT, 0, 32, 0, 384, 0), (OUT, 0, 32, 384, 384, 1), (OUT, 0, 32, 768, 256, 4),
    (MISC, 0, 32, 0, 384, 2), (MISC, 0, 32, 384, 384, 3), (MISC, 0, 32, 768, 256, 5))
SECOND_STREAMS = (
    (FC, 0, 32, 0, 896, 0), (FC, 0, 32, 896, 896, 1), (FC, 0, 32, 1792, 384, 2), (FC, 0, 32, 2176, 384, 3),
    (FC, 0, 32, 2560, 768, 4), (FC, 0, 32, 3328, 768, 5), (PROJ, 0, 128, 0, 128, 0), (PROJ, 0, 128, 128, 128, 1),
    (PROJ, 0, 128, 256, 256, 2), (PROJ, 0, 128, 512, 256, 3), (PROJ, 0, 128, 768, 128, 4), (PROJ, 0, 128, 896, 128, 5))
MLP_STREAMS = tuple((FC, 0, 64, 384 * k, 384, k) for k in range(4)) + ((FC, 0, 64, 1536, 256, 4), (FC, 0, 64, 1792, 256, 5)) + tuple(
    (PROJ, 128 * (place % 2), 128, 128 * (place // 2), 128, ring) for place, ring in enumerate((0, 1, 2, 3, 4, 5, 4, 5)))
REST_STREAMS = tuple((QKV, 0, 64, 256 * k, 256, k) for k in range(6)) + tuple((OUT, 0, 64, 128 * k, 128, k) for k in range(4)) + (
    (MISC, 0, 64, 0, 128, 4), (MISC, 0, 64, 128, 128, 5), (MISC, 0, 32, 256, 128, 0), (MISC, 32, 32, 256, 128, 1),
    (MISC, 0, 32, 384, 128, 2), (MISC, 32, 32, 384, 128, 3))


def pick(table, index):
    value = jnp.int32(table[0])
    for place in range(1, len(table)):
        value = jnp.where(index == place, jnp.int32(table[place]), value)
    return value


class Place:
    def __init__(self):
        me = lax.axis_index(MESH_AXIS)
        self.core = lax.rem(me, 2)
        self.chip = lax.div(me, 2)
        self.sibling = me + 1 - 2 * self.core
        where_in = [[ring.index(chip) for chip in range(N_CHIP)] for ring in RINGS]
        self.spot = [pick(table, self.chip) for table in where_in]
        self.after = [2 * pick([ring[(table[chip] + 1) % N_CHIP] for chip in range(N_CHIP)], self.chip) + self.core
                      for ring, table in zip(RINGS, where_in)]
        self.before = [2 * pick([ring[(table[chip] - 1) % N_CHIP] for chip in range(N_CHIP)], self.chip) + self.core
                       for ring, table in zip(RINGS, where_in)]

    def chips_back(self, steps):
        return [pick(ring, lax.rem(self.spot[k] + 2 * N_CHIP - steps, N_CHIP)) for k, ring in enumerate(RINGS)]

    def meet(self):
        barrier = pltpu.get_barrier_semaphore()
        for other in self.after + self.before + [self.sibling]:
            pl.semaphore_signal(barrier, inc=1, device_id=(other,), device_id_type=MESH_ID)
        pl.semaphore_wait(barrier, 2 * len(RINGS) + 1)


class RingGather:
    def __init__(self, place, arrays, streams, shards, wholes, sems):
        self.place, self.arrays, self.streams = place, arrays, streams
        self.shards, self.wholes = dict(zip(arrays, shards)), dict(zip(arrays, wholes))
        self.own_sem, self.send_sem, self.recv_sem, self.twin_send, self.twin_recv = sems

    def block(self, i, chip, core):
        arr, row, rows, col, cols, _ = self.streams[i]
        first = (2 * chip + core) * ARRAYS[arr][0] + row
        return self.wholes[arr].at[pl.ds(pl.multiple_of(first, 32), rows), pl.ds(col, cols)]

    def ring_copy(self, i, src, dst, step, back):
        towards, place = (self.place.before, step + N_CHIP // 2) if back else (self.place.after, step)
        return pltpu.make_async_remote_copy(src_ref=src, dst_ref=dst, send_sem=self.send_sem.at[i, place], recv_sem=self.recv_sem.at[i, place],
                                            device_id=(towards[self.streams[i][5]],), device_id_type=MESH_ID)

    def twin_copy(self, i, src, dst, step):
        return pltpu.make_async_remote_copy(src_ref=src, dst_ref=dst, send_sem=self.twin_send.at[i, step], recv_sem=self.twin_recv.at[i, step],
                                            device_id=(self.place.sibling,), device_id_type=MESH_ID)

    def own_copies(self):
        for place, arr in enumerate(self.arrays):
            rows = ARRAYS[arr][0]
            first = pl.multiple_of((2 * self.place.chip + self.place.core) * rows, 32)
            yield pltpu.make_async_copy(self.shards[arr], self.wholes[arr].at[pl.ds(first, rows), :], self.own_sem.at[place])

    def pass_along(self, step, back):
        place, far = self.place, N_CHIP // 2 - (1 if back else 0)
        chips = place.chips_back(-step if back else step)
        for i in range(len(self.streams)):
            here = self.block(i, chips[self.streams[i][5]], place.core)
            self.ring_copy(i, here, here, step - 1, back).wait_recv()

            @pl.when(step < far)
            def _():
                self.ring_copy(i, here, here, step, back).start()

            self.twin_copy(i, here, here, step + (N_CHIP // 2 if back else 0)).start()

    def run(self, hook):
        place, half = self.place, N_CHIP // 2
        for i in range(len(self.streams)):
            arr, row, rows, col, cols, _ = self.streams[i]
            mine = self.shards[arr].at[pl.ds(row, rows), pl.ds(col, cols)]
            here = self.block(i, place.chip, place.core)
            self.ring_copy(i, mine, here, 0, False).start()
            self.ring_copy(i, mine, here, 0, True).start()
            self.twin_copy(i, mine, here, 0).start()
        for copy in self.own_copies():
            copy.start()
        hook(jnp.int32(0))

        def ring_step(step, carry):
            self.pass_along(step, False)
            hook(2 * step - 1)

            @pl.when(step < half)
            def _():
                self.pass_along(step, True)
                hook(2 * step)
            return carry

        lax.fori_loop(1, half + 1, ring_step, 0)

        def drain(step, carry):
            chips = [place.chips_back(step), place.chips_back(-step)]
            for i in range(len(self.streams)):
                k = self.streams[i][5]
                for back in (False, True):
                    here, there = self.block(i, chips[back][k], place.core), self.block(i, chips[back][k], 1 - place.core)
                    far = half - 1 if back else half

                    @pl.when(step < far)
                    def _():
                        self.ring_copy(i, here, here, step, back).wait_send()

                    at = step + (half if back else 0)

                    @pl.when(jnp.logical_and(step >= 1, step < half) if back else step >= 0)
                    def _():
                        self.twin_copy(i, here, here, at).wait_send()
                        self.twin_copy(i, there, there, at).wait_recv()
            return carry

        lax.fori_loop(0, half + 1, drain, 0)
        for copy in self.own_copies():
            copy.wait()


def gather_sems(arrays, streams):
    ring, twin = pltpu.SemaphoreType.DMA((len(streams), N_CHIP - 1)), pltpu.SemaphoreType.DMA((len(streams), N_CHIP))
    return [pltpu.SemaphoreType.DMA((len(arrays),)), ring, ring, twin, twin]


def gathered_shapes(arrays):
    return [jax.ShapeDtypeStruct((2 * N_CHIP * ARRAYS[arr][0], ARRAYS[arr][1]), jnp.bfloat16) for arr in arrays]


FIRST_ARRAYS, SECOND_ARRAYS = (QKV, OUT, MISC), (FC, PROJ)


def gather_first_kernel(*refs):
    place = Place()
    place.meet()
    RingGather(place, FIRST_ARRAYS, FIRST_STREAMS, refs[:3], refs[3:6], refs[6:]).run(lambda step: None)


def gather_first(shards):
    return pl.pallas_call(
        gather_first_kernel, out_shape=gathered_shapes(FIRST_ARRAYS),
        in_specs=[pl.BlockSpec(memory_space=pltpu.VMEM)] * 3, out_specs=[pl.BlockSpec(memory_space=pl.ANY)] * 3,
        scratch_shapes=gather_sems(FIRST_ARRAYS, FIRST_STREAMS),
        compiler_params=pltpu.CompilerParams(collective_id=0, has_side_effects=True), name='gather_first',
    )(*shards)


class RingSum:
    def __init__(self, place, arrays, streams, accs, owns, gives, twins, sems, term):
        self.place, self.streams, self.term, self.arrays = place, streams, term, arrays
        self.accs, self.owns, self.gives, self.twins = [dict(zip(arrays, refs)) for refs in (accs, owns, gives, twins)]
        (self.twin_send, self.twin_recv, self.send_sem, self.recv_sem, self.ring_free, self.twin_free,
         self.end_own, self.end_send, self.end_recv) = sems

    def part(self, i, ref, *slot):
        _, row, rows, col, cols, _ = self.streams[i]
        return ref.at[(*slot, pl.ds(row, rows), pl.ds(col, cols))]

    def push(self, i, slot):
        arr = self.streams[i][0]
        return pltpu.make_async_remote_copy(src_ref=self.part(i, self.gives[arr], slot), dst_ref=self.part(i, self.twins[arr], slot),
                                            send_sem=self.twin_send.at[i, slot], recv_sem=self.twin_recv.at[i, slot],
                                            device_id=(self.place.sibling,), device_id_type=MESH_ID)

    def pass_on(self, i, slot, slot_next):
        arr, k = self.streams[i][0], self.streams[i][5]
        return pltpu.make_async_remote_copy(src_ref=self.part(i, self.accs[arr], slot), dst_ref=self.part(i, self.accs[arr], slot_next),
                                            send_sem=self.send_sem.at[i, slot], recv_sem=self.recv_sem.at[i, slot_next],
                                            device_id=(self.place.after[k],), device_id_type=MESH_ID)

    def make_own(self, group, step):
        chips = self.place.chips_back(step + 1)
        for i in group:
            arr, k = self.streams[i][0], self.streams[i][5]
            self.part(i, self.owns[arr])[...] = self.term(i, chips[k], self.place.core)

    def make_give(self, group, step):
        chips, slot = self.place.chips_back(step + 1), lax.rem(jnp.int32(step), 2)
        for i in group:
            arr, k = self.streams[i][0], self.streams[i][5]
            self.part(i, self.gives[arr], slot)[...] = self.term(i, chips[k], 1 - self.place.core)

    def push_next(self, group, step):
        slot, slot_next = lax.rem(step, 2), lax.rem(step + 1, 2)
        for i in group:
            self.push(i, slot).wait_send()

            @pl.when(step >= 1)
            def _():
                pl.semaphore_wait(self.twin_free.at[i], 1)
            self.push(i, slot_next).start()

    def advance(self, group, step):
        slot, slot_next, slot_last, pair = lax.rem(step, 3), lax.rem(step + 1, 3), lax.rem(step + 2, 3), lax.rem(step, 2)
        for i in group:
            arr, row, rows, col, cols, k = self.streams[i]
            acc, own, twin = self.part(i, self.accs[arr], slot), self.part(i, self.owns[arr]), self.part(i, self.twins[arr], pair)
            self.push(i, pair).wait_recv()

            @pl.when(step == 0)
            def _():
                acc[...] = own[...] + twin[...]

            @pl.when(step > 0)
            def _():
                self.pass_on(i, slot, slot).wait_recv()
                acc[...] = acc[...] + (own[...] + twin[...])

            @pl.when(jnp.logical_and(step >= 2, step < N_CHIP - 1))
            def _():
                pl.semaphore_wait(self.ring_free.at[i], 1)

            @pl.when(step < N_CHIP - 1)
            def _():
                self.pass_on(i, slot, slot_next).start()

            @pl.when(step < N_CHIP - 2)
            def _():
                pl.semaphore_signal(self.twin_free.at[i], inc=1, device_id=(self.place.sibling,), device_id_type=MESH_ID)

        for i in group:
            k = self.streams[i][5]

            @pl.when(step >= 1)
            def _():
                self.pass_on(i, slot_last, slot).wait_send()

            @pl.when(jnp.logical_and(step >= 1, step < N_CHIP - 2))
            def _():
                pl.semaphore_signal(self.ring_free.at[i], inc=1, device_id=(self.place.before[k],), device_id_type=MESH_ID)

    def run(self, groups, hook):
        for group in groups:
            self.make_give(group, 0)
            for i in group:
                self.push(i, 0).start()
            self.make_own(group, 0)
            self.make_give(group, 1)

        def ring_step(step, carry):
            for place, group in enumerate(groups):
                self.advance(group, step)

                @pl.when(step < N_CHIP - 1)
                def _():
                    self.push_next(group, step)
                    self.make_own(group, step + 1)

                @pl.when(step < N_CHIP - 2)
                def _():
                    self.make_give(group, step + 2)

                hook(place, step)
            return carry

        lax.fori_loop(0, N_CHIP, ring_step, 0)

    def finish(self, outs):
        for i in range(len(self.streams)):
            self.push(i, (N_CHIP - 1) % 2).wait_send()
        last = (N_CHIP - 1) % 3
        ends = []
        for place, arr in enumerate(self.arrays):
            rows, half, core = ARRAYS[arr][0], ARRAYS[arr][1] // 2, self.place.core
            target = outs[place].at[:, pl.ds(pl.multiple_of(core * half, 128), half)]
            keep_rows = self.accs[arr].at[last, pl.ds(pl.multiple_of(core * rows, 32), rows), :]
            give_rows = self.accs[arr].at[last, pl.ds(pl.multiple_of((1 - core) * rows, 32), rows), :]
            ends.append(pltpu.make_async_copy(keep_rows, target, self.end_own.at[place]))
            ends.append(pltpu.make_async_remote_copy(src_ref=give_rows, dst_ref=target, send_sem=self.end_send.at[place], recv_sem=self.end_recv.at[place],
                                                     device_id=(self.place.sibling,), device_id_type=MESH_ID))
        for end in ends:
            end.start()
        for end in ends:
            end.wait()


def ring_scratch(arrays, streams):
    shapes = [(2 * ARRAYS[arr][0], ARRAYS[arr][1] // 2) for arr in arrays]
    buffers = [pltpu.VMEM((*lead, *shape), jnp.float32) for lead in ((3,), (), (2,), (2,)) for shape in shapes]
    dma, regular, n = pltpu.SemaphoreType.DMA, pltpu.SemaphoreType.REGULAR, len(streams)
    return buffers + [dma((n, 2)), dma((n, 2)), dma((n, 3)), dma((n, 3)), regular((n,)), regular((n,))] + [dma((len(arrays),))] * 3


def split_scratch(refs, n_arrays):
    buffers, sems = refs[:4 * n_arrays], refs[4 * n_arrays:4 * n_arrays + 9]
    return [buffers[n_arrays * b:n_arrays * (b + 1)] for b in range(4)], sems


def term_of(streams, lefts, rights):
    def term(i, chip, core):
        arr, row, rows, col, cols, _ = streams[i]
        half = ARRAYS[arr][1] // 2
        first = pl.multiple_of(2 * chip * ARRAYS[arr][0] + row, 16)
        return dot_nn(lefts[arr][pl.ds(first, rows), :], rights[arr][:, pl.ds(pl.multiple_of(core * half + col, 128), cols)])
    return term


HEAD_GROUP, HEAD_DIM, SEQ, N_TOKEN = 256, 64, 64, 50
ROWS = 256
LOGIT_SCALE = HEAD_DIM ** -0.5
VEC_NAMES = ('b_patch', 'cls_tok', 'lnp_g', 'lnp_b', 'ln1_g', 'ln1_b', 'b_out', 'ln2_g', 'ln2_b', 'b_proj')
VEC_AT = {name: place for place, name in enumerate(VEC_NAMES)}
VEC_QKV, VEC_FC, VEC_ROWS = 10, 13, 24


def dot_nn(left, right):
    return lax.dot_general(left, right, (((1,), (0,)), ((), ())), preferred_element_type=jnp.float32)


def dot_nt(left, right):
    return lax.dot_general(left, right, (((1,), (1,)), ((), ())), preferred_element_type=jnp.float32)


def dot_tn(left, right):
    return lax.dot_general(left, right, (((0,), (0,)), ((), ())), preferred_element_type=jnp.float32)


def normalize(x_in):
    centered = x_in - jnp.mean(x_in, axis=-1, keepdims=True)
    inv_std = lax.rsqrt(jnp.mean(centered * centered, axis=-1, keepdims=True) + LN_EPS)
    return centered * inv_std, inv_std


def normalize_back(d_norm, x_hat, inv_std, gain):
    d_hat = d_norm * gain
    return inv_std * (d_hat - jnp.mean(d_hat, axis=-1, keepdims=True) - x_hat * jnp.mean(d_hat * x_hat, axis=-1, keepdims=True))


def lane_ids(shape):
    return lax.broadcasted_iota(jnp.int32, shape, 1)


def stack_heads(block):
    head = lane_ids((1, HEAD_GROUP)) // HEAD_DIM
    return jnp.concatenate([block * (head == h).astype(jnp.bfloat16) for h in range(4)], axis=0)


def unstack_heads(stacked):
    head = lane_ids((1, HEAD_GROUP)) // HEAD_DIM
    total = jnp.where(head == 0, stacked[:SEQ], 0.0)
    for h in range(1, 4):
        total = jnp.where(head == h, stacked[h * SEQ:(h + 1) * SEQ], total)
    return total


def per_head(block, reducer, neutral):
    halves = []
    for j in range(2):
        half = block[:, 128 * j:128 * (j + 1)]
        low = lane_ids(half.shape) < HEAD_DIM
        first = reducer(jnp.where(low, half, neutral), axis=1, keepdims=True)
        second = reducer(jnp.where(low, neutral, half), axis=1, keepdims=True)
        halves.append(jnp.where(low, first, second))
    return jnp.concatenate(halves, axis=1)


def probabilities(q_block, k_stack):
    logits = dot_nt(q_block, k_stack) * LOGIT_SCALE
    logits = jnp.where(lane_ids(logits.shape) % HEAD_DIM < N_TOKEN, logits, -jnp.inf)
    powers = jnp.exp(logits - per_head(logits, jnp.max, -jnp.inf))
    return powers / per_head(powers, jnp.sum, 0.0)


def row_of(vecs, name):
    place = VEC_AT[name]
    return vecs[place:place + 1, :]


def is_cls(rows):
    return lax.broadcasted_iota(jnp.int32, (rows, 1), 0) % SEQ == 0


PAIR = 2 * SEQ


def gather_second_kernel(*refs):
    fc_shard, proj_shard, in_hbm, misc_hbm, qkv_w_hbm, out_w_hbm, vecs = refs[:7]
    fc_whole, proj_whole = refs[7:9]
    results = refs[9:16]
    x_in, misc, w_qkv, w_out, h_zero, ctx = refs[16:22]
    buffers = refs[22:29]
    x_zero, a_turned, qkv, ctx_turned, h_mid, c_out, c_turned = buffers
    load_sem, out_sem = refs[29:31]
    place = Place()
    loads = [pltpu.make_async_copy(src, dst, load_sem.at[n]) for n, (src, dst) in enumerate(
        ((in_hbm, x_in), (misc_hbm, misc), (qkv_w_hbm, w_qkv), (out_w_hbm, w_out)))]
    for load in loads:
        load.start()
    place.meet()

    def pair_out(p, slot):
        span = pl.ds(pl.multiple_of(p * PAIR, PAIR), PAIR)
        for n, (src, dst) in enumerate(zip(buffers, results)):
            target = dst.at[:, span] if n in (1, 3, 6) else dst.at[span, :]
            yield pltpu.make_async_copy(src.at[slot], target, out_sem.at[n, slot])

    def enter(p, slot):
        rows = pl.ds(pl.multiple_of(p * PAIR, PAIR), PAIR)
        start = jnp.where(is_cls(PAIR), row_of(vecs, 'cls_tok'), row_of(vecs, 'b_patch'))
        x_sum = dot_nt(x_in[rows, :], misc[...]) + start
        x_zero[slot] = x_sum
        h_sum = normalize(x_sum)[0] * row_of(vecs, 'lnp_g') + row_of(vecs, 'lnp_b')
        h_zero[...] = h_sum
        a_in = (normalize(h_sum)[0] * row_of(vecs, 'ln1_g') + row_of(vecs, 'ln1_b')).astype(jnp.bfloat16)
        a_turned[slot] = a_in.T
        for s in range(3):
            cols = pl.ds(1024 * s, 1024)
            qkv[slot, :, cols] = (dot_nn(a_in, w_qkv[:, cols]) + vecs[VEC_QKV + s:VEC_QKV + s + 1, :]).astype(jnp.bfloat16)

    def attend(slot):
        for b in range(2):
            rows = pl.ds(b * SEQ, SEQ)
            for g in range(4):
                q_block, k_block, v_block = [qkv[slot, rows, pl.ds(1024 * s + HEAD_GROUP * g, HEAD_GROUP)] for s in range(3)]
                prob = probabilities(q_block, stack_heads(k_block)).astype(jnp.bfloat16)
                ctx[rows, pl.ds(HEAD_GROUP * g, HEAD_GROUP)] = dot_nn(prob, stack_heads(v_block)).astype(jnp.bfloat16)
        context = ctx[...]
        ctx_turned[slot] = context.T
        mid = h_zero[...] + dot_nn(context, w_out[...]) + row_of(vecs, 'b_out')
        h_mid[slot] = mid
        c_in = (normalize(mid)[0] * row_of(vecs, 'ln2_g') + row_of(vecs, 'ln2_b')).astype(jnp.bfloat16)
        c_out[slot] = c_in
        c_turned[slot] = c_in.T

    def hook(step):
        p = lax.div(step, 2)
        slot = lax.rem(p, 2)

        @pl.when(step == 0)
        def _():
            for load in loads:
                load.wait()

        @pl.when(lax.rem(step, 2) == 0)
        def _():
            @pl.when(p >= 2)
            def _():
                for copy in pair_out(p - 2, slot):
                    copy.wait()
            enter(p, slot)

        @pl.when(lax.rem(step, 2) == 1)
        def _():
            attend(slot)
            for copy in pair_out(p, slot):
                copy.start()

    RingGather(place, SECOND_ARRAYS, SECOND_STREAMS, (fc_shard, proj_shard), (fc_whole, proj_whole), refs[31:]).run(hook)
    for p in (N_CHIP // 2 - 2, N_CHIP // 2 - 1):
        for copy in pair_out(p, p % 2):
            copy.wait()


def gather_second(fc_shard, proj_shard, x_in, misc, w_qkv, w_out, vecs):
    bf, f32, dma = jnp.bfloat16, jnp.float32, pltpu.SemaphoreType.DMA
    n_rows = x_in.shape[0]
    assert n_rows // SEQ == N_CHIP
    anywhere, vmem = pl.BlockSpec(memory_space=pl.ANY), pl.BlockSpec(memory_space=pltpu.VMEM)
    kinds = ((1024, f32), (-1024, bf), (3072, bf), (-1024, bf), (1024, f32), (1024, bf), (-1024, bf))
    out_shape = gathered_shapes(SECOND_ARRAYS) + [jax.ShapeDtypeStruct((n_rows, width) if width > 0 else (-width, n_rows), dtype) for width, dtype in kinds]
    scratch = [pltpu.VMEM(a.shape, bf) for a in (x_in, misc, w_qkv, w_out)] + [pltpu.VMEM((PAIR, 1024), f32), pltpu.VMEM((PAIR, 1024), bf)]
    scratch += [pltpu.VMEM((2, PAIR, width) if width > 0 else (2, -width, PAIR), dtype) for width, dtype in kinds]
    scratch += [dma((4,)), dma((7, 2))]
    return pl.pallas_call(
        gather_second_kernel, out_shape=out_shape, in_specs=[vmem, vmem] + [anywhere] * 4 + [vmem], out_specs=[anywhere] * len(out_shape),
        scratch_shapes=scratch + gather_sems(SECOND_ARRAYS, SECOND_STREAMS),
        compiler_params=pltpu.CompilerParams(collective_id=3, has_side_effects=True, vmem_limit_bytes=62 * 1024 * 1024), name='gather_second',
    )(fc_shard, proj_shard, x_in, misc, w_qkv, w_out, vecs)


def add_row(sums, place, value):
    sums[place:place + 1, :] += jnp.sum(value, axis=0, keepdims=True)


def clear_first(sums):
    @pl.when(pl.program_id(0) == 0)
    def _():
        sums[...] = jnp.zeros_like(sums)


def stage_two(c_in, h_mid, grad_h1, w_fc, w_proj, vecs, gelu_turned, d_pre_out, h_one, d_mid, d_mid_b, sums, h_acc, d_c_acc):
    clear_first(sums)
    c_block, g_block = c_in[...], grad_h1[...]
    tile = 1024
    for f in range(4096 // tile):
        cols = pl.ds(tile * f, tile)
        pre_act = dot_nn(c_block, w_fc[:, cols]) + vecs[VEC_FC + f:VEC_FC + f + 1, :]
        normal_cdf = 0.5 * (1.0 + lax.erf(pre_act * INV_SQRT2))
        gelu = (pre_act * normal_cdf).astype(jnp.bfloat16)
        gelu_turned[cols, :] = gelu.T
        slope = normal_cdf + pre_act * jnp.exp(-0.5 * pre_act * pre_act) * INV_SQRT_2PI
        d_pre = dot_nt(g_block, w_proj[cols, :]) * slope
        add_row(sums, VEC_FC + f, d_pre)
        d_pre_b = d_pre.astype(jnp.bfloat16)
        d_pre_out[:, cols] = d_pre_b
        h_part = dot_nn(gelu, w_proj[cols, :])
        d_part = dot_nt(d_pre_b, w_fc[:, cols])
        if f == 0:
            h_acc[...] = h_part
            d_c_acc[...] = d_part
        else:
            h_acc[...] += h_part
            d_c_acc[...] += d_part
    mid = h_mid[...]
    h_one[...] = (mid + h_acc[...] + row_of(vecs, 'b_proj')).astype(jnp.bfloat16)
    d_c = d_c_acc[...]
    x_hat, inv_std = normalize(mid)
    d_h = g_block.astype(jnp.float32)
    d_sum = normalize_back(d_c, x_hat, inv_std, row_of(vecs, 'ln2_g')) + d_h
    d_mid[...] = d_sum
    d_mid_b[...] = d_sum.astype(jnp.bfloat16)
    add_row(sums, VEC_AT['ln2_g'], d_c * x_hat)
    add_row(sums, VEC_AT['ln2_b'], d_c)
    add_row(sums, VEC_AT['b_proj'], d_h)
    add_row(sums, VEC_AT['b_out'], d_sum)


def context_back(slot, b, qkv, d_ctx, d_qkv, d_part):
    rows = pl.ds(b * SEQ, SEQ)
    for g in range(4):
        places = [pl.ds(1024 * s + HEAD_GROUP * g, HEAD_GROUP) for s in range(3)]
        q_block, k_block, v_block = [qkv[slot, rows, place] for place in places]
        d_block = d_ctx[rows, pl.ds(HEAD_GROUP * g, HEAD_GROUP)]
        k_stack = stack_heads(k_block)
        prob = probabilities(q_block, k_stack)
        d_prob = dot_nt(d_block, stack_heads(v_block))
        d_logit = (prob * (d_prob - per_head(prob * d_prob, jnp.sum, 0.0)) * LOGIT_SCALE).astype(jnp.bfloat16)
        g_q = dot_nn(d_logit, k_stack)
        g_k = unstack_heads(dot_tn(d_logit, q_block))
        g_v = unstack_heads(dot_tn(prob.astype(jnp.bfloat16), d_block))
        for place, grad in zip(places, (g_q, g_k, g_v)):
            d_qkv[slot, rows, place] = grad.astype(jnp.bfloat16)
            d_part[:, place] += jnp.sum(grad.reshape(SEQ // 8, 8, HEAD_GROUP), axis=0)


def entry_back(x_sum, d_mid, d_a, vecs, sums):
    hat_p, inv_p = normalize(x_sum)
    h_zero = hat_p * row_of(vecs, 'lnp_g') + row_of(vecs, 'lnp_b')
    hat_1, inv_1 = normalize(h_zero)
    add_row(sums, VEC_AT['ln1_g'], d_a * hat_1)
    add_row(sums, VEC_AT['ln1_b'], d_a)
    d_zero = normalize_back(d_a, hat_1, inv_1, row_of(vecs, 'ln1_g')) + d_mid
    add_row(sums, VEC_AT['lnp_g'], d_zero * hat_p)
    add_row(sums, VEC_AT['lnp_b'], d_zero)
    d_x = normalize_back(d_zero, hat_p, inv_p, row_of(vecs, 'lnp_g'))
    cls = is_cls(PAIR)
    d_emb = jnp.where(cls, 0.0, d_x)
    add_row(sums, VEC_AT['cls_tok'], jnp.where(cls, d_x, 0.0))
    add_row(sums, VEC_AT['b_patch'], d_emb)
    return d_emb.astype(jnp.bfloat16)


def mlp_sums_kernel(*refs):
    (c_hbm, pre_hbm, gelu_hbm, rows_hbm, qkv_w_hbm, out_w_hbm, vecs, x_hbm, mid_hbm, mid_b_hbm, qkv_hbm) = refs[:11]
    fc_out, proj_out, d_qkv_out, d_emb_out, sums = refs[11:16]
    (c_turned, d_pre, gelu_turned, grad_rows, w_qkv, w_out, x_zero, d_mid, d_mid_b, qkv, d_qkv, d_emb, d_part,
     d_ctx, d_a, load_sem, in_sem, out_sem) = refs[16:34]
    (accs, owns, gives, twins), sems = split_scratch(refs[34:], 2)
    place = Place()
    loads = [pltpu.make_async_copy(src, dst, load_sem.at[n]) for n, (src, dst) in enumerate(
        ((c_hbm, c_turned), (pre_hbm, d_pre), (gelu_hbm, gelu_turned), (rows_hbm, grad_rows), (qkv_w_hbm, w_qkv), (out_w_hbm, w_out)))]
    for load in loads:
        load.start()
    n_pair = x_hbm.shape[0] // PAIR

    def span(p):
        return pl.ds(pl.multiple_of(p * PAIR, PAIR), PAIR)

    def pair_in(p, slot):
        return [pltpu.make_async_copy(src.at[span(p), :], dst.at[slot], in_sem.at[n, slot]) for n, (src, dst) in enumerate(
            ((x_hbm, x_zero), (mid_hbm, d_mid), (mid_b_hbm, d_mid_b), (qkv_hbm, qkv)))]

    def pair_out(p, slot):
        return [pltpu.make_async_copy(d_qkv.at[slot], d_qkv_out.at[span(p), :], out_sem.at[0, slot]),
                pltpu.make_async_copy(d_emb.at[slot], d_emb_out.at[:, span(p)], out_sem.at[1, slot])]

    for copy in pair_in(0, 0):
        copy.start()
    sums[...] = jnp.zeros_like(sums)
    d_part[...] = jnp.zeros_like(d_part)
    place.meet()
    term = term_of(MLP_STREAMS, {FC: c_turned, PROJ: gelu_turned}, {FC: d_pre, PROJ: grad_rows})
    ring = RingSum(place, (FC, PROJ), MLP_STREAMS, accs, owns, gives, twins, sems, term)
    for load in loads:
        load.wait()

    def hook(half, step):
        p = lax.div(step, 2)
        slot = lax.rem(p, 2)

        @pl.when(lax.rem(step, 2) == 0)
        def _():
            if half == 0:
                @pl.when(p < n_pair - 1)
                def _():
                    for copy in pair_in(p + 1, 1 - slot):
                        copy.start()

                for copy in pair_in(p, slot):
                    copy.wait()

                @pl.when(p >= 2)
                def _():
                    for copy in pair_out(p - 2, slot):
                        copy.wait()

                d_ctx[...] = dot_nt(d_mid_b[slot], w_out[...]).astype(jnp.bfloat16)
            context_back(slot, half, qkv, d_ctx, d_qkv, d_part)

        @pl.when(lax.rem(step, 2) == 1)
        def _():
            if half == 0:
                d_a[...] = dot_nt(d_qkv[slot], w_qkv[...])
            else:
                d_emb[slot] = entry_back(x_zero[slot], d_mid[slot], d_a[...], vecs, sums).T
                for copy in pair_out(p, slot):
                    copy.start()

    ring.run((tuple(range(6)), tuple(range(6, len(MLP_STREAMS)))), hook)
    for p in (n_pair - 2, n_pair - 1):
        for copy in pair_out(p, p % 2):
            copy.wait()
    for s in range(3):
        add_row(sums, VEC_QKV + s, d_part[:, pl.ds(1024 * s, 1024)])
    ring.finish((fc_out, proj_out))


def mlp_sums(c_turned, d_pre, gelu_turned, grad_rows, w_qkv, w_out, vecs, x_zero, d_mid, d_mid_b, qkv):
    bf, f32, dma = jnp.bfloat16, jnp.float32, pltpu.SemaphoreType.DMA
    n_rows = x_zero.shape[0]
    assert n_rows // SEQ == N_CHIP
    out_shape = [jax.ShapeDtypeStruct(ARRAYS[FC], f32), jax.ShapeDtypeStruct(ARRAYS[PROJ], f32), jax.ShapeDtypeStruct((n_rows, 3072), bf),
                 jax.ShapeDtypeStruct((1024, n_rows), bf), jax.ShapeDtypeStruct((VEC_ROWS, 1024), f32)]
    anywhere, vmem = pl.BlockSpec(memory_space=pl.ANY), pl.BlockSpec(memory_space=pltpu.VMEM)
    scratch = [pltpu.VMEM(a.shape, bf) for a in (c_turned, d_pre, gelu_turned, grad_rows, w_qkv, w_out)]
    scratch += [pltpu.VMEM((2, PAIR, 1024), f32), pltpu.VMEM((2, PAIR, 1024), f32), pltpu.VMEM((2, PAIR, 1024), bf), pltpu.VMEM((2, PAIR, 3072), bf),
                pltpu.VMEM((2, PAIR, 3072), bf), pltpu.VMEM((2, 1024, PAIR), bf), pltpu.VMEM((8, 3072), f32),
                pltpu.VMEM((PAIR, 1024), bf), pltpu.VMEM((PAIR, 1024), f32), dma((6,)), dma((4, 2)), dma((2, 2))]
    return pl.pallas_call(
        mlp_sums_kernel, out_shape=out_shape, in_specs=[anywhere] * 6 + [vmem] + [anywhere] * 4, out_specs=[anywhere] * 4 + [vmem],
        scratch_shapes=scratch + ring_scratch((FC, PROJ), MLP_STREAMS),
        compiler_params=pltpu.CompilerParams(collective_id=1, has_side_effects=True, vmem_limit_bytes=62 * 1024 * 1024), name='mlp_sums',
    )(c_turned, d_pre, gelu_turned, grad_rows, w_qkv, w_out, vecs, x_zero, d_mid, d_mid_b, qkv)


def rest_sums_kernel(*refs):
    (a_hbm, dqkv_hbm, ctx_hbm, mid_hbm, emb_hbm, in_hbm, vec_hbm) = refs[:7]
    outs = refs[7:10]
    (a_turned, d_qkv, ctx_turned, d_mid_b, emb_turned, x_in, g_vec, load_sem) = refs[10:18]
    (accs, owns, gives, twins), sems = split_scratch(refs[18:], 3)
    place = Place()
    loads = [pltpu.make_async_copy(src, dst, load_sem.at[n]) for n, (src, dst) in enumerate(
        ((a_hbm, a_turned), (dqkv_hbm, d_qkv), (ctx_hbm, ctx_turned), (mid_hbm, d_mid_b), (emb_hbm, emb_turned), (in_hbm, x_in), (vec_hbm, g_vec)))]
    for load in loads:
        load.start()
    place.meet()
    product = term_of(REST_STREAMS, {QKV: a_turned, OUT: ctx_turned, MISC: emb_turned}, {QKV: d_qkv, OUT: d_mid_b, MISC: x_in})

    def term(i, chip, core):
        arr, row, rows, col, cols, _ = REST_STREAMS[i]
        block = product(i, chip, core)
        if arr == MISC and col >= 256:
            first = pl.multiple_of(2 * chip * ARRAYS[arr][0] + row, 16)
            block = block + jnp.where(core == 1, g_vec[pl.ds(first, rows), pl.ds(col - 256, cols)], 0.0)
        return block

    ring = RingSum(place, (QKV, OUT, MISC), REST_STREAMS, accs, owns, gives, twins, sems, term)
    for load in loads:
        load.wait()
    ring.run((tuple(range(6)), tuple(range(6, len(REST_STREAMS)))), lambda half, step: None)
    ring.finish(outs)


def rest_sums(a_turned, d_qkv, ctx_turned, d_mid_b, emb_turned, x_in, g_vec):
    arrays = (QKV, OUT, MISC)
    operands = (a_turned, d_qkv, ctx_turned, d_mid_b, emb_turned, x_in, g_vec)
    anywhere = pl.BlockSpec(memory_space=pl.ANY)
    return pl.pallas_call(
        rest_sums_kernel, out_shape=[jax.ShapeDtypeStruct(ARRAYS[arr], jnp.float32) for arr in arrays],
        in_specs=[anywhere] * 7, out_specs=[anywhere] * 3,
        scratch_shapes=[pltpu.VMEM(a.shape, a.dtype) for a in operands] + [pltpu.SemaphoreType.DMA((7,))] + ring_scratch(arrays, REST_STREAMS),
        compiler_params=pltpu.CompilerParams(collective_id=2, has_side_effects=True, vmem_limit_bytes=62 * 1024 * 1024), name='rest_sums',
    )(*operands)


def whole(shape):
    return pl.BlockSpec(shape, lambda i: (0, 0), pipeline_mode=pl.Buffered(1))


def rows_of(width):
    return pl.BlockSpec((ROWS, width), lambda i: (i, 0))


def stage_call(body, name, n_rows, ins, outs, scratch=()):
    in_specs = [rows_of(a.shape[1]) if a.shape[0] == n_rows and not held else whole(a.shape) for a, held in ins]
    out_specs, out_shape = [], []
    for width, dtype in outs:
        if dtype is None:
            out_specs.append(pl.BlockSpec((VEC_ROWS, 1024), lambda i: (0, 0)))
            out_shape.append(jax.ShapeDtypeStruct((VEC_ROWS, 1024), jnp.float32))
        elif width < 0:
            out_specs.append(pl.BlockSpec((-width, ROWS), lambda i: (0, i)))
            out_shape.append(jax.ShapeDtypeStruct((-width, n_rows), dtype))
        else:
            out_specs.append(rows_of(width))
            out_shape.append(jax.ShapeDtypeStruct((n_rows, width), dtype))
    return pl.pallas_call(body, grid=(n_rows // ROWS,), in_specs=in_specs, out_specs=out_specs, out_shape=out_shape, scratch_shapes=list(scratch),
                          compiler_params=pltpu.CompilerParams(vmem_limit_bytes=62 * 1024 * 1024, dimension_semantics=('arbitrary',)), name=name)(*[a for a, _ in ins])

N_PIXEL, N_POS = 768, 197
MISC_USED = N_PIXEL + N_POS + len(VEC_NAMES) + 3 + 4


def solution(mesh):
    n_dev = mesh.shape[MESH_AXIS]

    def spec_of(name):
        return P(None, MESH_AXIS) if name in LAST_SPLIT else P(MESH_AXIS)

    def pack_misc(part):
        lane = part['b_patch'].shape[0]
        rows = [part['w_patch'], part['pos_table']] + [part[name].reshape(1, lane) for name in VEC_NAMES]
        rows += [part['b_qkv'].reshape(3, lane), part['b_fc'].reshape(4, lane), jnp.zeros((1024 - MISC_USED, lane), jnp.float32)]
        return jnp.concatenate(rows, axis=0).astype(jnp.bfloat16).T

    def unpack_misc(misc):
        turned = misc.T
        part = {'w_patch': turned[:N_PIXEL], 'pos_table': turned[N_PIXEL:N_PIXEL + N_POS]}
        first = N_PIXEL + N_POS
        for place, name in enumerate(VEC_NAMES):
            part[name] = turned[first + place]
        first += len(VEC_NAMES)
        part['b_qkv'] = turned[first:first + 3].reshape(-1)
        part['b_fc'] = turned[first + 3:first + 7].reshape(-1)
        return part

    def flat_of(rows):
        return rows.reshape(rows.shape[0], n_dev, -1).transpose(1, 0, 2).reshape(rows.shape)

    def shards_of(rows):
        return rows.reshape(n_dev, rows.shape[0], -1).transpose(1, 0, 2).reshape(rows.shape)

    def local_step(patches, keep, *rest):
        shards = dict(zip(PARAM_NAMES, rest[:-1]))
        grad_h1 = rest[-1]
        n_img, n_patch, _ = patches.shape
        n_token, d_model = grad_h1.shape[1:]
        n_shard, _, n_heads, head_dim = shards['w_qkv'].shape
        n_rows = n_img * SEQ
        casts = {name: shards[name].astype(jnp.bfloat16) for name in ('w_fc', 'w_proj', 'w_qkv', 'w_out')}
        w_qkv, w_out, misc = gather_first((casts['w_qkv'].reshape(n_shard, -1), casts['w_out'], pack_misc(shards)))
        position = jnp.pad(keep + 1, ((0, 0), (1, 0)))
        position = jnp.pad(position, ((0, 0), (0, SEQ - n_token)), constant_values=-1)[:, :, None]
        onehot_patch = (position == 1 + lax.broadcasted_iota(jnp.int32, (1, 1, n_patch), 2)).astype(jnp.bfloat16)
        onehot_pos = (position == lax.broadcasted_iota(jnp.int32, (1, 1, 1024 - N_PIXEL), 2)).astype(jnp.bfloat16)
        kept_rows = jnp.einsum('bkp,bpq->bkq', onehot_patch, patches, preferred_element_type=jnp.float32).astype(jnp.bfloat16)
        x_in = jnp.concatenate([kept_rows, onehot_pos], axis=2).reshape(n_rows, 1024)
        grad_rows = jnp.pad(grad_h1, ((0, 0), (0, SEQ - n_token), (0, 0))).reshape(n_rows, d_model)

        n_vec = len(VEC_NAMES)
        packed = misc[:, 896:].T[N_PIXEL + N_POS - 896:MISC_USED - 896].astype(jnp.float32)
        vecs = jnp.concatenate([packed[:n_vec], flat_of(packed[n_vec:n_vec + 3]), flat_of(packed[n_vec + 3:]), jnp.zeros((VEC_ROWS - packed.shape[0], 1024), jnp.float32)], axis=0)

        bf, f32 = jnp.bfloat16, jnp.float32
        w_fc, w_proj, x_zero, a_turned, qkv, ctx_turned, h_mid, c_in, c_turned = gather_second(casts['w_fc'], casts['w_proj'], x_in, misc, w_qkv, w_out, vecs)
        gelu_turned, d_pre, h_one, d_mid, d_mid_b, sums_two = stage_call(
            stage_two, 'stage_two', n_rows, [(c_in, False), (h_mid, False), (grad_rows, False), (w_fc, True), (w_proj, True), (vecs, True)],
            [(-4096, bf), (4096, bf), (1024, bf), (1024, f32), (1024, bf), (0, None)],
            [pltpu.VMEM((ROWS, 1024), f32), pltpu.VMEM((ROWS, 1024), f32)])
        h_one = h_one.reshape(n_img, SEQ, d_model)[:, :n_token]
        fc_sum, proj_sum, d_qkv, emb_turned, sums_three = mlp_sums(c_turned, d_pre, gelu_turned, grad_rows, w_qkv, w_out, vecs, x_zero, d_mid, d_mid_b, qkv)
        sums = sums_two + sums_three
        vec_rows = jnp.concatenate([sums[:n_vec], shards_of(sums[VEC_QKV:VEC_QKV + 3]), shards_of(sums[VEC_FC:VEC_FC + 4])], axis=0)
        g_rows = jnp.concatenate([sums[VEC_AT['cls_tok']][None], jnp.zeros((N_POS - 1, 1024), f32), vec_rows], axis=0)
        g_vec = jnp.pad(g_rows, ((0, 1024 - N_PIXEL - g_rows.shape[0]), (0, 0))).T
        qkv_sum, out_sum, misc_sum = rest_sums(a_turned, d_qkv, ctx_turned, d_mid_b, emb_turned, x_in, g_vec)
        own = unpack_misc(misc_sum)
        own.update(w_fc=fc_sum, w_proj=proj_sum, w_qkv=qkv_sum.reshape(n_shard, 3, n_heads, head_dim), w_out=out_sum)
        return (h_one,) + tuple(own[name] for name in PARAM_NAMES)

    batch_spec = P(MESH_AXIS)
    param_specs = tuple(spec_of(name) for name in PARAM_NAMES)
    return jax.shard_map(local_step, mesh=mesh, in_specs=(batch_spec, batch_spec) + param_specs + (batch_spec,), out_specs=(batch_spec,) + param_specs, check_vma=False)
```

```python
import jax
import jax.numpy as jnp
from jax import lax
from jax.experimental import pallas as pl
from jax.experimental.pallas import tpu as pltpu
from jax.sharding import PartitionSpec as P

MESH_AXIS = 'fsdp'
LN_EPS = 1e-5
INV_SQRT2 = 0.7071067811865476
INV_SQRT_2PI = 0.3989422804014327
PARAM_NAMES = ('w_patch', 'b_patch', 'pos_table', 'cls_tok', 'lnp_g', 'lnp_b', 'ln1_g', 'ln1_b', 'w_qkv', 'b_qkv', 'w_out', 'b_out', 'ln2_g', 'ln2_b', 'w_fc', 'b_fc', 'w_proj', 'b_proj')
LAST_SPLIT = ('w_patch', 'pos_table')


RINGS = (
    (0, 4, 8, 10, 11, 15, 14, 12, 13, 9, 5, 7, 6, 2, 3, 1),
    (0, 2, 3, 7, 11, 9, 8, 12, 13, 15, 14, 10, 6, 4, 5, 1),
    (0, 1, 3, 7, 5, 4, 8, 9, 11, 15, 13, 12, 14, 10, 6, 2),
    (0, 1, 5, 7, 3, 2, 6, 10, 14, 15, 11, 9, 13, 12, 8, 4),
    (0, 4, 6, 7, 11, 10, 8, 12, 14, 15, 13, 9, 5, 1, 3, 2),
    (0, 2, 6, 7, 3, 1, 5, 9, 13, 15, 11, 10, 14, 12, 8, 4),
)
N_CHIP = 16
MESH_ID = pl.DeviceIdType.MESH
ARRAYS = ((32, 4096), (128, 1024), (32, 3072), (32, 1024), (32, 1024))
FC, PROJ, QKV, OUT, MISC = range(5)
FIRST_STREAMS = tuple((QKV, 0, 32, 512 * k, 512, k) for k in range(6)) + (
    (OUT, 0, 32, 0, 384, 0), (OUT, 0, 32, 384, 384, 1), (OUT, 0, 32, 768, 256, 4),
    (MISC, 0, 32, 0, 384, 2), (MISC, 0, 32, 384, 384, 3), (MISC, 0, 32, 768, 256, 5))
SECOND_STREAMS = (
    (FC, 0, 32, 0, 896, 0), (FC, 0, 32, 896, 896, 1), (FC, 0, 32, 1792, 384, 2), (FC, 0, 32, 2176, 384, 3),
    (FC, 0, 32, 2560, 768, 4), (FC, 0, 32, 3328, 768, 5), (PROJ, 0, 128, 0, 128, 0), (PROJ, 0, 128, 128, 128, 1),
    (PROJ, 0, 128, 256, 256, 2), (PROJ, 0, 128, 512, 256, 3), (PROJ, 0, 128, 768, 128, 4), (PROJ, 0, 128, 896, 128, 5))
MLP_STREAMS = tuple((FC, 0, 64, 384 * k, 384, k) for k in range(4)) + ((FC, 0, 64, 1536, 256, 4), (FC, 0, 64, 1792, 256, 5)) + tuple(
    (PROJ, 128 * (place % 2), 128, 128 * (place // 2), 128, ring) for place, ring in enumerate((0, 1, 2, 3, 4, 5, 4, 5)))
REST_STREAMS = tuple((QKV, 0, 64, 256 * k, 256, k) for k in range(6)) + tuple((OUT, 0, 64, 128 * k, 128, k) for k in range(4)) + (
    (MISC, 0, 64, 0, 128, 4), (MISC, 0, 64, 128, 128, 5), (MISC, 0, 32, 256, 128, 0), (MISC, 32, 32, 256, 128, 1),
    (MISC, 0, 32, 384, 128, 2), (MISC, 32, 32, 384, 128, 3))


def pick(table, index):
    value = jnp.int32(table[0])
    for place in range(1, len(table)):
        value = jnp.where(index == place, jnp.int32(table[place]), value)
    return value


class Place:
    def __init__(self):
        me = lax.axis_index(MESH_AXIS)
        self.core = lax.rem(me, 2)
        self.chip = lax.div(me, 2)
        self.sibling = me + 1 - 2 * self.core
        where_in = [[ring.index(chip) for chip in range(N_CHIP)] for ring in RINGS]
        self.spot = [pick(table, self.chip) for table in where_in]
        self.after = [2 * pick([ring[(table[chip] + 1) % N_CHIP] for chip in range(N_CHIP)], self.chip) + self.core
                      for ring, table in zip(RINGS, where_in)]
        self.before = [2 * pick([ring[(table[chip] - 1) % N_CHIP] for chip in range(N_CHIP)], self.chip) + self.core
                       for ring, table in zip(RINGS, where_in)]

    def chips_back(self, steps):
        return [pick(ring, lax.rem(self.spot[k] + 2 * N_CHIP - steps, N_CHIP)) for k, ring in enumerate(RINGS)]

    def meet(self):
        barrier = pltpu.get_barrier_semaphore()
        for other in self.after + self.before + [self.sibling]:
            pl.semaphore_signal(barrier, inc=1, device_id=(other,), device_id_type=MESH_ID)
        pl.semaphore_wait(barrier, 2 * len(RINGS) + 1)


class RingGather:
    def __init__(self, place, arrays, streams, shards, wholes, sems):
        self.place, self.arrays, self.streams = place, arrays, streams
        self.shards, self.wholes = dict(zip(arrays, shards)), dict(zip(arrays, wholes))
        self.own_sem, self.send_sem, self.recv_sem, self.twin_send, self.twin_recv = sems

    def block(self, i, chip, core):
        arr, row, rows, col, cols, _ = self.streams[i]
        first = (2 * chip + core) * ARRAYS[arr][0] + row
        return self.wholes[arr].at[pl.ds(pl.multiple_of(first, 32), rows), pl.ds(col, cols)]

    def ring_copy(self, i, src, dst, step, back):
        towards, place = (self.place.before, step + N_CHIP // 2) if back else (self.place.after, step)
        return pltpu.make_async_remote_copy(src_ref=src, dst_ref=dst, send_sem=self.send_sem.at[i, place], recv_sem=self.recv_sem.at[i, place],
                                            device_id=(towards[self.streams[i][5]],), device_id_type=MESH_ID)

    def twin_copy(self, i, src, dst, step):
        return pltpu.make_async_remote_copy(src_ref=src, dst_ref=dst, send_sem=self.twin_send.at[i, step], recv_sem=self.twin_recv.at[i, step],
                                            device_id=(self.place.sibling,), device_id_type=MESH_ID)

    def own_copies(self):
        for place, arr in enumerate(self.arrays):
            rows = ARRAYS[arr][0]
            first = pl.multiple_of((2 * self.place.chip + self.place.core) * rows, 32)
            yield pltpu.make_async_copy(self.shards[arr], self.wholes[arr].at[pl.ds(first, rows), :], self.own_sem.at[place])

    def pass_along(self, step, back):
        place, far = self.place, N_CHIP // 2 - (1 if back else 0)
        chips = place.chips_back(-step if back else step)
        for i in range(len(self.streams)):
            here = self.block(i, chips[self.streams[i][5]], place.core)
            self.ring_copy(i, here, here, step - 1, back).wait_recv()

            @pl.when(step < far)
            def _():
                self.ring_copy(i, here, here, step, back).start()

            self.twin_copy(i, here, here, step + (N_CHIP // 2 if back else 0)).start()

    def run(self, hook):
        place, half = self.place, N_CHIP // 2
        for i in range(len(self.streams)):
            arr, row, rows, col, cols, _ = self.streams[i]
            mine = self.shards[arr].at[pl.ds(row, rows), pl.ds(col, cols)]
            here = self.block(i, place.chip, place.core)
            self.ring_copy(i, mine, here, 0, False).start()
            self.ring_copy(i, mine, here, 0, True).start()
            self.twin_copy(i, mine, here, 0).start()
        for copy in self.own_copies():
            copy.start()
        hook(jnp.int32(0))

        def ring_step(step, carry):
            self.pass_along(step, False)
            hook(2 * step - 1)

            @pl.when(step < half)
            def _():
                self.pass_along(step, True)
                hook(2 * step)
            return carry

        lax.fori_loop(1, half + 1, ring_step, 0)

        def drain(step, carry):
            chips = [place.chips_back(step), place.chips_back(-step)]
            for i in range(len(self.streams)):
                k = self.streams[i][5]
                for back in (False, True):
                    here, there = self.block(i, chips[back][k], place.core), self.block(i, chips[back][k], 1 - place.core)
                    far = half - 1 if back else half

                    @pl.when(step < far)
                    def _():
                        self.ring_copy(i, here, here, step, back).wait_send()

                    at = step + (half if back else 0)

                    @pl.when(jnp.logical_and(step >= 1, step < half) if back else step >= 0)
                    def _():
                        self.twin_copy(i, here, here, at).wait_send()
                        self.twin_copy(i, there, there, at).wait_recv()
            return carry

        lax.fori_loop(0, half + 1, drain, 0)
        for copy in self.own_copies():
            copy.wait()


def gather_sems(arrays, streams):
    ring, twin = pltpu.SemaphoreType.DMA((len(streams), N_CHIP - 1)), pltpu.SemaphoreType.DMA((len(streams), N_CHIP))
    return [pltpu.SemaphoreType.DMA((len(arrays),)), ring, ring, twin, twin]


def gathered_shapes(arrays):
    return [jax.ShapeDtypeStruct((2 * N_CHIP * ARRAYS[arr][0], ARRAYS[arr][1]), jnp.bfloat16) for arr in arrays]


FIRST_ARRAYS, SECOND_ARRAYS = (QKV, OUT, MISC), (FC, PROJ)


def gather_first_kernel(*refs):
    place = Place()
    place.meet()
    RingGather(place, FIRST_ARRAYS, FIRST_STREAMS, refs[:3], refs[3:6], refs[6:]).run(lambda step: None)


def gather_first(shards):
    return pl.pallas_call(
        gather_first_kernel, out_shape=gathered_shapes(FIRST_ARRAYS),
        in_specs=[pl.BlockSpec(memory_space=pltpu.VMEM)] * 3, out_specs=[pl.BlockSpec(memory_space=pl.ANY)] * 3,
        scratch_shapes=gather_sems(FIRST_ARRAYS, FIRST_STREAMS),
        compiler_params=pltpu.CompilerParams(collective_id=0, has_side_effects=True), name='gather_first',
    )(*shards)


class RingSum:
    def __init__(self, place, arrays, streams, accs, owns, gives, twins, sems, term):
        self.place, self.streams, self.term, self.arrays = place, streams, term, arrays
        self.accs, self.owns, self.gives, self.twins = [dict(zip(arrays, refs)) for refs in (accs, owns, gives, twins)]
        (self.twin_send, self.twin_recv, self.send_sem, self.recv_sem, self.ring_free, self.twin_free,
         self.end_own, self.end_send, self.end_recv) = sems

    def part(self, i, ref, *slot):
        _, row, rows, col, cols, _ = self.streams[i]
        return ref.at[(*slot, pl.ds(row, rows), pl.ds(col, cols))]

    def push(self, i, slot):
        arr = self.streams[i][0]
        return pltpu.make_async_remote_copy(src_ref=self.part(i, self.gives[arr], slot), dst_ref=self.part(i, self.twins[arr], slot),
                                            send_sem=self.twin_send.at[i, slot], recv_sem=self.twin_recv.at[i, slot],
                                            device_id=(self.place.sibling,), device_id_type=MESH_ID)

    def pass_on(self, i, slot, slot_next):
        arr, k = self.streams[i][0], self.streams[i][5]
        return pltpu.make_async_remote_copy(src_ref=self.part(i, self.accs[arr], slot), dst_ref=self.part(i, self.accs[arr], slot_next),
                                            send_sem=self.send_sem.at[i, slot], recv_sem=self.recv_sem.at[i, slot_next],
                                            device_id=(self.place.after[k],), device_id_type=MESH_ID)

    def make(self, group, step):
        chips, slot = self.place.chips_back(step + 1), lax.rem(jnp.int32(step), 2)
        for i in group:
            arr, cols, k = self.streams[i][0], self.streams[i][4], self.streams[i][5]
            block = self.term(i, chips[k])
            self.part(i, self.owns[arr], slot)[...] = block[:, :cols]
            self.part(i, self.gives[arr], slot)[...] = block[:, cols:]

    def push_next(self, group, step):
        slot, slot_next = lax.rem(step, 2), lax.rem(step + 1, 2)
        for i in group:
            self.push(i, slot).wait_send()

            @pl.when(step >= 1)
            def _():
                pl.semaphore_wait(self.twin_free.at[i], 1)
            self.push(i, slot_next).start()

    def advance(self, group, step):
        slot, slot_next, slot_last, pair = lax.rem(step, 3), lax.rem(step + 1, 3), lax.rem(step + 2, 3), lax.rem(step, 2)
        for i in group:
            arr, row, rows, col, cols, k = self.streams[i]
            acc, own, twin = self.part(i, self.accs[arr], slot), self.part(i, self.owns[arr], pair), self.part(i, self.twins[arr], pair)
            self.push(i, pair).wait_recv()

            @pl.when(step == 0)
            def _():
                acc[...] = own[...] + twin[...]

            @pl.when(step > 0)
            def _():
                self.pass_on(i, slot, slot).wait_recv()
                acc[...] = acc[...] + (own[...] + twin[...])

            @pl.when(jnp.logical_and(step >= 2, step < N_CHIP - 1))
            def _():
                pl.semaphore_wait(self.ring_free.at[i], 1)

            @pl.when(step < N_CHIP - 1)
            def _():
                self.pass_on(i, slot, slot_next).start()

            @pl.when(step < N_CHIP - 2)
            def _():
                pl.semaphore_signal(self.twin_free.at[i], inc=1, device_id=(self.place.sibling,), device_id_type=MESH_ID)

        for i in group:
            k = self.streams[i][5]

            @pl.when(step >= 1)
            def _():
                self.pass_on(i, slot_last, slot).wait_send()

            @pl.when(jnp.logical_and(step >= 1, step < N_CHIP - 2))
            def _():
                pl.semaphore_signal(self.ring_free.at[i], inc=1, device_id=(self.place.before[k],), device_id_type=MESH_ID)

    def run(self, groups, hook, ready):
        for place, group in enumerate(groups):
            ready(place)
            self.make(group, 0)
            for i in group:
                self.push(i, 0).start()

        def ring_step(step, carry):
            for place, group in enumerate(groups):
                self.advance(group, step)

                @pl.when(step == 0)
                def _():
                    self.make(group, 1)

                @pl.when(step < N_CHIP - 1)
                def _():
                    self.push_next(group, step)

                @pl.when(step < N_CHIP - 2)
                def _():
                    self.make(group, step + 2)

                hook(place, step)
            return carry

        lax.fori_loop(0, N_CHIP, ring_step, 0)

    def finish(self, outs):
        for i in range(len(self.streams)):
            self.push(i, (N_CHIP - 1) % 2).wait_send()
        last = (N_CHIP - 1) % 3
        ends = []
        for place, arr in enumerate(self.arrays):
            rows, half, core = ARRAYS[arr][0], ARRAYS[arr][1] // 2, self.place.core
            target = outs[place].at[:, pl.ds(pl.multiple_of(core * half, 128), half)]
            keep_rows = self.accs[arr].at[last, pl.ds(pl.multiple_of(core * rows, 32), rows), :]
            give_rows = self.accs[arr].at[last, pl.ds(pl.multiple_of((1 - core) * rows, 32), rows), :]
            ends.append(pltpu.make_async_copy(keep_rows, target, self.end_own.at[place]))
            ends.append(pltpu.make_async_remote_copy(src_ref=give_rows, dst_ref=target, send_sem=self.end_send.at[place], recv_sem=self.end_recv.at[place],
                                                     device_id=(self.place.sibling,), device_id_type=MESH_ID))
        for end in ends:
            end.start()
        for end in ends:
            end.wait()


def ring_scratch(arrays, streams):
    shapes = [(2 * ARRAYS[arr][0], ARRAYS[arr][1] // 2) for arr in arrays]
    buffers = [pltpu.VMEM((*lead, *shape), jnp.float32) for lead in ((3,), (2,), (2,), (2,)) for shape in shapes]
    dma, regular, n = pltpu.SemaphoreType.DMA, pltpu.SemaphoreType.REGULAR, len(streams)
    return buffers + [dma((n, 2)), dma((n, 2)), dma((n, 3)), dma((n, 3)), regular((n,)), regular((n,))] + [dma((len(arrays),))] * 3


def split_scratch(refs, n_arrays):
    buffers, sems = refs[:4 * n_arrays], refs[4 * n_arrays:4 * n_arrays + 9]
    return [buffers[n_arrays * b:n_arrays * (b + 1)] for b in range(4)], sems


def term_of(streams, lefts, rights, core):
    def term(i, chip):
        arr, row, rows, col, cols, _ = streams[i]
        half = ARRAYS[arr][1] // 2
        first = pl.multiple_of(2 * chip * ARRAYS[arr][0] + row, 16)
        right = jnp.concatenate([rights[arr][:, pl.ds(pl.multiple_of(side * half + col, 128), cols)] for side in (core, 1 - core)], axis=1)
        return dot_nn(lefts[arr][pl.ds(first, rows), :], right)
    return term


HEAD_GROUP, HEAD_DIM, SEQ, N_TOKEN = 256, 64, 64, 50
ROWS = 256
LOGIT_SCALE = HEAD_DIM ** -0.5
VEC_NAMES = ('b_patch', 'cls_tok', 'lnp_g', 'lnp_b', 'ln1_g', 'ln1_b', 'b_out', 'ln2_g', 'ln2_b', 'b_proj')
VEC_AT = {name: place for place, name in enumerate(VEC_NAMES)}
VEC_QKV, VEC_FC, VEC_ROWS = 10, 13, 24


def dot_nn(left, right):
    return lax.dot_general(left, right, (((1,), (0,)), ((), ())), preferred_element_type=jnp.float32)


def dot_nt(left, right):
    return lax.dot_general(left, right, (((1,), (1,)), ((), ())), preferred_element_type=jnp.float32)


def dot_tn(left, right):
    return lax.dot_general(left, right, (((0,), (0,)), ((), ())), preferred_element_type=jnp.float32)


def normalize(x_in):
    centered = x_in - jnp.mean(x_in, axis=-1, keepdims=True)
    inv_std = lax.rsqrt(jnp.mean(centered * centered, axis=-1, keepdims=True) + LN_EPS)
    return centered * inv_std, inv_std


def normalize_back(d_norm, x_hat, inv_std, gain):
    d_hat = d_norm * gain
    return inv_std * (d_hat - jnp.mean(d_hat, axis=-1, keepdims=True) - x_hat * jnp.mean(d_hat * x_hat, axis=-1, keepdims=True))


def lane_ids(shape):
    return lax.broadcasted_iota(jnp.int32, shape, 1)


def stack_heads(block):
    head = lane_ids((1, HEAD_GROUP)) // HEAD_DIM
    return jnp.concatenate([block * (head == h).astype(jnp.bfloat16) for h in range(4)], axis=0)


def unstack_heads(stacked):
    head = lane_ids((1, HEAD_GROUP)) // HEAD_DIM
    total = jnp.where(head == 0, stacked[:SEQ], 0.0)
    for h in range(1, 4):
        total = jnp.where(head == h, stacked[h * SEQ:(h + 1) * SEQ], total)
    return total


def per_head(block, reducer, neutral):
    halves = []
    for j in range(2):
        half = block[:, 128 * j:128 * (j + 1)]
        low = lane_ids(half.shape) < HEAD_DIM
        first = reducer(jnp.where(low, half, neutral), axis=1, keepdims=True)
        second = reducer(jnp.where(low, neutral, half), axis=1, keepdims=True)
        halves.append(jnp.where(low, first, second))
    return jnp.concatenate(halves, axis=1)


def probabilities(q_block, k_stack):
    logits = dot_nt(q_block, k_stack) * LOGIT_SCALE
    logits = jnp.where(lane_ids(logits.shape) % HEAD_DIM < N_TOKEN, logits, -jnp.inf)
    powers = jnp.exp(logits - per_head(logits, jnp.max, -jnp.inf))
    return powers / per_head(powers, jnp.sum, 0.0)


def row_of(vecs, name):
    place = VEC_AT[name]
    return vecs[place:place + 1, :]


def is_cls(rows):
    return lax.broadcasted_iota(jnp.int32, (rows, 1), 0) % SEQ == 0


PAIR = 2 * SEQ


def gather_second_kernel(*refs):
    fc_shard, proj_shard, in_hbm, misc_hbm, qkv_w_hbm, out_w_hbm, vecs = refs[:7]
    fc_whole, proj_whole = refs[7:9]
    results = refs[9:16]
    x_in, misc, w_qkv, w_out, h_zero, ctx = refs[16:22]
    buffers = refs[22:29]
    x_zero, a_turned, qkv, ctx_turned, h_mid, c_out, c_turned = buffers
    load_sem, out_sem = refs[29:31]
    place = Place()
    loads = [pltpu.make_async_copy(src, dst, load_sem.at[n]) for n, (src, dst) in enumerate(
        ((in_hbm, x_in), (misc_hbm, misc), (qkv_w_hbm, w_qkv), (out_w_hbm, w_out)))]
    for load in loads:
        load.start()
    place.meet()

    def pair_out(p, slot):
        span = pl.ds(pl.multiple_of(p * PAIR, PAIR), PAIR)
        for n, (src, dst) in enumerate(zip(buffers, results)):
            target = dst.at[:, span] if n in (1, 3, 6) else dst.at[span, :]
            yield pltpu.make_async_copy(src.at[slot], target, out_sem.at[n, slot])

    def enter(p, slot):
        rows = pl.ds(pl.multiple_of(p * PAIR, PAIR), PAIR)
        start = jnp.where(is_cls(PAIR), row_of(vecs, 'cls_tok'), row_of(vecs, 'b_patch'))
        x_sum = dot_nt(x_in[rows, :], misc[...]) + start
        x_zero[slot] = x_sum
        h_sum = normalize(x_sum)[0] * row_of(vecs, 'lnp_g') + row_of(vecs, 'lnp_b')
        h_zero[...] = h_sum
        a_in = (normalize(h_sum)[0] * row_of(vecs, 'ln1_g') + row_of(vecs, 'ln1_b')).astype(jnp.bfloat16)
        a_turned[slot] = a_in.T
        for s in range(3):
            cols = pl.ds(1024 * s, 1024)
            qkv[slot, :, cols] = (dot_nn(a_in, w_qkv[:, cols]) + vecs[VEC_QKV + s:VEC_QKV + s + 1, :]).astype(jnp.bfloat16)

    def attend(slot):
        for b in range(2):
            rows = pl.ds(b * SEQ, SEQ)
            for g in range(4):
                q_block, k_block, v_block = [qkv[slot, rows, pl.ds(1024 * s + HEAD_GROUP * g, HEAD_GROUP)] for s in range(3)]
                prob = probabilities(q_block, stack_heads(k_block)).astype(jnp.bfloat16)
                ctx[rows, pl.ds(HEAD_GROUP * g, HEAD_GROUP)] = dot_nn(prob, stack_heads(v_block)).astype(jnp.bfloat16)
        context = ctx[...]
        ctx_turned[slot] = context.T
        mid = h_zero[...] + dot_nn(context, w_out[...]) + row_of(vecs, 'b_out')
        h_mid[slot] = mid
        c_in = (normalize(mid)[0] * row_of(vecs, 'ln2_g') + row_of(vecs, 'ln2_b')).astype(jnp.bfloat16)
        c_out[slot] = c_in
        c_turned[slot] = c_in.T

    def hook(step):
        p = lax.div(step, 2)
        slot = lax.rem(p, 2)

        @pl.when(step == 0)
        def _():
            for load in loads:
                load.wait()

        @pl.when(lax.rem(step, 2) == 0)
        def _():
            @pl.when(p >= 2)
            def _():
                for copy in pair_out(p - 2, slot):
                    copy.wait()
            enter(p, slot)

        @pl.when(lax.rem(step, 2) == 1)
        def _():
            attend(slot)
            for copy in pair_out(p, slot):
                copy.start()

    RingGather(place, SECOND_ARRAYS, SECOND_STREAMS, (fc_shard, proj_shard), (fc_whole, proj_whole), refs[31:]).run(hook)
    for p in (N_CHIP // 2 - 2, N_CHIP // 2 - 1):
        for copy in pair_out(p, p % 2):
            copy.wait()


def gather_second(fc_shard, proj_shard, x_in, misc, w_qkv, w_out, vecs):
    bf, f32, dma = jnp.bfloat16, jnp.float32, pltpu.SemaphoreType.DMA
    n_rows = x_in.shape[0]
    assert n_rows // SEQ == N_CHIP
    anywhere, vmem = pl.BlockSpec(memory_space=pl.ANY), pl.BlockSpec(memory_space=pltpu.VMEM)
    kinds = ((1024, f32), (-1024, bf), (3072, bf), (-1024, bf), (1024, f32), (1024, bf), (-1024, bf))
    out_shape = gathered_shapes(SECOND_ARRAYS) + [jax.ShapeDtypeStruct((n_rows, width) if width > 0 else (-width, n_rows), dtype) for width, dtype in kinds]
    scratch = [pltpu.VMEM(a.shape, bf) for a in (x_in, misc, w_qkv, w_out)] + [pltpu.VMEM((PAIR, 1024), f32), pltpu.VMEM((PAIR, 1024), bf)]
    scratch += [pltpu.VMEM((2, PAIR, width) if width > 0 else (2, -width, PAIR), dtype) for width, dtype in kinds]
    scratch += [dma((4,)), dma((7, 2))]
    return pl.pallas_call(
        gather_second_kernel, out_shape=out_shape, in_specs=[vmem, vmem] + [anywhere] * 4 + [vmem], out_specs=[anywhere] * len(out_shape),
        scratch_shapes=scratch + gather_sems(SECOND_ARRAYS, SECOND_STREAMS),
        compiler_params=pltpu.CompilerParams(collective_id=3, has_side_effects=True, vmem_limit_bytes=62 * 1024 * 1024), name='gather_second',
    )(fc_shard, proj_shard, x_in, misc, w_qkv, w_out, vecs)


def add_row(sums, place, value):
    sums[place:place + 1, :] += jnp.sum(value, axis=0, keepdims=True)


def clear_first(sums):
    @pl.when(pl.program_id(0) == 0)
    def _():
        sums[...] = jnp.zeros_like(sums)


def stage_two(c_in, h_mid, grad_h1, w_fc, w_proj, vecs, gelu_turned, d_pre_out, h_one, d_mid, d_mid_b, sums, h_acc, d_c_acc):
    clear_first(sums)
    c_block, g_block = c_in[...], grad_h1[...]
    tile = 1024
    for f in range(4096 // tile):
        cols = pl.ds(tile * f, tile)
        pre_act = dot_nn(c_block, w_fc[:, cols]) + vecs[VEC_FC + f:VEC_FC + f + 1, :]
        normal_cdf = 0.5 * (1.0 + lax.erf(pre_act * INV_SQRT2))
        gelu = (pre_act * normal_cdf).astype(jnp.bfloat16)
        gelu_turned[cols, :] = gelu.T
        slope = normal_cdf + pre_act * jnp.exp(-0.5 * pre_act * pre_act) * INV_SQRT_2PI
        d_pre = dot_nt(g_block, w_proj[cols, :]) * slope
        add_row(sums, VEC_FC + f, d_pre)
        d_pre_b = d_pre.astype(jnp.bfloat16)
        d_pre_out[:, cols] = d_pre_b
        h_part = dot_nn(gelu, w_proj[cols, :])
        d_part = dot_nt(d_pre_b, w_fc[:, cols])
        if f == 0:
            h_acc[...] = h_part
            d_c_acc[...] = d_part
        else:
            h_acc[...] += h_part
            d_c_acc[...] += d_part
    mid = h_mid[...]
    h_one[...] = (mid + h_acc[...] + row_of(vecs, 'b_proj')).astype(jnp.bfloat16)
    d_c = d_c_acc[...]
    x_hat, inv_std = normalize(mid)
    d_h = g_block.astype(jnp.float32)
    d_sum = normalize_back(d_c, x_hat, inv_std, row_of(vecs, 'ln2_g')) + d_h
    d_mid[...] = d_sum
    d_mid_b[...] = d_sum.astype(jnp.bfloat16)
    add_row(sums, VEC_AT['ln2_g'], d_c * x_hat)
    add_row(sums, VEC_AT['ln2_b'], d_c)
    add_row(sums, VEC_AT['b_proj'], d_h)
    add_row(sums, VEC_AT['b_out'], d_sum)


def context_back(slot, b, qkv, d_ctx, d_qkv, d_part):
    rows = pl.ds(b * SEQ, SEQ)
    for g in range(4):
        places = [pl.ds(1024 * s + HEAD_GROUP * g, HEAD_GROUP) for s in range(3)]
        q_block, k_block, v_block = [qkv[slot, rows, place] for place in places]
        d_block = d_ctx[rows, pl.ds(HEAD_GROUP * g, HEAD_GROUP)]
        k_stack = stack_heads(k_block)
        prob = probabilities(q_block, k_stack)
        d_prob = dot_nt(d_block, stack_heads(v_block))
        d_logit = (prob * (d_prob - per_head(prob * d_prob, jnp.sum, 0.0)) * LOGIT_SCALE).astype(jnp.bfloat16)
        g_q = dot_nn(d_logit, k_stack)
        g_k = unstack_heads(dot_tn(d_logit, q_block))
        g_v = unstack_heads(dot_tn(prob.astype(jnp.bfloat16), d_block))
        for place, grad in zip(places, (g_q, g_k, g_v)):
            d_qkv[slot, rows, place] = grad.astype(jnp.bfloat16)
            d_part[:, place] += jnp.sum(grad.reshape(SEQ // 8, 8, HEAD_GROUP), axis=0)


def entry_back(x_sum, d_mid, d_a, vecs, sums):
    hat_p, inv_p = normalize(x_sum)
    h_zero = hat_p * row_of(vecs, 'lnp_g') + row_of(vecs, 'lnp_b')
    hat_1, inv_1 = normalize(h_zero)
    add_row(sums, VEC_AT['ln1_g'], d_a * hat_1)
    add_row(sums, VEC_AT['ln1_b'], d_a)
    d_zero = normalize_back(d_a, hat_1, inv_1, row_of(vecs, 'ln1_g')) + d_mid
    add_row(sums, VEC_AT['lnp_g'], d_zero * hat_p)
    add_row(sums, VEC_AT['lnp_b'], d_zero)
    d_x = normalize_back(d_zero, hat_p, inv_p, row_of(vecs, 'lnp_g'))
    cls = is_cls(PAIR)
    d_emb = jnp.where(cls, 0.0, d_x)
    add_row(sums, VEC_AT['cls_tok'], jnp.where(cls, d_x, 0.0))
    add_row(sums, VEC_AT['b_patch'], d_emb)
    return d_emb.astype(jnp.bfloat16)


def mlp_sums_kernel(*refs):
    (c_hbm, pre_hbm, gelu_hbm, rows_hbm, qkv_w_hbm, out_w_hbm, vecs, x_hbm, mid_hbm, mid_b_hbm, qkv_hbm) = refs[:11]
    fc_out, proj_out, d_qkv_out, d_emb_out, sums = refs[11:16]
    (c_turned, d_pre, gelu_turned, grad_rows, w_qkv, w_out, x_zero, d_mid, d_mid_b, qkv, d_qkv, d_emb, d_part,
     d_ctx, d_a, load_sem, in_sem, out_sem) = refs[16:34]
    (accs, owns, gives, twins), sems = split_scratch(refs[34:], 2)
    place = Place()
    loads = [pltpu.make_async_copy(src, dst, load_sem.at[n]) for n, (src, dst) in enumerate(
        ((c_hbm, c_turned), (pre_hbm, d_pre), (gelu_hbm, gelu_turned), (rows_hbm, grad_rows), (qkv_w_hbm, w_qkv), (out_w_hbm, w_out)))]
    for load in loads[:2]:
        load.start()
    n_pair = x_hbm.shape[0] // PAIR

    def span(p):
        return pl.ds(pl.multiple_of(p * PAIR, PAIR), PAIR)

    def pair_in(p, slot):
        return [pltpu.make_async_copy(src.at[span(p), :], dst.at[slot], in_sem.at[n, slot]) for n, (src, dst) in enumerate(
            ((x_hbm, x_zero), (mid_hbm, d_mid), (mid_b_hbm, d_mid_b), (qkv_hbm, qkv)))]

    def pair_out(p, slot):
        return [pltpu.make_async_copy(d_qkv.at[slot], d_qkv_out.at[span(p), :], out_sem.at[0, slot]),
                pltpu.make_async_copy(d_emb.at[slot], d_emb_out.at[:, span(p)], out_sem.at[1, slot])]

    for copy in pair_in(0, 0):
        copy.start()
    sums[...] = jnp.zeros_like(sums)
    d_part[...] = jnp.zeros_like(d_part)
    place.meet()
    term = term_of(MLP_STREAMS, {FC: c_turned, PROJ: gelu_turned}, {FC: d_pre, PROJ: grad_rows}, place.core)
    ring = RingSum(place, (FC, PROJ), MLP_STREAMS, accs, owns, gives, twins, sems, term)

    def ready(group):
        for load in loads[2 * group:2 * group + 2]:
            load.wait()
        for load in loads[2 * group + 2:2 * group + 4]:
            load.start()

    def hook(half, step):
        p = lax.div(step, 2)
        slot = lax.rem(p, 2)

        @pl.when(lax.rem(step, 2) == 0)
        def _():
            if half == 0:
                @pl.when(step == 0)
                def _():
                    for load in loads[4:]:
                        load.wait()

                @pl.when(p < n_pair - 1)
                def _():
                    for copy in pair_in(p + 1, 1 - slot):
                        copy.start()

                for copy in pair_in(p, slot):
                    copy.wait()

                @pl.when(p >= 2)
                def _():
                    for copy in pair_out(p - 2, slot):
                        copy.wait()

                d_ctx[...] = dot_nt(d_mid_b[slot], w_out[...]).astype(jnp.bfloat16)
            context_back(slot, half, qkv, d_ctx, d_qkv, d_part)

        @pl.when(lax.rem(step, 2) == 1)
        def _():
            if half == 0:
                d_a[...] = dot_nt(d_qkv[slot], w_qkv[...])
            else:
                d_emb[slot] = entry_back(x_zero[slot], d_mid[slot], d_a[...], vecs, sums).T
                for copy in pair_out(p, slot):
                    copy.start()

    ring.run((tuple(range(6)), tuple(range(6, len(MLP_STREAMS)))), hook, ready)
    for p in (n_pair - 2, n_pair - 1):
        for copy in pair_out(p, p % 2):
            copy.wait()
    for s in range(3):
        add_row(sums, VEC_QKV + s, d_part[:, pl.ds(1024 * s, 1024)])
    ring.finish((fc_out, proj_out))


def mlp_sums(c_turned, d_pre, gelu_turned, grad_rows, w_qkv, w_out, vecs, x_zero, d_mid, d_mid_b, qkv):
    bf, f32, dma = jnp.bfloat16, jnp.float32, pltpu.SemaphoreType.DMA
    n_rows = x_zero.shape[0]
    assert n_rows // SEQ == N_CHIP
    out_shape = [jax.ShapeDtypeStruct(ARRAYS[FC], f32), jax.ShapeDtypeStruct(ARRAYS[PROJ], f32), jax.ShapeDtypeStruct((n_rows, 3072), bf),
                 jax.ShapeDtypeStruct((1024, n_rows), bf), jax.ShapeDtypeStruct((VEC_ROWS, 1024), f32)]
    anywhere, vmem = pl.BlockSpec(memory_space=pl.ANY), pl.BlockSpec(memory_space=pltpu.VMEM)
    scratch = [pltpu.VMEM(a.shape, bf) for a in (c_turned, d_pre, gelu_turned, grad_rows, w_qkv, w_out)]
    scratch += [pltpu.VMEM((2, PAIR, 1024), f32), pltpu.VMEM((2, PAIR, 1024), f32), pltpu.VMEM((2, PAIR, 1024), bf), pltpu.VMEM((2, PAIR, 3072), bf),
                pltpu.VMEM((2, PAIR, 3072), bf), pltpu.VMEM((2, 1024, PAIR), bf), pltpu.VMEM((8, 3072), f32),
                pltpu.VMEM((PAIR, 1024), bf), pltpu.VMEM((PAIR, 1024), f32), dma((6,)), dma((4, 2)), dma((2, 2))]
    return pl.pallas_call(
        mlp_sums_kernel, out_shape=out_shape, in_specs=[anywhere] * 6 + [vmem] + [anywhere] * 4, out_specs=[anywhere] * 4 + [vmem],
        scratch_shapes=scratch + ring_scratch((FC, PROJ), MLP_STREAMS),
        compiler_params=pltpu.CompilerParams(collective_id=1, has_side_effects=True, vmem_limit_bytes=62 * 1024 * 1024), name='mlp_sums',
    )(c_turned, d_pre, gelu_turned, grad_rows, w_qkv, w_out, vecs, x_zero, d_mid, d_mid_b, qkv)


def rest_sums_kernel(*refs):
    (a_hbm, dqkv_hbm, ctx_hbm, mid_hbm, emb_hbm, in_hbm, vec_hbm) = refs[:7]
    outs = refs[7:10]
    (a_turned, d_qkv, ctx_turned, d_mid_b, emb_turned, x_in, g_vec, load_sem) = refs[10:18]
    (accs, owns, gives, twins), sems = split_scratch(refs[18:], 3)
    place = Place()
    loads = [pltpu.make_async_copy(src, dst, load_sem.at[n]) for n, (src, dst) in enumerate(
        ((a_hbm, a_turned), (dqkv_hbm, d_qkv), (ctx_hbm, ctx_turned), (mid_hbm, d_mid_b), (emb_hbm, emb_turned), (in_hbm, x_in), (vec_hbm, g_vec)))]
    for load in loads[:2]:
        load.start()
    place.meet()
    product = term_of(REST_STREAMS, {QKV: a_turned, OUT: ctx_turned, MISC: emb_turned}, {QKV: d_qkv, OUT: d_mid_b, MISC: x_in}, place.core)

    def term(i, chip):
        arr, row, rows, col, cols, _ = REST_STREAMS[i]
        block = product(i, chip)
        if arr == MISC and col >= 256:
            first = pl.multiple_of(2 * chip * ARRAYS[arr][0] + row, 16)
            extra = g_vec[pl.ds(first, rows), pl.ds(col - 256, cols)]
            block = block + jnp.concatenate([jnp.where(place.core == side, extra, 0.0) for side in (1, 0)], axis=1)
        return block

    ring = RingSum(place, (QKV, OUT, MISC), REST_STREAMS, accs, owns, gives, twins, sems, term)

    def ready(group):
        for load in loads[2:] if group else loads[:2]:
            load.wait()
        if not group:
            for load in loads[2:]:
                load.start()

    ring.run((tuple(range(6)), tuple(range(6, len(REST_STREAMS)))), lambda half, step: None, ready)
    ring.finish(outs)


def rest_sums(a_turned, d_qkv, ctx_turned, d_mid_b, emb_turned, x_in, g_vec):
    arrays = (QKV, OUT, MISC)
    operands = (a_turned, d_qkv, ctx_turned, d_mid_b, emb_turned, x_in, g_vec)
    anywhere = pl.BlockSpec(memory_space=pl.ANY)
    return pl.pallas_call(
        rest_sums_kernel, out_shape=[jax.ShapeDtypeStruct(ARRAYS[arr], jnp.float32) for arr in arrays],
        in_specs=[anywhere] * 7, out_specs=[anywhere] * 3,
        scratch_shapes=[pltpu.VMEM(a.shape, a.dtype) for a in operands] + [pltpu.SemaphoreType.DMA((7,))] + ring_scratch(arrays, REST_STREAMS),
        compiler_params=pltpu.CompilerParams(collective_id=2, has_side_effects=True, vmem_limit_bytes=62 * 1024 * 1024), name='rest_sums',
    )(*operands)


def whole(shape):
    return pl.BlockSpec(shape, lambda i: (0, 0), pipeline_mode=pl.Buffered(1))


def rows_of(width):
    return pl.BlockSpec((ROWS, width), lambda i: (i, 0))


def stage_call(body, name, n_rows, ins, outs, scratch=()):
    in_specs = [rows_of(a.shape[1]) if a.shape[0] == n_rows and not held else whole(a.shape) for a, held in ins]
    out_specs, out_shape = [], []
    for width, dtype in outs:
        if dtype is None:
            out_specs.append(pl.BlockSpec((VEC_ROWS, 1024), lambda i: (0, 0)))
            out_shape.append(jax.ShapeDtypeStruct((VEC_ROWS, 1024), jnp.float32))
        elif width < 0:
            out_specs.append(pl.BlockSpec((-width, ROWS), lambda i: (0, i)))
            out_shape.append(jax.ShapeDtypeStruct((-width, n_rows), dtype))
        else:
            out_specs.append(rows_of(width))
            out_shape.append(jax.ShapeDtypeStruct((n_rows, width), dtype))
    return pl.pallas_call(body, grid=(n_rows // ROWS,), in_specs=in_specs, out_specs=out_specs, out_shape=out_shape, scratch_shapes=list(scratch),
                          compiler_params=pltpu.CompilerParams(vmem_limit_bytes=62 * 1024 * 1024, dimension_semantics=('arbitrary',)), name=name)(*[a for a, _ in ins])

N_PIXEL, N_POS = 768, 197
MISC_USED = N_PIXEL + N_POS + len(VEC_NAMES) + 3 + 4


def solution(mesh):
    n_dev = mesh.shape[MESH_AXIS]

    def spec_of(name):
        return P(None, MESH_AXIS) if name in LAST_SPLIT else P(MESH_AXIS)

    def pack_misc(part):
        lane = part['b_patch'].shape[0]
        flat = [part[name] for name in VEC_NAMES] + [part['b_qkv'], part['b_fc'], jnp.zeros(((1024 - MISC_USED) * lane,), jnp.float32)]
        vectors = lax.optimization_barrier(jnp.concatenate(flat)).reshape(-1, lane)
        return jnp.concatenate([part['w_patch'], part['pos_table'], vectors], axis=0).astype(jnp.bfloat16).T

    def unpack_misc(misc):
        turned = misc.T
        part = {'w_patch': turned[:N_PIXEL], 'pos_table': turned[N_PIXEL:N_PIXEL + N_POS]}
        first = N_PIXEL + N_POS
        for place, name in enumerate(VEC_NAMES):
            part[name] = turned[first + place]
        first += len(VEC_NAMES)
        part['b_qkv'] = turned[first:first + 3].reshape(-1)
        part['b_fc'] = turned[first + 3:first + 7].reshape(-1)
        return part

    def flat_of(rows):
        return rows.reshape(rows.shape[0], n_dev, -1).transpose(1, 0, 2).reshape(rows.shape)

    def shards_of(rows):
        return rows.reshape(n_dev, rows.shape[0], -1).transpose(1, 0, 2).reshape(rows.shape)

    def local_step(patches, keep, *rest):
        shards = dict(zip(PARAM_NAMES, rest[:-1]))
        grad_h1 = rest[-1]
        n_img, n_patch, _ = patches.shape
        n_token, d_model = grad_h1.shape[1:]
        n_shard, _, n_heads, head_dim = shards['w_qkv'].shape
        n_rows = n_img * SEQ
        casts = {name: shards[name].astype(jnp.bfloat16) for name in ('w_fc', 'w_proj', 'w_qkv', 'w_out')}
        w_qkv, w_out, misc = gather_first((casts['w_qkv'].reshape(n_shard, -1), casts['w_out'], pack_misc(shards)))
        position = jnp.pad(keep + 1, ((0, 0), (1, 0)))
        position = jnp.pad(position, ((0, 0), (0, SEQ - n_token)), constant_values=-1)[:, :, None]
        onehot_patch = (position == 1 + lax.broadcasted_iota(jnp.int32, (1, 1, n_patch), 2)).astype(jnp.bfloat16)
        onehot_pos = (position == lax.broadcasted_iota(jnp.int32, (1, 1, 1024 - N_PIXEL), 2)).astype(jnp.bfloat16)
        kept_rows = jnp.einsum('bkp,bpq->bkq', onehot_patch, patches, preferred_element_type=jnp.float32).astype(jnp.bfloat16)
        x_in = jnp.concatenate([kept_rows, onehot_pos], axis=2).reshape(n_rows, 1024)
        grad_rows = jnp.pad(grad_h1, ((0, 0), (0, SEQ - n_token), (0, 0))).reshape(n_rows, d_model)

        n_vec = len(VEC_NAMES)
        packed = misc[:, 896:].T[N_PIXEL + N_POS - 896:MISC_USED - 896].astype(jnp.float32)
        vecs = jnp.concatenate([packed[:n_vec], flat_of(packed[n_vec:n_vec + 3]), flat_of(packed[n_vec + 3:]), jnp.zeros((VEC_ROWS - packed.shape[0], 1024), jnp.float32)], axis=0)

        bf, f32 = jnp.bfloat16, jnp.float32
        w_fc, w_proj, x_zero, a_turned, qkv, ctx_turned, h_mid, c_in, c_turned = gather_second(casts['w_fc'], casts['w_proj'], x_in, misc, w_qkv, w_out, vecs)
        gelu_turned, d_pre, h_one, d_mid, d_mid_b, sums_two = stage_call(
            stage_two, 'stage_two', n_rows, [(c_in, False), (h_mid, False), (grad_rows, False), (w_fc, True), (w_proj, True), (vecs, True)],
            [(-4096, bf), (4096, bf), (1024, bf), (1024, f32), (1024, bf), (0, None)],
            [pltpu.VMEM((ROWS, 1024), f32), pltpu.VMEM((ROWS, 1024), f32)])
        h_one = h_one.reshape(n_img, SEQ, d_model)[:, :n_token]
        fc_sum, proj_sum, d_qkv, emb_turned, sums_three = mlp_sums(c_turned, d_pre, gelu_turned, grad_rows, w_qkv, w_out, vecs, x_zero, d_mid, d_mid_b, qkv)
        sums = sums_two + sums_three
        vec_rows = jnp.concatenate([sums[:n_vec], shards_of(sums[VEC_QKV:VEC_QKV + 3]), shards_of(sums[VEC_FC:VEC_FC + 4])], axis=0)
        g_rows = jnp.concatenate([sums[VEC_AT['cls_tok']][None], jnp.zeros((N_POS - 1, 1024), f32), vec_rows], axis=0)
        g_vec = jnp.pad(g_rows, ((0, 1024 - N_PIXEL - g_rows.shape[0]), (0, 0))).T
        qkv_sum, out_sum, misc_sum = rest_sums(a_turned, d_qkv, ctx_turned, d_mid_b, emb_turned, x_in, g_vec)
        own = unpack_misc(misc_sum)
        own.update(w_fc=fc_sum, w_proj=proj_sum, w_qkv=qkv_sum.reshape(n_shard, 3, n_heads, head_dim), w_out=out_sum)
        return (h_one,) + tuple(own[name] for name in PARAM_NAMES)

    batch_spec = P(MESH_AXIS)
    param_specs = tuple(spec_of(name) for name in PARAM_NAMES)
    return jax.shard_map(local_step, mesh=mesh, in_specs=(batch_spec, batch_spec) + param_specs + (batch_spec,), out_specs=(batch_spec,) + param_specs, check_vma=False)
```
